256 devices in a mesh: site: 32 (over x_hi, z, core), sec: 8 (over y, x_lo).
Axes of the slice: x: 4 (x_hi: 2, x_lo: 2; x = x_hi * 2 + x_lo), y: 4, z: 8, core: 2. Of those that a mesh axis runs over, the one named last changes fastest.
Arguments:
- left_canon: bfloat16 [32, 4, 16, 128, 128], P('site', None, 'sec'), may hold values from -1.5 to 1.5
- right_canon: bfloat16 [32, 4, 16, 128, 128], P('site', None, 'sec'), may hold values from -1.5 to 1.5
- center_site: bfloat16 [32, 4, 16, 128, 128], P('site', None, 'sec'), may hold values from -6 to 6
- center_bond: bfloat16 [32, 16, 128, 128], P('site', 'sec'), may hold values from -2 to 3
- left_seed: bfloat16 [32, 16, 128, 128], P('site', 'sec'), may hold values from -2 to 4
- right_seed: bfloat16 [32, 16, 128, 128], P('site', 'sec'), may hold values from -2 to 4
- left_sector: int32 [32, 4, 16], P('site'), may hold values from 0 to 15, each once within a row
- onsite: float32 [32, 4], P('site'), may hold values from 0.5 to 2
- bond_shift: float32 [32], P('site'), may hold values from 0.5 to 2
Outputs:
- left_new: bfloat16 [32, 4, 16, 128, 128], P('site', None, 'sec')
- right_new: bfloat16 [32, 4, 16, 128, 128], P('site', None, 'sec')
The draws below stay inside these ranges and needn't reach their ends.
Inputs may be any that keep to these rules, and one draw needn't show every extreme that they name: `left_sector`: for each site and local state the 16 entries are a permutation of the sectors.
All inputs are finite; a program needn't handle non-finite values.
Results may differ from the reference program's by a relative error of at most 0.028.
Values may be sent and summed in bfloat16 or wider, within the bound.
A program may use at most 64 MiB of HBM per device.

```python
import math
import jax
import jax.numpy as jnp
from jax import lax

B = 128
PHYS = 4
NSI = 10
NAPP = 2
SITES = 32
NSEC = 16
RCH = 8


def noise_shaped(key, shape):
    values = jnp.clip(jax.random.normal(key, shape, jnp.float32), -4.0, 4.0)
    return values


def noise_field(key):
    return noise_shaped(key, (SITES, NSEC, B, B))


def canon_tensor(key):
    values = noise_shaped(jax.random.fold_in(key, 3), (SITES, PHYS, NSEC, B, B))
    leading = jax.random.randint(jax.random.fold_in(key, 5), (SITES,), 0, PHYS)
    states = jnp.arange(PHYS, dtype=jnp.int32)
    weights = jnp.where(states[None, :] == leading[:, None], 0.9, 0.2).astype(jnp.float32)
    identity = jnp.eye(B, dtype=jnp.float32)
    return (weights[:, :, None, None, None] * identity + 0.25 / math.sqrt(B) * values).astype(jnp.bfloat16)


def symmetric_seed(key):
    values = noise_field(jax.random.fold_in(key, 1))
    mixed = (values + jnp.swapaxes(values, -1, -2)) * 0.70710678
    levels = jnp.exp(jax.random.uniform(jax.random.fold_in(key, 2), (SITES, NSEC), jnp.float32, math.log(0.5), math.log(2.0)))
    blocks = jnp.eye(B, dtype=jnp.float32) + 0.5 / math.sqrt(B) * mixed
    return (levels[:, :, None, None] * blocks).astype(jnp.bfloat16)


def draw_left_canon(key, part):
    return canon_tensor(jax.random.fold_in(key, 41))


def draw_right_canon(key, part):
    return canon_tensor(jax.random.fold_in(key, 53))


def draw_center_bond(key, part):
    values = noise_field(jax.random.fold_in(key, 11))
    return (jnp.eye(B, dtype=jnp.float32) + 0.3 / math.sqrt(B) * values).astype(jnp.bfloat16)


def draw_left_seed(key, part):
    return symmetric_seed(jax.random.fold_in(key, 23))


def draw_right_seed(key, part):
    return symmetric_seed(jax.random.fold_in(key, 37))


def shard_levels(key, dims, shards, smallest, largest):
    gain, own = 1.0, jax.random.fold_in(key, 6)
    for position, shards_of in shards:
        draws = jnp.exp(jax.random.uniform(jax.random.fold_in(own, position), (shards_of,), jnp.float32, smallest / len(shards), largest / len(shards)))
        gain = gain * jnp.repeat(draws, dims[position] // shards_of).reshape([-1 if axis == position else 1 for axis in range(len(dims))])
    return gain


def bell_draw(own_key, shape, width, bound, pieces=(), kind=jnp.bfloat16):
    drawn = jax.random.normal(own_key, shape, jnp.float32) * width
    if len(pieces) > 0:
        drawn = shard_levels(own_key, shape, pieces, -0.22, 0.18) * drawn
    return jnp.clip(drawn, min=-bound, max=bound).astype(kind)


def setup_inputs(seed: int = 0) -> dict:
    keys = jax.random.split(jax.random.key(seed), 10)
    left_canon = draw_left_canon(jax.random.fold_in(keys[9], 71), 0)
    right_canon = draw_right_canon(jax.random.fold_in(keys[9], 71), 0)
    center_site = bell_draw(keys[2], (SITES, PHYS, NSEC, B, B), 1.0, 6.0, ((0, 32), (2, 8)))
    center_bond = draw_center_bond(jax.random.fold_in(keys[9], 71), 0)
    left_seed = draw_left_seed(jax.random.fold_in(keys[9], 71), 0)
    right_seed = draw_right_seed(jax.random.fold_in(keys[9], 71), 0)
    left_sector = jax.vmap(lambda own: jax.random.permutation(own, NSEC))(jax.random.split(keys[6], SITES * PHYS)).reshape((SITES, PHYS, NSEC)).astype(jnp.int32)
    onsite = jnp.clip(jnp.exp(math.log(2.0) - 1.3862944 * jax.random.uniform(keys[7], (SITES, PHYS), jnp.float32) ** shard_levels(keys[7], (SITES, PHYS), ((0, 32),), -0.2, 0.2)), 0.5, 2.0)
    bond_shift = jnp.clip(jnp.exp(math.log(2.0) - 1.3862944 * jax.random.uniform(keys[8], (SITES,), jnp.float32) ** shard_levels(keys[8], (SITES,), ((0, 32),), -0.2, 0.2)), 0.5, 2.0)
    return {"left_canon": left_canon, "right_canon": right_canon, "center_site": center_site, "center_bond": center_bond, "left_seed": left_seed, "right_seed": right_seed, "left_sector": left_sector, "onsite": onsite, "bond_shift": bond_shift}


def pick_blocks(blocks, indices):
    return jax.vmap(lambda chosen, where_at: jnp.take(chosen, where_at, axis=0))(blocks, indices)

def inverse_root(gram_mat):
    scaling = jnp.sqrt(lax.optimization_barrier(jnp.sum(gram_mat * gram_mat, axis=(-2, -1), keepdims=True)))
    identity = jnp.eye(gram_mat.shape[-1], dtype=jnp.float32)
    upper_part = gram_mat / scaling
    lower_part = jnp.broadcast_to(identity, gram_mat.shape)
    for repeat in range(NSI):
        middle = 1.5 * identity - 0.5 * jnp.matmul(lower_part, upper_part, precision=lax.Precision.HIGHEST)
        upper_part = jnp.matmul(upper_part, middle, precision=lax.Precision.HIGHEST)
        lower_part = jnp.matmul(middle, lower_part, precision=lax.Precision.HIGHEST)
    return lower_part / jnp.sqrt(scaling)

def trace_sum(blocks):
    return lax.optimization_barrier(jnp.sum(jnp.diagonal(blocks.astype(jnp.float32), axis1=2, axis2=3), axis=(1, 2)))

def reference(left_canon, right_canon, center_site, center_bond, left_seed, right_seed, left_sector, onsite, bond_shift):
    labels = jnp.arange(NSEC, dtype=jnp.int32)
    right_of = lax.optimization_barrier(jnp.sum(jnp.where(left_sector[:, :, :, None] == labels[None, None, None, :], labels[None, None, :, None], 0), axis=2)).astype(jnp.int32)
    routing = (left_sector[:, :, :, None] == labels[None, None, None, :]).astype(jnp.float32)

    def left_step(hold):
        running = jnp.zeros(hold.shape, jnp.float32)
        for physical in range(PHYS):
            tensor = left_canon[:, physical].astype(jnp.float32)
            chosen = pick_blocks(hold, left_sector[:, physical]).astype(jnp.float32)
            product = jnp.einsum('jkab,jkbc->jkac', chosen, tensor).astype(jnp.bfloat16)
            running = running + jnp.einsum('jkba,jkbc->jkac', tensor, product.astype(jnp.float32))
        return running.astype(jnp.bfloat16)

    def right_step(hold):
        running = jnp.zeros(hold.shape, jnp.float32)
        for physical in range(PHYS):
            picked = pick_blocks(right_canon[:, physical], right_of[:, physical]).astype(jnp.float32)
            env_chosen = pick_blocks(hold, right_of[:, physical]).astype(jnp.float32)
            product = jnp.einsum('jkab,jkbc->jkac', picked, env_chosen).astype(jnp.bfloat16)
            running = running + jnp.einsum('jkac,jkdc->jkad', product.astype(jnp.float32), picked)
        return running.astype(jnp.bfloat16)
    left_hold = left_seed
    right_hold = right_seed
    left_fresh = left_seed
    for step in range(RCH):
        left_fresh = left_step(left_hold)
        right_fresh = right_step(right_hold)
        left_hold = jnp.roll(left_fresh, 1, axis=0)
        right_hold = jnp.roll(right_fresh, -1, axis=0)
    dim_all = NSEC * B

    def scaled(blocks):
        return (blocks.astype(jnp.float32) * (dim_all / trace_sum(blocks))[:, None, None, None]).astype(jnp.bfloat16)
    cur_scaled = scaled(left_hold)
    next_scaled = scaled(left_fresh)
    right_scaled = scaled(right_hold)
    chosen_left = pick_blocks(cur_scaled, left_sector).astype(jnp.float32)
    site_now = center_site
    bond_now = center_bond
    for repeat in range(NAPP):
        half_site = jnp.einsum('jskab,jskbc->jskac', chosen_left, site_now.astype(jnp.float32)).astype(jnp.bfloat16)
        site_now = (jnp.einsum('jskab,jkbc->jskac', half_site.astype(jnp.float32), right_scaled.astype(jnp.float32)) + onsite[:, :, None, None, None] * site_now.astype(jnp.float32)).astype(jnp.bfloat16)
        half_bond = jnp.einsum('jkab,jkbc->jkac', next_scaled.astype(jnp.float32), bond_now.astype(jnp.float32)).astype(jnp.bfloat16)
        bond_now = (jnp.einsum('jkab,jkbc->jkac', half_bond.astype(jnp.float32), right_scaled.astype(jnp.float32)) + bond_shift[:, None, None, None] * bond_now.astype(jnp.float32)).astype(jnp.bfloat16)
    site_wide = site_now.astype(jnp.float32)
    bond_wide = bond_now.astype(jnp.float32)
    gram_left = jnp.einsum('jskab,jskac->jkbc', site_wide, site_wide)
    gram_bond = jnp.einsum('jkab,jkac->jkbc', bond_wide, bond_wide)
    unit_left = jnp.matmul(bond_wide, inverse_root(gram_bond), precision=lax.Precision.HIGHEST)
    factor_left = jnp.matmul(inverse_root(gram_left), jnp.swapaxes(unit_left, -1, -2), precision=lax.Precision.HIGHEST).astype(jnp.bfloat16)
    left_new = jnp.einsum('jskab,jkbc->jskac', site_wide, factor_left.astype(jnp.float32)).astype(jnp.bfloat16)
    outer_terms = jnp.einsum('jskab,jskcb->jskac', site_wide, site_wide)
    gram_right = jnp.einsum('jskm,jskac->jmac', routing, outer_terms)
    previous = jnp.roll(bond_now, 1, axis=0).astype(jnp.float32)
    gram_prev = jnp.matmul(previous, jnp.swapaxes(previous, -1, -2), precision=lax.Precision.HIGHEST)
    unit_right = jnp.matmul(inverse_root(gram_prev), previous, precision=lax.Precision.HIGHEST)
    factor_right = jnp.matmul(jnp.swapaxes(unit_right, -1, -2), inverse_root(gram_right), precision=lax.Precision.HIGHEST).astype(jnp.bfloat16)
    factor_chosen = pick_blocks(factor_right, left_sector).astype(jnp.float32)
    right_new = jnp.einsum('jskab,jskbc->jskac', factor_chosen, site_wide).astype(jnp.bfloat16)
    return (left_new, right_new)
```

```python
import functools

import jax
import jax.numpy as jnp
from jax import lax
from jax.experimental import pallas as pl
from jax.experimental.pallas import tpu as pltpu
from jax.sharding import PartitionSpec as P

NSI = 10
NAPP = 2
CHUNKS = 4
MESH = pl.DeviceIdType.MESH


def from_behind(block, axis, distance):
    devices = range(lax.axis_size(axis))
    route = [((i - distance) % len(devices), i) for i in devices]
    return lax.ppermute(block, axis, route)


def in_blocks(array, dim, length):
    lengths = array.shape
    blocks = array.reshape(*lengths[:dim], length, lengths[dim] // length, *lengths[dim + 1 :])
    return jnp.moveaxis(blocks, dim, 0)


def sent_and_summed(array, axis, dim):
    length = lax.axis_size(axis)
    blocks = lax.all_to_all(in_blocks(array, dim, length), axis, 0, 0, tiled=True)
    return jnp.sum(blocks, axis=0)


def in_order(blocks, dim):
    blocks = jnp.moveaxis(blocks, 0, dim)
    lengths = blocks.shape
    return blocks.reshape(*lengths[:dim], lengths[dim] * lengths[dim + 1], *lengths[dim + 2 :])


def from_everyone(array, axis):
    copies = jnp.broadcast_to(array, (lax.axis_size(axis), *array.shape))
    return lax.all_to_all(copies, axis, split_axis=0, concat_axis=0, tiled=True)


def collect(array, axis, dim):
    return in_order(from_everyone(array, axis), dim)


def inverse_root(gram_mat):
    scaling = jnp.sqrt(jnp.sum(gram_mat * gram_mat, axis=(-2, -1), keepdims=True))
    identity = jnp.eye(gram_mat.shape[-1], dtype=jnp.float32)
    upper_part = gram_mat / scaling
    lower_part = jnp.broadcast_to(identity, gram_mat.shape)
    for repeat in range(NSI):
        middle = 1.5 * identity - 0.5 * jnp.matmul(
            lower_part, upper_part, precision=lax.Precision.HIGHEST
        )
        upper_part = jnp.matmul(upper_part, middle, precision=lax.Precision.HIGHEST)
        lower_part = jnp.matmul(middle, lower_part, precision=lax.Precision.HIGHEST)
    return lower_part / jnp.sqrt(scaling)


def env_kernel(
    sites, secs, steps,
    tab, canon_l, canon_r, seed_l, seed_r,
    cur_out, nxt_out, rgt_out,
    own_c, own_s, tall, wab, hold, fresh, pbuf, give, got_n, got_r,
    loc_sem, gsend, grecv, ssend, srecv, tsend, trecv, xsend, xrecv,
):
    site, sec = lax.axis_index("site"), lax.axis_index("sec")
    role = lax.rem(sec, 2)
    row = sec // 2
    rows = secs // 2
    phys, owned, width = canon_l.shape[0], canon_l.shape[1], canon_l.shape[2]
    sectors = secs * owned
    per = sectors // CHUNKS
    target = lax.rem(site + 1 - 2 * role + sites, sites)
    source = lax.rem(site - 1 + 2 * role + sites, sites)
    peer_sec = row * 2 + 1 - role

    loads = [
        pltpu.make_async_copy(canon_l, own_c.at[0], loc_sem.at[0]),
        pltpu.make_async_copy(canon_r, own_c.at[1], loc_sem.at[1]),
    ]
    for load in loads:
        load.start()
    for i in range(owned):
        own_s[0, i] = seed_l[i]
        own_s[1, i] = seed_r[i].T

    barrier = pltpu.get_barrier_semaphore()
    others = [(dy, e) for dy in range(rows) for e in range(2) if (dy, e) != (0, 0)]

    def sec_of(dy, e):
        other_role = role + e - 2 * role * e
        return lax.rem(row + dy, rows) * 2 + other_role, other_role

    for dy, e in others:
        pl.semaphore_signal(barrier, inc=1, device_id=(site, sec_of(dy, e)[0]), device_id_type=MESH)
    for other in (target, source):
        pl.semaphore_signal(barrier, inc=1, device_id=(other, sec), device_id_type=MESH)
    pl.semaphore_wait(barrier, len(others) + 2)

    place = pl.ds(sec * owned, owned)
    sent = []
    for n, (dy, e) in enumerate(others):
        to, to_role = sec_of(dy, e)
        sent.append(pltpu.make_async_remote_copy(
            src_ref=own_s.at[to_role], dst_ref=hold.at[0, place],
            send_sem=ssend.at[n], recv_sem=srecv.at[n],
            device_id=(site, to), device_id_type=MESH))
        sent[-1].start()
    for load in loads:
        load.wait()
    keep = [
        pltpu.make_async_copy(own_c.at[role], tall.at[:, place], loc_sem.at[0]),
        pltpu.make_async_copy(own_s.at[role], hold.at[0, place], loc_sem.at[1]),
    ]
    for n, (dy, e) in enumerate(others):
        to, to_role = sec_of(dy, e)
        sent.append(pltpu.make_async_remote_copy(
            src_ref=own_c.at[to_role], dst_ref=tall.at[:, place],
            send_sem=gsend.at[n], recv_sem=grecv.at[n],
            device_id=(site, to), device_id_type=MESH))
        sent[-1].start()
    for copy in keep:
        copy.start()
    for copy in keep:
        copy.wait()
    for copy in sent:
        copy.wait_recv()

    def arrange(i, carry):
        for s in range(phys):
            cols = slice(s * width, (s + 1) * width)
            wab[role, i, :, cols] = tall[s, tab[1, s, i]]
            wab[1 - role, i, :, cols] = tall[s, i].T
        return carry

    lax.fori_loop(0, sectors, arrange, 0)

    def chunk_copy(t, c):
        part = pl.ds(c * per, per)
        return pltpu.make_async_remote_copy(
            src_ref=fresh.at[t, part], dst_ref=hold.at[t + 1, part],
            send_sem=tsend.at[t, c], recv_sem=trecv.at[t, c],
            device_id=(target, sec), device_id_type=MESH)

    def turn(t, carry):
        for c in range(CHUNKS):
            @pl.when(t > 0)
            def _():
                chunk_copy(t - 1, c).wait_recv()

            for i in range(c * per, (c + 1) * per):
                product = jnp.dot(
                    hold[t, i], wab[0, i], preferred_element_type=jnp.float32
                ).astype(jnp.bfloat16)
                for s in range(phys):
                    pbuf[i, s] = product[:, s * width : (s + 1) * width]
        for c in range(CHUNKS):
            for o in range(c * per, (c + 1) * per):
                stack = jnp.concatenate([pbuf[tab[role, s, o], s] for s in range(phys)], axis=0)
                fresh[t, o] = jnp.dot(
                    wab[1, o], stack, preferred_element_type=jnp.float32
                ).astype(jnp.bfloat16)
            chunk_copy(t, c).start()
        return carry

    lax.fori_loop(0, steps, turn, 0)
    for c in range(CHUNKS):
        chunk_copy(steps - 1, c).wait_recv()

    rows_at = lax.broadcasted_iota(jnp.int32, (width, width), 0)
    cols_at = lax.broadcasted_iota(jnp.int32, (width, width), 1)
    diagonal = rows_at == cols_at

    def factor(ref, t):
        total = ref[t, 0].astype(jnp.float32)
        for i in range(1, sectors):
            total = total + ref[t, i].astype(jnp.float32)
        return (sectors * width) / jnp.sum(jnp.where(diagonal, total, 0.0))

    own_at = sec * owned
    peer_at = peer_sec * owned
    cur_copies = [pltpu.make_async_remote_copy(
        src_ref=give.at[pl.ds(c * per, per)], dst_ref=cur_out.at[pl.ds(c * per, per)],
        send_sem=xsend.at[c], recv_sem=xrecv.at[c],
        device_id=(site, peer_sec), device_id_type=MESH) for c in range(CHUNKS)]
    nxt_copy = pltpu.make_async_remote_copy(
        src_ref=got_r, dst_ref=got_n,
        send_sem=xsend.at[CHUNKS], recv_sem=xrecv.at[CHUNKS],
        device_id=(site, peer_sec), device_id_type=MESH)

    @pl.when(role == 0)
    def _():
        scale_next = factor(fresh, steps - 1)
        for i in range(owned):
            got_r[i] = (fresh[steps - 1, peer_at + i].astype(jnp.float32) * scale_next).astype(jnp.bfloat16)
            nxt_out[i] = (fresh[steps - 1, own_at + i].astype(jnp.float32) * scale_next).astype(jnp.bfloat16)
        nxt_copy.start()
        scale_cur = factor(hold, steps)
        for c in range(CHUNKS):
            for i in range(c * per, (c + 1) * per):
                give[i] = (hold[steps, i].astype(jnp.float32) * scale_cur).astype(jnp.bfloat16)
            cur_copies[c].start()
        for i in range(sectors):
            cur_out[i] = give[i]
        nxt_copy.wait_recv()
        for i in range(owned):
            rgt_out[i] = got_n[i].T
        nxt_copy.wait_send()
        for copy in cur_copies:
            copy.wait_send()

    @pl.when(role == 1)
    def _():
        scale_right = factor(hold, steps)
        for i in range(owned):
            got_r[i] = (hold[steps, peer_at + i].astype(jnp.float32) * scale_right).astype(jnp.bfloat16)
        nxt_copy.start()
        for i in range(owned):
            rgt_out[i] = (hold[steps, own_at + i].astype(jnp.float32) * scale_right).astype(jnp.bfloat16).T
        nxt_copy.wait_recv()
        for i in range(owned):
            nxt_out[i] = got_n[i]
        nxt_copy.wait_send()
        for copy in cur_copies:
            copy.wait_recv()

    for copy in sent:
        copy.wait_send()

    def drain(t, carry):
        for c in range(CHUNKS):
            chunk_copy(t, c).wait_send()
        return carry

    lax.fori_loop(0, steps, drain, 0)


def environments(canon_l, canon_r, seed_l, seed_r, tables):
    sites, secs = lax.axis_size("site"), lax.axis_size("sec")
    steps = sites // 4
    phys, owned, width = canon_l.shape[:3]
    sectors = owned * secs
    bf16 = jnp.bfloat16
    block = (width, width)
    dma = pltpu.SemaphoreType.DMA
    vmem = pl.BlockSpec(memory_space=pltpu.VMEM)
    hbm = pl.BlockSpec(memory_space=pl.ANY)
    return pl.pallas_call(
        functools.partial(env_kernel, sites, secs, steps),
        out_shape=(
            jax.ShapeDtypeStruct((sectors, *block), bf16),
            jax.ShapeDtypeStruct((owned, *block), bf16),
            jax.ShapeDtypeStruct((owned, *block), bf16),
        ),
        in_specs=[pl.BlockSpec(memory_space=pltpu.SMEM), hbm, hbm, vmem, vmem],
        out_specs=(vmem, vmem, vmem),
        scratch_shapes=[
            pltpu.VMEM((2, phys, owned, *block), bf16),
            pltpu.VMEM((2, owned, *block), bf16),
            pltpu.VMEM((phys, sectors, *block), bf16),
            pltpu.VMEM((2, sectors, width, phys * width), bf16),
            pltpu.VMEM((steps + 1, sectors, *block), bf16),
            pltpu.VMEM((steps, sectors, *block), bf16),
            pltpu.VMEM((sectors, phys, *block), bf16),
            pltpu.VMEM((sectors, *block), bf16),
            pltpu.VMEM((owned, *block), bf16),
            pltpu.VMEM((owned, *block), bf16),
            dma((2,)), dma((secs - 1,)), dma((secs - 1,)), dma((secs - 1,)), dma((secs - 1,)),
            dma((steps, CHUNKS)), dma((steps, CHUNKS)), dma((CHUNKS + 1,)), dma((CHUNKS + 1,)),
        ],
        compiler_params=pltpu.CompilerParams(
            collective_id=0, has_side_effects=True, vmem_limit_bytes=48 * 1024 * 1024
        ),
        name="environments",
    )(tables, canon_l, canon_r, seed_l, seed_r)


def per_device(
    left_canon,
    right_canon,
    center_site,
    center_bond,
    left_seed,
    right_seed,
    left_sector,
    onsite,
    bond_shift,
):
    canon_left = left_canon[0]
    canon_right = right_canon[0]
    site_now = center_site[0]
    bond_now = center_bond[0]
    sources = left_sector[0]
    energy = onsite[0]
    bond_add = bond_shift[0]
    owned = canon_left.shape[1]
    sectors = sources.shape[1]
    offset = lax.axis_index("sec") * owned
    labels = jnp.arange(sectors, dtype=jnp.int32)
    right_of = jnp.sum(
        jnp.where(sources[:, :, None] == labels[None, None, :], labels[None, :, None], 0), axis=1
    )
    own_sources = lax.dynamic_slice_in_dim(sources, offset, owned, 1)
    cur_scaled, next_scaled, right_scaled = environments(
        canon_left, canon_right, left_seed[0], right_seed[0], jnp.stack([sources, right_of])
    )
    chosen_left = jnp.take(cur_scaled, own_sources, axis=0)
    for repeat in range(NAPP):
        half_site = jnp.einsum(
            "skab,skbc->skac", chosen_left, site_now, preferred_element_type=jnp.float32
        ).astype(jnp.bfloat16)
        site_now = (
            jnp.einsum(
                "skab,kbc->skac", half_site, right_scaled, preferred_element_type=jnp.float32
            )
            + energy[:, None, None, None] * site_now.astype(jnp.float32)
        ).astype(jnp.bfloat16)
        half_bond = jnp.einsum(
            "kab,kbc->kac", next_scaled, bond_now, preferred_element_type=jnp.float32
        ).astype(jnp.bfloat16)
        bond_now = (
            jnp.einsum("kab,kbc->kac", half_bond, right_scaled, preferred_element_type=jnp.float32)
            + bond_add * bond_now.astype(jnp.float32)
        ).astype(jnp.bfloat16)
    gram_left = jnp.einsum("skab,skac->kbc", site_now, site_now, preferred_element_type=jnp.float32)
    gram_bond = jnp.einsum("kab,kac->kbc", bond_now, bond_now, preferred_element_type=jnp.float32)
    unit_left = jnp.matmul(
        bond_now.astype(jnp.float32), inverse_root(gram_bond), precision=lax.Precision.HIGHEST
    )
    factor_left = jnp.matmul(
        inverse_root(gram_left), jnp.swapaxes(unit_left, -1, -2), precision=lax.Precision.HIGHEST
    ).astype(jnp.bfloat16)
    left_new = jnp.einsum(
        "skab,kbc->skac", site_now, factor_left, preferred_element_type=jnp.float32
    ).astype(jnp.bfloat16)
    outer_terms = jnp.einsum(
        "skab,skcb->skac", site_now, site_now, preferred_element_type=jnp.float32
    )
    routing = (own_sources[:, :, None] == labels[None, None, :]).astype(jnp.float32)
    buffer_all = jnp.einsum("skm,skac->mac", routing, outer_terms, precision=lax.Precision.HIGHEST)
    unit_right = from_behind(unit_left, "site", 1)
    gram_right = sent_and_summed(buffer_all, "sec", 0)
    factor_part = jnp.matmul(
        jnp.swapaxes(unit_right, -1, -2), inverse_root(gram_right), precision=lax.Precision.HIGHEST
    ).astype(jnp.bfloat16)
    factor_right = collect(factor_part, "sec", 0)
    factor_chosen = jnp.take(factor_right, own_sources, axis=0)
    right_new = jnp.einsum(
        "skab,skbc->skac", factor_chosen, site_now, preferred_element_type=jnp.float32
    ).astype(jnp.bfloat16)
    return (left_new[None], right_new[None])


def solution(mesh):
    return jax.shard_map(
        per_device,
        mesh=mesh,
        in_specs=(
            P("site", None, "sec", None, None),
            P("site", None, "sec", None, None),
            P("site", None, "sec", None, None),
            P("site", "sec", None, None),
            P("site", "sec", None, None),
            P("site", "sec", None, None),
            P("site", None, None),
            P("site", None),
            P("site"),
        ),
        out_specs=(P("site", None, "sec", None, None), P("site", None, "sec", None, None)),
        check_vma=False,
    )
```

```python
import functools

import jax
import jax.numpy as jnp
from jax import lax
from jax.experimental import pallas as pl
from jax.experimental.pallas import tpu as pltpu
from jax.sharding import PartitionSpec as P

NSI = 10
NAPP = 2
CHUNKS = 4
MESH = pl.DeviceIdType.MESH


def update_kernel(
    sites, secs, steps,
    tab, energy, bond_add, canon_l, canon_r, seed_l, seed_r, site_in, bond_in,
    left_out, right_out,
    own_c, own_s, tall, wab, hold, fresh, pbuf, give, got, nxt, rgt, site_v, bond_v,
    outer, gram_s, gram_r, unit_s, unit_r, fac_s, fac,
    loc_sem, gsend, grecv, ssend, srecv, tsend, trecv, xsend, xrecv,
    usem, osend, orecv, fsend, frecv,
):
    site, sec = lax.axis_index("site"), lax.axis_index("sec")
    role = lax.rem(sec, 2)
    row = sec // 2
    rows = secs // 2
    phys, owned, width = canon_l.shape[0], canon_l.shape[1], canon_l.shape[2]
    sectors = secs * owned
    per = sectors // CHUNKS
    target = lax.rem(site + 1 - 2 * role + sites, sites)
    source = lax.rem(site - 1 + 2 * role + sites, sites)
    peer_sec = row * 2 + 1 - role

    loads = [
        pltpu.make_async_copy(canon_l, own_c.at[0], loc_sem.at[0]),
        pltpu.make_async_copy(canon_r, own_c.at[1], loc_sem.at[1]),
    ]
    center = [
        pltpu.make_async_copy(site_in, site_v, loc_sem.at[2]),
        pltpu.make_async_copy(bond_in, bond_v, loc_sem.at[3]),
    ]
    for load in loads + center:
        load.start()
    for i in range(owned):
        own_s[0, i] = seed_l[i]
        own_s[1, i] = seed_r[i].T

    barrier = pltpu.get_barrier_semaphore()
    others = [(dy, e) for dy in range(rows) for e in range(2) if (dy, e) != (0, 0)]

    def sec_of(dy, e):
        other_role = role + e - 2 * role * e
        return lax.rem(row + dy, rows) * 2 + other_role, other_role

    for dy, e in others:
        pl.semaphore_signal(barrier, inc=1, device_id=(site, sec_of(dy, e)[0]), device_id_type=MESH)
    for other in (target, source):
        pl.semaphore_signal(barrier, inc=1, device_id=(other, sec), device_id_type=MESH)
    pl.semaphore_wait(barrier, len(others) + 2)

    place = pl.ds(sec * owned, owned)
    sent = []
    for n, (dy, e) in enumerate(others):
        to, to_role = sec_of(dy, e)
        sent.append(pltpu.make_async_remote_copy(
            src_ref=own_s.at[to_role], dst_ref=hold.at[0, place],
            send_sem=ssend.at[n], recv_sem=srecv.at[n],
            device_id=(site, to), device_id_type=MESH))
        sent[-1].start()
    for load in loads:
        load.wait()
    keep = [
        pltpu.make_async_copy(own_c.at[role], tall.at[:, place], loc_sem.at[0]),
        pltpu.make_async_copy(own_s.at[role], hold.at[0, place], loc_sem.at[1]),
    ]
    for n, (dy, e) in enumerate(others):
        to, to_role = sec_of(dy, e)
        sent.append(pltpu.make_async_remote_copy(
            src_ref=own_c.at[to_role], dst_ref=tall.at[:, place],
            send_sem=gsend.at[n], recv_sem=grecv.at[n],
            device_id=(site, to), device_id_type=MESH))
        sent[-1].start()
    for copy in keep:
        copy.start()
    for copy in keep:
        copy.wait()
    for copy in sent:
        copy.wait_recv()

    def arrange(i, carry):
        for s in range(phys):
            cols = slice(s * width, (s + 1) * width)
            wab[role, i, :, cols] = tall[s, tab[1, s, i]]
            wab[1 - role, i, :, cols] = tall[s, i].T
        return carry

    lax.fori_loop(0, sectors, arrange, 0)

    def chunk_copy(t, c):
        part = pl.ds(c * per, per)
        return pltpu.make_async_remote_copy(
            src_ref=fresh.at[t, part], dst_ref=hold.at[t + 1, part],
            send_sem=tsend.at[t, c], recv_sem=trecv.at[t, c],
            device_id=(target, sec), device_id_type=MESH)

    def turn(t, carry):
        for c in range(CHUNKS):
            @pl.when(t > 0)
            def _():
                chunk_copy(t - 1, c).wait_recv()

            for i in range(c * per, (c + 1) * per):
                product = jnp.dot(
                    hold[t, i], wab[0, i], preferred_element_type=jnp.float32
                ).astype(jnp.bfloat16)
                for s in range(phys):
                    pbuf[i, s] = product[:, s * width : (s + 1) * width]
        for c in range(CHUNKS):
            for o in range(c * per, (c + 1) * per):
                stack = jnp.concatenate([pbuf[tab[role, s, o], s] for s in range(phys)], axis=0)
                fresh[t, o] = jnp.dot(
                    wab[1, o], stack, preferred_element_type=jnp.float32
                ).astype(jnp.bfloat16)
            chunk_copy(t, c).start()
        return carry

    lax.fori_loop(0, steps, turn, 0)
    for load in center:
        load.wait()

    rows_at = lax.broadcasted_iota(jnp.int32, (width, width), 0)
    cols_at = lax.broadcasted_iota(jnp.int32, (width, width), 1)
    diagonal = rows_at == cols_at
    own_at = sec * owned
    peer_at = peer_sec * owned
    f32, bf16 = jnp.float32, jnp.bfloat16

    def scale_of(ref, t):
        total = ref[t, 0].astype(f32)
        for i in range(1, sectors):
            total = total + ref[t, i].astype(f32)
        return (sectors * width) / jnp.sum(jnp.where(diagonal, total, 0.0))

    def scaled(block, scale):
        return (block.astype(f32) * scale).astype(bf16)

    cur_copies = [pltpu.make_async_remote_copy(
        src_ref=hold.at[steps, pl.ds(c * per, per)], dst_ref=hold.at[steps + 1, pl.ds(c * per, per)],
        send_sem=xsend.at[c], recv_sem=xrecv.at[c],
        device_id=(site, peer_sec), device_id_type=MESH) for c in range(CHUNKS)]
    swap = pltpu.make_async_remote_copy(
        src_ref=give, dst_ref=got,
        send_sem=xsend.at[CHUNKS], recv_sem=xrecv.at[CHUNKS],
        device_id=(site, peer_sec), device_id_type=MESH)

    @pl.when(role == 0)
    def _():
        scale_next = scale_of(fresh, steps - 1)
        for i in range(owned):
            give[i] = scaled(fresh[steps - 1, peer_at + i], scale_next)
        swap.start()
        for i in range(owned):
            nxt[i] = scaled(fresh[steps - 1, own_at + i], scale_next)
        for c in range(CHUNKS):
            chunk_copy(steps - 1, c).wait_recv()
            cur_copies[c].start()
        swap.wait_recv()
        for i in range(owned):
            rgt[i] = got[i].T

    @pl.when(role == 1)
    def _():
        for c in range(CHUNKS):
            chunk_copy(steps - 1, c).wait_recv()
        scale_right = scale_of(hold, steps)
        for i in range(owned):
            give[i] = scaled(hold[steps, peer_at + i], scale_right)
        swap.start()
        for i in range(owned):
            rgt[i] = scaled(hold[steps, own_at + i], scale_right).T
        swap.wait_recv()
        for i in range(owned):
            nxt[i] = got[i]

    def split(x):
        high = x.astype(bf16)
        return high, (x - high.astype(f32)).astype(bf16)

    def as_lhs(parts):
        return jnp.concatenate(parts, axis=1)

    def as_rhs(parts):
        wide = jnp.concatenate(parts, axis=1)
        return jnp.concatenate([wide, wide], axis=0)

    def product(lhs, rhs):
        both = jnp.dot(lhs, rhs, preferred_element_type=f32)
        return both[:, :width] + both[:, width:]

    def middle_of(part):
        return jnp.where(diagonal, 1.5, 0.0) - 0.5 * part

    def inverse_roots(grams):
        norms = [jnp.sqrt(jnp.sum(g * g, keepdims=True)) for g in grams]
        uppers, lowers = [], []
        for g, norm in zip(grams, norms):
            start = g / norm
            middle = middle_of(start)
            uppers.append(product(as_lhs(split(start)), as_rhs(split(middle))))
            lowers.append(middle)

        def repeat(n, carry):
            uppers, lowers = carry
            ups = [split(u) for u in uppers]
            lows = [split(l) for l in lowers]
            mids = [split(middle_of(product(as_lhs(l), as_rhs(u)))) for l, u in zip(lows, ups)]
            return (
                [product(as_lhs(u), as_rhs(m)) for u, m in zip(ups, mids)],
                [product(as_lhs(m), as_rhs(l)) for m, l in zip(mids, lows)],
            )

        uppers, lowers = lax.fori_loop(0, NSI - 2, repeat, (uppers, lowers))
        ups = [split(u) for u in uppers]
        lows = [split(l) for l in lowers]
        mids = [split(middle_of(product(as_lhs(l), as_rhs(u)))) for l, u in zip(lows, ups)]
        return [
            product(as_lhs(m), as_rhs(l)) / jnp.sqrt(norm)
            for m, l, norm in zip(mids, lows, norms)
        ]

    def with_itself(x, dim):
        return lax.dot_general(x, x, (((dim,), (dim,)), ((), ())), preferred_element_type=f32)

    grams = []
    for i in range(owned):
        bond = bond_v[i]
        for repeat in range(NAPP):
            half = jnp.dot(nxt[i], bond, preferred_element_type=f32).astype(bf16)
            bond = (
                jnp.dot(half, rgt[i], preferred_element_type=f32) + bond_add[0] * bond.astype(f32)
            ).astype(bf16)
        bond_v[i] = bond
        grams.append(with_itself(bond, 0))
    for i, root in enumerate(inverse_roots(grams)):
        turned = bond_v[i].T
        unit_s[i] = jnp.dot(
            as_lhs(split(root)), jnp.concatenate([turned, turned], axis=0), preferred_element_type=f32
        )
    unit_copy = pltpu.make_async_remote_copy(
        src_ref=unit_s, dst_ref=unit_r, send_sem=usem.at[0], recv_sem=usem.at[1],
        device_id=(lax.rem(site + 1, sites), sec), device_id_type=MESH)
    unit_copy.start()

    @pl.when(role == 1)
    def _():
        for copy in cur_copies:
            copy.wait_recv()

    scale_cur = scale_of(hold, steps + role)
    for i in range(owned):
        lefts = [scaled(hold[steps + role, tab[0, s, own_at + i]], scale_cur) for s in range(phys)]
        nows = [site_v[s, i] for s in range(phys)]
        for repeat in range(NAPP):
            halves = jnp.concatenate(
                [jnp.dot(l, x, preferred_element_type=f32).astype(bf16) for l, x in zip(lefts, nows)],
                axis=0,
            )
            done = jnp.dot(halves, rgt[i], preferred_element_type=f32)
            nows = [
                (done[s * width : (s + 1) * width] + energy[s] * nows[s].astype(f32)).astype(bf16)
                for s in range(phys)
            ]
        for s in range(phys):
            site_v[s, i] = nows[s]
            outer[s, i] = with_itself(nows[s], 1)

    def pack(d, carry):
        sums = []
        for n in range(owned):
            total = jnp.zeros((width, width), f32)
            for s in range(phys):
                at = tab[1, s, d * owned + n] - own_at
                mine = jnp.logical_and(at >= 0, at < owned)
                block = outer[s, jnp.clip(at, 0, owned - 1)]
                total = total + jnp.where(mine, block, 0.0)
            sums.append(total)
        gram_s[d, :width] = jnp.where(cols_at >= rows_at, sums[0], sums[1])
        line = jnp.sum(jnp.where(diagonal, sums[1], 0.0), axis=0, keepdims=True)
        gram_s[d, width:] = jnp.broadcast_to(line, (8, width))
        return carry

    lax.fori_loop(0, secs, pack, 0)
    gram_copies = []
    for n, (dy, e) in enumerate(others):
        to, _ = sec_of(dy, e)
        gram_copies.append(pltpu.make_async_remote_copy(
            src_ref=gram_s.at[to], dst_ref=gram_r.at[n], send_sem=osend.at[n], recv_sem=orecv.at[n],
            device_id=(site, to), device_id_type=MESH))
        gram_copies[-1].start()

    stacks = [jnp.concatenate([site_v[s, i] for s in range(phys)], axis=0) for i in range(owned)]
    roots = inverse_roots([with_itself(stack, 0) for stack in stacks])
    for i in range(owned):
        factor = product(as_lhs(split(roots[i])), as_rhs(split(unit_s[i]))).astype(bf16)
        stack = jnp.concatenate([site_v[s, i] for s in range(phys)], axis=0)
        fresh_left = jnp.dot(stack, factor, preferred_element_type=f32).astype(bf16)
        for s in range(phys):
            left_out[s, i] = fresh_left[s * width : (s + 1) * width]

    for copy in gram_copies:
        copy.wait_recv()
    total = gram_s[sec]
    for n in range(len(others)):
        total = total + gram_r[n]
    packed, line = total[:width], total[width : width + 1]
    flipped = packed.T
    grams = [
        jnp.where(cols_at >= rows_at, packed, flipped),
        jnp.where(diagonal, line, jnp.where(rows_at > cols_at, packed, flipped)),
    ]
    roots = inverse_roots(grams)
    unit_copy.wait_recv()
    for i in range(owned):
        fac_s[i] = product(as_lhs(split(unit_r[i])), as_rhs(split(roots[i]))).astype(bf16)
    fac_copies = []
    for n, (dy, e) in enumerate(others):
        to, _ = sec_of(dy, e)
        fac_copies.append(pltpu.make_async_remote_copy(
            src_ref=fac_s, dst_ref=fac.at[place], send_sem=fsend.at[n], recv_sem=frecv.at[n],
            device_id=(site, to), device_id_type=MESH))
        fac_copies[-1].start()
    for i in range(owned):
        fac[own_at + i] = fac_s[i]
    for copy in fac_copies:
        copy.wait_recv()
    for i in range(owned):
        for s in range(phys):
            right_out[s, i] = jnp.dot(
                fac[tab[0, s, own_at + i]], site_v[s, i], preferred_element_type=f32
            ).astype(bf16)

    for copy in sent + gram_copies + fac_copies + [swap, unit_copy]:
        copy.wait_send()

    @pl.when(role == 0)
    def _():
        for copy in cur_copies:
            copy.wait_send()

    def drain(t, carry):
        for c in range(CHUNKS):
            chunk_copy(t, c).wait_send()
        return carry

    lax.fori_loop(0, steps, drain, 0)


def update(tables, energy, bond_add, canon_l, canon_r, seed_l, seed_r, site, bond):
    sites, secs = lax.axis_size("site"), lax.axis_size("sec")
    steps = sites // 4
    phys, owned, width = canon_l.shape[:3]
    sectors = owned * secs
    bf16, f32 = jnp.bfloat16, jnp.float32
    block = (width, width)
    dma = pltpu.SemaphoreType.DMA
    smem = pl.BlockSpec(memory_space=pltpu.SMEM)
    vmem = pl.BlockSpec(memory_space=pltpu.VMEM)
    hbm = pl.BlockSpec(memory_space=pl.ANY)
    mail = pltpu.VMEM((secs, width + 8, width), f32)
    return pl.pallas_call(
        functools.partial(update_kernel, sites, secs, steps),
        out_shape=(
            jax.ShapeDtypeStruct((phys, owned, *block), bf16),
            jax.ShapeDtypeStruct((phys, owned, *block), bf16),
        ),
        in_specs=[smem, smem, smem, hbm, hbm, vmem, vmem, hbm, hbm],
        out_specs=(vmem, vmem),
        scratch_shapes=[
            pltpu.VMEM((2, phys, owned, *block), bf16),
            pltpu.VMEM((2, owned, *block), bf16),
            pltpu.VMEM((phys, sectors, *block), bf16),
            pltpu.VMEM((2, sectors, width, phys * width), bf16),
            pltpu.VMEM((steps + 2, sectors, *block), bf16),
            pltpu.VMEM((steps, sectors, *block), bf16),
            pltpu.VMEM((sectors, phys, *block), bf16),
            pltpu.VMEM((owned, *block), bf16),
            pltpu.VMEM((owned, *block), bf16),
            pltpu.VMEM((owned, *block), bf16),
            pltpu.VMEM((owned, *block), bf16),
            pltpu.VMEM((phys, owned, *block), bf16),
            pltpu.VMEM((owned, *block), bf16),
            pltpu.VMEM((phys, owned, *block), f32),
            mail, mail,
            pltpu.VMEM((owned, *block), f32),
            pltpu.VMEM((owned, *block), f32),
            pltpu.VMEM((owned, *block), bf16),
            pltpu.VMEM((sectors, *block), bf16),
            dma((4,)), dma((secs - 1,)), dma((secs - 1,)), dma((secs - 1,)), dma((secs - 1,)),
            dma((steps, CHUNKS)), dma((steps, CHUNKS)), dma((CHUNKS + 1,)), dma((CHUNKS + 1,)),
            dma((2,)), dma((secs - 1,)), dma((secs - 1,)), dma((secs - 1,)), dma((secs - 1,)),
        ],
        compiler_params=pltpu.CompilerParams(
            collective_id=0, has_side_effects=True, vmem_limit_bytes=56 * 1024 * 1024
        ),
        name="environments",
    )(tables, energy, bond_add, canon_l, canon_r, seed_l, seed_r, site, bond)


def per_device(
    left_canon,
    right_canon,
    center_site,
    center_bond,
    left_seed,
    right_seed,
    left_sector,
    onsite,
    bond_shift,
):
    sources = left_sector[0]
    labels = jnp.arange(sources.shape[1], dtype=jnp.int32)
    right_of = jnp.sum(
        jnp.where(sources[:, :, None] == labels[None, None, :], labels[None, :, None], 0), axis=1
    )
    left_new, right_new = update(
        jnp.stack([sources, right_of]), onsite[0], bond_shift, left_canon[0], right_canon[0],
        left_seed[0], right_seed[0], center_site[0], center_bond[0],
    )
    return (left_new[None], right_new[None])


def solution(mesh):
    return jax.shard_map(
        per_device,
        mesh=mesh,
        in_specs=(
            P("site", None, "sec", None, None),
            P("site", None, "sec", None, None),
            P("site", None, "sec", None, None),
            P("site", "sec", None, None),
            P("site", "sec", None, None),
            P("site", "sec", None, None),
            P("site", None, None),
            P("site", None),
            P("site"),
        ),
        out_specs=(P("site", None, "sec", None, None), P("site", None, "sec", None, None)),
        check_vma=False,
    )
```

```python
import functools

import jax
import jax.numpy as jnp
from jax import lax
from jax.experimental import pallas as pl
from jax.experimental.pallas import tpu as pltpu
from jax.sharding import PartitionSpec as P

NSI = 10
NAPP = 2
CHUNKS = (3, 3, 4, 3, 3)
MESH = pl.DeviceIdType.MESH


def update_kernel(
    sites, secs, steps,
    tab, energy, bond_add, canon_l, canon_r, seed_l, seed_r, site_in, bond_in,
    left_out, right_out,
    own_c, own_s, tall, wab, hold, fresh, pbuf, give_n, got_n, give_r, got_r, nxt, rgt, site_v, bond_v,
    outer, gram_s, gram_r, unit_s, unit_r, fac_s, fac,
    loc_sem, gsend, grecv, ssend, srecv, tsend, trecv, xsend, xrecv,
    usem, osend, orecv, fsend, frecv, psend, rsend, rrecv,
):
    site, sec = lax.axis_index("site"), lax.axis_index("sec")
    role = lax.rem(sec, 2)
    row = sec // 2
    rows = secs // 2
    phys, owned, width = canon_l.shape[0], canon_l.shape[1], canon_l.shape[2]
    sectors = secs * owned
    target = lax.rem(site + 1 - 2 * role + sites, sites)
    source = lax.rem(site - 1 + 2 * role + sites, sites)
    peer_sec = row * 2 + 1 - role
    half = lax.rem(row, 2)
    pair_sec = sec + 2 - 4 * half
    far_target = lax.rem(site, 2) != role
    far_source = lax.rem(site, 2) == role
    ends = sectors - CHUNKS[0] - CHUNKS[1]
    starts = (
        half * ends, half * ends + CHUNKS[0], CHUNKS[0] + CHUNKS[1],
        (1 - half) * ends, (1 - half) * ends + CHUNKS[0],
    )
    last = steps - 1

    loads = [
        pltpu.make_async_copy(canon_l, own_c.at[0], loc_sem.at[0]),
        pltpu.make_async_copy(canon_r, own_c.at[1], loc_sem.at[1]),
    ]
    center = [
        pltpu.make_async_copy(site_in, site_v, loc_sem.at[2]),
        pltpu.make_async_copy(bond_in, bond_v, loc_sem.at[3]),
    ]
    for load in loads + center:
        load.start()
    for i in range(owned):
        own_s[0, i] = seed_l[i]
        own_s[1, i] = seed_r[i].T

    barrier = pltpu.get_barrier_semaphore()
    others = [(dy, e) for dy in range(rows) for e in range(2) if (dy, e) != (0, 0)]

    def sec_of(dy, e):
        other_role = role + e - 2 * role * e
        return lax.rem(row + dy, rows) * 2 + other_role, other_role

    for dy, e in others:
        pl.semaphore_signal(barrier, inc=1, device_id=(site, sec_of(dy, e)[0]), device_id_type=MESH)
    for other in (target, source):
        pl.semaphore_signal(barrier, inc=1, device_id=(other, sec), device_id_type=MESH)
    across = lax.rem(site + 1 - 2 * role + sites, sites)
    pl.semaphore_signal(barrier, inc=1, device_id=(across, peer_sec), device_id_type=MESH)
    pl.semaphore_wait(barrier, len(others) + 3)

    place = pl.ds(sec * owned, owned)
    sent = []
    for n, (dy, e) in enumerate(others):
        to, to_role = sec_of(dy, e)
        sent.append(pltpu.make_async_remote_copy(
            src_ref=own_s.at[to_role], dst_ref=hold.at[0, place],
            send_sem=ssend.at[n], recv_sem=srecv.at[n],
            device_id=(site, to), device_id_type=MESH))
        sent[-1].start()
    for load in loads:
        load.wait()
    keep = [
        pltpu.make_async_copy(own_c.at[role], tall.at[:, place], loc_sem.at[0]),
        pltpu.make_async_copy(own_s.at[role], hold.at[0, place], loc_sem.at[1]),
    ]
    for n, (dy, e) in enumerate(others):
        to, to_role = sec_of(dy, e)
        sent.append(pltpu.make_async_remote_copy(
            src_ref=own_c.at[to_role], dst_ref=tall.at[:, place],
            send_sem=gsend.at[n], recv_sem=grecv.at[n],
            device_id=(site, to), device_id_type=MESH))
        sent[-1].start()
    for copy in keep:
        copy.start()
    for copy in keep:
        copy.wait()
    for copy in sent:
        copy.wait_recv()

    def arrange(i, carry):
        for s in range(phys):
            cols = slice(s * width, (s + 1) * width)
            wab[role, i, :, cols] = tall[s, tab[1, s, i]]
            wab[1 - role, i, :, cols] = tall[s, i].T
        return carry

    lax.fori_loop(0, sectors, arrange, 0)

    def chunk_copy(t, c):
        part = pl.ds(starts[c], CHUNKS[c])
        return pltpu.make_async_remote_copy(
            src_ref=fresh.at[t, part], dst_ref=hold.at[t + 1, part],
            send_sem=tsend.at[t, c], recv_sem=trecv.at[t, c],
            device_id=(target, sec), device_id_type=MESH)

    def pair_copy(t, c):
        part = pl.ds(starts[c], CHUNKS[c])
        return pltpu.make_async_remote_copy(
            src_ref=hold.at[t + 1, part], dst_ref=hold.at[t + 1, part],
            send_sem=psend.at[t, c], recv_sem=trecv.at[t, c + 3],
            device_id=(site, pair_sec), device_id_type=MESH)

    def arrive(t, c):
        chunk_copy(t, c).wait_recv()
        if c < 2:
            @pl.when(far_source)
            def _():
                pair_copy(t, c).start()

    def first_half(t):
        for c, length in enumerate(CHUNKS):
            @pl.when(t > 0)
            def _():
                arrive(t - 1, c)

            for i in range(length):
                at = starts[c] + i
                product = jnp.dot(
                    hold[t, at], wab[0, at], preferred_element_type=jnp.float32
                ).astype(jnp.bfloat16)
                for s in range(phys):
                    pbuf[at, s] = product[:, s * width : (s + 1) * width]

    def second_half(t, send):
        for c, length in enumerate(CHUNKS):
            for i in range(length):
                at = starts[c] + i
                stack = jnp.concatenate([pbuf[tab[role, s, at], s] for s in range(phys)], axis=0)
                fresh[t, at] = jnp.dot(
                    wab[1, at], stack, preferred_element_type=jnp.float32
                ).astype(jnp.bfloat16)
            send(t, c)

    def send_on(t, c):
        if c < 3:
            chunk_copy(t, c).start()
        else:
            @pl.when(jnp.logical_not(far_target))
            def _():
                chunk_copy(t, c).start()

    def send_left(t, c):
        @pl.when(role == 0)
        def _():
            send_on(t, c)

    def turn(t, carry):
        first_half(t)
        second_half(t, send_on)
        return carry

    lax.fori_loop(0, last, turn, 0)
    first_half(last)
    second_half(last, send_left)
    for load in center:
        load.wait()

    rows_at = lax.broadcasted_iota(jnp.int32, (width, width), 0)
    cols_at = lax.broadcasted_iota(jnp.int32, (width, width), 1)
    diagonal = rows_at == cols_at
    own_at = sec * owned
    peer_at = peer_sec * owned
    f32, bf16 = jnp.float32, jnp.bfloat16

    def scale_of(ref, t):
        total = ref[t, 0].astype(f32)
        for i in range(1, sectors):
            total = total + ref[t, i].astype(f32)
        return (sectors * width) / jnp.sum(jnp.where(diagonal, total, 0.0))

    def scaled(block, scale):
        return (block.astype(f32) * scale).astype(bf16)

    cur_copies = [pltpu.make_async_remote_copy(
        src_ref=hold.at[steps, pl.ds(starts[c], CHUNKS[c])],
        dst_ref=hold.at[steps + 1, pl.ds(starts[c], CHUNKS[c])],
        send_sem=xsend.at[c], recv_sem=xrecv.at[c],
        device_id=(site, peer_sec), device_id_type=MESH) for c in range(len(CHUNKS))]
    nxt_copy = pltpu.make_async_remote_copy(
        src_ref=give_n, dst_ref=got_n,
        send_sem=xsend.at[len(CHUNKS)], recv_sem=xrecv.at[len(CHUNKS)],
        device_id=(site, peer_sec), device_id_type=MESH)
    rgt_copies = [pltpu.make_async_remote_copy(
        src_ref=give_r.at[n], dst_ref=got_r,
        send_sem=rsend.at[n], recv_sem=rrecv.at[0],
        device_id=(target, to), device_id_type=MESH) for n, to in enumerate((peer_sec, sec))]

    @pl.when(role == 0)
    def _():
        scale_next = scale_of(fresh, last)
        for i in range(owned):
            give_n[i] = scaled(fresh[last, peer_at + i], scale_next)
        nxt_copy.start()
        for i in range(owned):
            nxt[i] = scaled(fresh[last, own_at + i], scale_next)
        for c in range(len(CHUNKS)):
            arrive(last, c)
            cur_copies[c].start()

    @pl.when(role == 1)
    def _():
        scale_right = scale_of(fresh, last)
        for n, start in enumerate((peer_at, own_at)):
            for i in range(owned):
                give_r[n, i] = scaled(fresh[last, start + i], scale_right)
            rgt_copies[n].start()
        nxt_copy.wait_recv()
        for i in range(owned):
            nxt[i] = got_n[i]

    rgt_copies[0].wait_recv()
    for i in range(owned):
        rgt[i] = got_r[i].T

    def split(x):
        high = x.astype(bf16)
        return high, (x - high.astype(f32)).astype(bf16)

    def as_lhs(parts):
        return jnp.concatenate(parts, axis=1)

    def as_rhs(parts):
        wide = jnp.concatenate(parts, axis=1)
        return jnp.concatenate([wide, wide], axis=0)

    def product(lhs, rhs):
        both = jnp.dot(lhs, rhs, preferred_element_type=f32)
        return both[:, :width] + both[:, width:]

    def middle_of(part):
        return jnp.where(diagonal, 1.5, 0.0) - 0.5 * part

    def inverse_roots(grams):
        norms = [jnp.sqrt(jnp.sum(g * g, keepdims=True)) for g in grams]
        uppers, lowers = [], []
        for g, norm in zip(grams, norms):
            start = g / norm
            middle = middle_of(start)
            uppers.append(product(as_lhs(split(start)), as_rhs(split(middle))))
            lowers.append(middle)

        def repeat(n, carry):
            uppers, lowers = carry
            ups = [split(u) for u in uppers]
            lows = [split(l) for l in lowers]
            mids = [split(middle_of(product(as_lhs(l), as_rhs(u)))) for l, u in zip(lows, ups)]
            return (
                [product(as_lhs(u), as_rhs(m)) for u, m in zip(ups, mids)],
                [product(as_lhs(m), as_rhs(l)) for m, l in zip(mids, lows)],
            )

        uppers, lowers = lax.fori_loop(0, NSI - 2, repeat, (uppers, lowers))
        ups = [split(u) for u in uppers]
        lows = [split(l) for l in lowers]
        mids = [split(middle_of(product(as_lhs(l), as_rhs(u)))) for l, u in zip(lows, ups)]
        return [
            product(as_lhs(m), as_rhs(l)) / jnp.sqrt(norm)
            for m, l, norm in zip(mids, lows, norms)
        ]

    def with_itself(x, dim):
        return lax.dot_general(x, x, (((dim,), (dim,)), ((), ())), preferred_element_type=f32)

    grams = []
    for i in range(owned):
        bond = bond_v[i]
        for repeat in range(NAPP):
            half = jnp.dot(nxt[i], bond, preferred_element_type=f32).astype(bf16)
            bond = (
                jnp.dot(half, rgt[i], preferred_element_type=f32) + bond_add[0] * bond.astype(f32)
            ).astype(bf16)
        bond_v[i] = bond
        grams.append(with_itself(bond, 0))
    for i, root in enumerate(inverse_roots(grams)):
        turned = bond_v[i].T
        unit_s[i] = jnp.dot(
            as_lhs(split(root)), jnp.concatenate([turned, turned], axis=0), preferred_element_type=f32
        )
    unit_copy = pltpu.make_async_remote_copy(
        src_ref=unit_s, dst_ref=unit_r, send_sem=usem.at[0], recv_sem=usem.at[1],
        device_id=(lax.rem(site + 1, sites), sec), device_id_type=MESH)
    unit_copy.start()

    @pl.when(role == 1)
    def _():
        for copy in cur_copies:
            copy.wait_recv()

    scale_cur = scale_of(hold, steps + role)
    for i in range(owned):
        lefts = [scaled(hold[steps + role, tab[0, s, own_at + i]], scale_cur) for s in range(phys)]
        nows = [site_v[s, i] for s in range(phys)]
        for repeat in range(NAPP):
            halves = jnp.concatenate(
                [jnp.dot(l, x, preferred_element_type=f32).astype(bf16) for l, x in zip(lefts, nows)],
                axis=0,
            )
            done = jnp.dot(halves, rgt[i], preferred_element_type=f32)
            nows = [
                (done[s * width : (s + 1) * width] + energy[s] * nows[s].astype(f32)).astype(bf16)
                for s in range(phys)
            ]
        for s in range(phys):
            site_v[s, i] = nows[s]
            outer[s, i] = with_itself(nows[s], 1)

    def pack(d, carry):
        sums = []
        for n in range(owned):
            total = jnp.zeros((width, width), f32)
            for s in range(phys):
                at = tab[1, s, d * owned + n] - own_at
                mine = jnp.logical_and(at >= 0, at < owned)
                block = outer[s, jnp.clip(at, 0, owned - 1)]
                total = total + jnp.where(mine, block, 0.0)
            sums.append(total)
        gram_s[d, :width] = jnp.where(cols_at >= rows_at, sums[0], sums[1])
        line = jnp.sum(jnp.where(diagonal, sums[1], 0.0), axis=0, keepdims=True)
        gram_s[d, width:] = jnp.broadcast_to(line, (8, width))
        return carry

    lax.fori_loop(0, secs, pack, 0)
    gram_copies = []
    for n, (dy, e) in enumerate(others):
        to, _ = sec_of(dy, e)
        gram_copies.append(pltpu.make_async_remote_copy(
            src_ref=gram_s.at[to], dst_ref=gram_r.at[n], send_sem=osend.at[n], recv_sem=orecv.at[n],
            device_id=(site, to), device_id_type=MESH))
        gram_copies[-1].start()

    stacks = [jnp.concatenate([site_v[s, i] for s in range(phys)], axis=0) for i in range(owned)]
    roots = inverse_roots([with_itself(stack, 0) for stack in stacks])
    for i in range(owned):
        factor = product(as_lhs(split(roots[i])), as_rhs(split(unit_s[i]))).astype(bf16)
        stack = jnp.concatenate([site_v[s, i] for s in range(phys)], axis=0)
        fresh_left = jnp.dot(stack, factor, preferred_element_type=f32).astype(bf16)
        for s in range(phys):
            left_out[s, i] = fresh_left[s * width : (s + 1) * width]

    for copy in gram_copies:
        copy.wait_recv()
    total = gram_s[sec]
    for n in range(len(others)):
        total = total + gram_r[n]
    packed, line = total[:width], total[width : width + 1]
    flipped = packed.T
    grams = [
        jnp.where(cols_at >= rows_at, packed, flipped),
        jnp.where(diagonal, line, jnp.where(rows_at > cols_at, packed, flipped)),
    ]
    roots = inverse_roots(grams)
    unit_copy.wait_recv()
    for i in range(owned):
        fac_s[i] = product(as_lhs(split(unit_r[i])), as_rhs(split(roots[i]))).astype(bf16)
    fac_copies = []
    for n, (dy, e) in enumerate(others):
        to, _ = sec_of(dy, e)
        fac_copies.append(pltpu.make_async_remote_copy(
            src_ref=fac_s, dst_ref=fac.at[place], send_sem=fsend.at[n], recv_sem=frecv.at[n],
            device_id=(site, to), device_id_type=MESH))
        fac_copies[-1].start()
    for i in range(owned):
        fac[own_at + i] = fac_s[i]
    for copy in fac_copies:
        copy.wait_recv()
    for i in range(owned):
        for s in range(phys):
            right_out[s, i] = jnp.dot(
                fac[tab[0, s, own_at + i]], site_v[s, i], preferred_element_type=f32
            ).astype(bf16)

    for copy in sent + gram_copies + fac_copies + [unit_copy]:
        copy.wait_send()

    def drain(t, carry):
        for c in range(3):
            chunk_copy(t, c).wait_send()

        @pl.when(jnp.logical_not(far_target))
        def _():
            for c in range(3, len(CHUNKS)):
                chunk_copy(t, c).wait_send()

        @pl.when(far_source)
        def _():
            for c in range(2):
                pair_copy(t, c).wait_send()

        return carry

    lax.fori_loop(0, last, drain, 0)

    @pl.when(role == 0)
    def _():
        drain(last, 0)
        nxt_copy.wait_send()
        for copy in cur_copies:
            copy.wait_send()

    @pl.when(role == 1)
    def _():
        for copy in rgt_copies:
            copy.wait_send()


def update(tables, energy, bond_add, canon_l, canon_r, seed_l, seed_r, site, bond):
    sites, secs = lax.axis_size("site"), lax.axis_size("sec")
    steps = sites // 4
    phys, owned, width = canon_l.shape[:3]
    sectors = owned * secs
    bf16, f32 = jnp.bfloat16, jnp.float32
    block = (width, width)
    dma = pltpu.SemaphoreType.DMA
    smem = pl.BlockSpec(memory_space=pltpu.SMEM)
    vmem = pl.BlockSpec(memory_space=pltpu.VMEM)
    hbm = pl.BlockSpec(memory_space=pl.ANY)
    mail = pltpu.VMEM((secs, width + 8, width), f32)
    return pl.pallas_call(
        functools.partial(update_kernel, sites, secs, steps),
        out_shape=(
            jax.ShapeDtypeStruct((phys, owned, *block), bf16),
            jax.ShapeDtypeStruct((phys, owned, *block), bf16),
        ),
        in_specs=[smem, smem, smem, hbm, hbm, vmem, vmem, hbm, hbm],
        out_specs=(vmem, vmem),
        scratch_shapes=[
            pltpu.VMEM((2, phys, owned, *block), bf16),
            pltpu.VMEM((2, owned, *block), bf16),
            pltpu.VMEM((phys, sectors, *block), bf16),
            pltpu.VMEM((2, sectors, width, phys * width), bf16),
            pltpu.VMEM((steps + 2, sectors, *block), bf16),
            pltpu.VMEM((steps, sectors, *block), bf16),
            pltpu.VMEM((sectors, phys, *block), bf16),
            pltpu.VMEM((owned, *block), bf16),
            pltpu.VMEM((owned, *block), bf16),
            pltpu.VMEM((2, owned, *block), bf16),
            pltpu.VMEM((owned, *block), bf16),
            pltpu.VMEM((owned, *block), bf16),
            pltpu.VMEM((owned, *block), bf16),
            pltpu.VMEM((phys, owned, *block), bf16),
            pltpu.VMEM((owned, *block), bf16),
            pltpu.VMEM((phys, owned, *block), f32),
            mail, mail,
            pltpu.VMEM((owned, *block), f32),
            pltpu.VMEM((owned, *block), f32),
            pltpu.VMEM((owned, *block), bf16),
            pltpu.VMEM((sectors, *block), bf16),
            dma((4,)), dma((secs - 1,)), dma((secs - 1,)), dma((secs - 1,)), dma((secs - 1,)),
            dma((steps, len(CHUNKS))), dma((steps, len(CHUNKS))),
            dma((len(CHUNKS) + 1,)), dma((len(CHUNKS) + 1,)),
            dma((2,)), dma((secs - 1,)), dma((secs - 1,)), dma((secs - 1,)), dma((secs - 1,)),
            dma((steps, 2)), dma((2,)), dma((1,)),
        ],
        compiler_params=pltpu.CompilerParams(
            collective_id=0, has_side_effects=True, vmem_limit_bytes=56 * 1024 * 1024
        ),
        name="environments",
    )(tables, energy, bond_add, canon_l, canon_r, seed_l, seed_r, site, bond)


def per_device(
    left_canon,
    right_canon,
    center_site,
    center_bond,
    left_seed,
    right_seed,
    left_sector,
    onsite,
    bond_shift,
):
    sources = left_sector[0]
    labels = jnp.arange(sources.shape[1], dtype=jnp.int32)
    right_of = jnp.sum(
        jnp.where(sources[:, :, None] == labels[None, None, :], labels[None, :, None], 0), axis=1
    )
    left_new, right_new = update(
        jnp.stack([sources, right_of]), onsite[0], bond_shift, left_canon[0], right_canon[0],
        left_seed[0], right_seed[0], center_site[0], center_bond[0],
    )
    return (left_new[None], right_new[None])


def solution(mesh):
    return jax.shard_map(
        per_device,
        mesh=mesh,
        in_specs=(
            P("site", None, "sec", None, None),
            P("site", None, "sec", None, None),
            P("site", None, "sec", None, None),
            P("site", "sec", None, None),
            P("site", "sec", None, None),
            P("site", "sec", None, None),
            P("site", None, None),
            P("site", None),
            P("site"),
        ),
        out_specs=(P("site", None, "sec", None, None), P("site", None, "sec", None, None)),
        check_vma=False,
    )
```

```python
import functools

import jax
import jax.numpy as jnp
from jax import lax
from jax.experimental import pallas as pl
from jax.experimental.pallas import tpu as pltpu
from jax.sharding import PartitionSpec as P

NSI = 10
NAPP = 2
NEAR = (8, 8)
FAR = (3, 5, 5, 3)
MESH = pl.DeviceIdType.MESH


def update_kernel(
    sites, secs, steps,
    tab, energy, bond_add, canon_l, canon_r, seed_l, seed_r, site_in, bond_in,
    left_out, right_out,
    own_c, own_s, tall, wab, hold, fresh, pbuf, give_n, got_n, give_r, got_r, give_c, lefts, nxt, rgt, site_v, bond_v,
    outer, gram_s, gram_r, unit_s, unit_r, fac_s, fac,
    loc_sem, gsend, grecv, ssend, srecv, tsend, trecv, xsend, xrecv,
    usem, osend, orecv, fsend, frecv, psend, rsend, rrecv,
):
    site, sec = lax.axis_index("site"), lax.axis_index("sec")
    role = lax.rem(sec, 2)
    row = sec // 2
    rows = secs // 2
    phys, owned, width = canon_l.shape[0], canon_l.shape[1], canon_l.shape[2]
    sectors = secs * owned
    target = lax.rem(site + 1 - 2 * role + sites, sites)
    source = lax.rem(site - 1 + 2 * role + sites, sites)
    peer_sec = row * 2 + 1 - role
    half = lax.rem(row, 2)
    pair_sec = sec + 2 - 4 * half
    far_target = lax.rem(site, 2) != role
    far_source = lax.rem(site, 2) == role
    ends = sectors - FAR[0]
    far_at = (half * ends, FAR[0], FAR[0] + FAR[1], (1 - half) * ends)
    near_at = (0, NEAR[0])
    last = steps - 1

    loads = [
        pltpu.make_async_copy(canon_l, own_c.at[0], loc_sem.at[0]),
        pltpu.make_async_copy(canon_r, own_c.at[1], loc_sem.at[1]),
    ]
    center = [
        pltpu.make_async_copy(site_in, site_v, loc_sem.at[2]),
        pltpu.make_async_copy(bond_in, bond_v, loc_sem.at[3]),
    ]
    for load in loads + center:
        load.start()
    for i in range(owned):
        own_s[0, i] = seed_l[i]
        own_s[1, i] = seed_r[i].T

    barrier = pltpu.get_barrier_semaphore()
    others = [(dy, e) for dy in range(rows) for e in range(2) if (dy, e) != (0, 0)]

    def sec_of(dy, e):
        other_role = role + e - 2 * role * e
        return lax.rem(row + dy, rows) * 2 + other_role, other_role

    for dy, e in others:
        pl.semaphore_signal(barrier, inc=1, device_id=(site, sec_of(dy, e)[0]), device_id_type=MESH)
    for other in (target, source):
        pl.semaphore_signal(barrier, inc=1, device_id=(other, sec), device_id_type=MESH)
    across = lax.rem(site + 1 - 2 * role + sites, sites)
    pl.semaphore_signal(barrier, inc=1, device_id=(across, peer_sec), device_id_type=MESH)
    pl.semaphore_wait(barrier, len(others) + 3)

    place = pl.ds(sec * owned, owned)
    sent = []
    for n, (dy, e) in enumerate(others):
        to, to_role = sec_of(dy, e)
        sent.append(pltpu.make_async_remote_copy(
            src_ref=own_s.at[to_role], dst_ref=hold.at[0, place],
            send_sem=ssend.at[n], recv_sem=srecv.at[n],
            device_id=(site, to), device_id_type=MESH))
        sent[-1].start()
    for load in loads:
        load.wait()
    keep = [
        pltpu.make_async_copy(own_c.at[role], tall.at[:, place], loc_sem.at[0]),
        pltpu.make_async_copy(own_s.at[role], hold.at[0, place], loc_sem.at[1]),
    ]
    for n, (dy, e) in enumerate(others):
        to, to_role = sec_of(dy, e)
        sent.append(pltpu.make_async_remote_copy(
            src_ref=own_c.at[to_role], dst_ref=tall.at[:, place],
            send_sem=gsend.at[n], recv_sem=grecv.at[n],
            device_id=(site, to), device_id_type=MESH))
        sent[-1].start()
    for copy in keep:
        copy.start()
    for copy in keep:
        copy.wait()
    for copy in sent:
        copy.wait_recv()

    def arrange(i, carry):
        for s in range(phys):
            cols = slice(s * width, (s + 1) * width)
            wab[role, i, :, cols] = tall[s, tab[1, s, i]]
            wab[1 - role, i, :, cols] = tall[s, i].T
        return carry

    lax.fori_loop(0, sectors, arrange, 0)

    def to_target(t, c, part):
        return pltpu.make_async_remote_copy(
            src_ref=fresh.at[t, part], dst_ref=hold.at[t + 1, part],
            send_sem=tsend.at[t, c], recv_sem=trecv.at[t, c],
            device_id=(target, sec), device_id_type=MESH)

    def far_copy(t, c):
        return to_target(t, c, pl.ds(far_at[c], FAR[c]))

    def near_copy(t, c):
        return to_target(t, c, pl.ds(near_at[c], NEAR[c]))

    def pair_copy(t):
        part = pl.ds(far_at[0], FAR[0])
        return pltpu.make_async_remote_copy(
            src_ref=hold.at[t + 1, part], dst_ref=hold.at[t + 1, part],
            send_sem=psend.at[t], recv_sem=trecv.at[t, 3],
            device_id=(site, pair_sec), device_id_type=MESH)

    def apply_right(t, start, length):
        for i in range(length):
            at = start + i
            product = jnp.dot(
                hold[t, at], wab[0, at], preferred_element_type=jnp.float32
            ).astype(jnp.bfloat16)
            for s in range(phys):
                pbuf[at, s] = product[:, s * width : (s + 1) * width]

    def apply_left(t, start, length):
        for i in range(length):
            at = start + i
            stack = jnp.concatenate([pbuf[tab[role, s, at], s] for s in range(phys)], axis=0)
            fresh[t, at] = jnp.dot(
                wab[1, at], stack, preferred_element_type=jnp.float32
            ).astype(jnp.bfloat16)

    def first_half(t):
        came_far = jnp.logical_and(t > 0, far_source)

        @pl.when(came_far)
        def _():
            far_copy(t - 1, 0).wait_recv()
            pair_copy(t - 1).start()
            far_copy(t - 1, 1).wait_recv()
            apply_right(t, far_at[0], FAR[0])
            apply_right(t, far_at[1], FAR[1])
            for c in (2, 3):
                far_copy(t - 1, c).wait_recv()
                apply_right(t, far_at[c], FAR[c])

        @pl.when(jnp.logical_not(came_far))
        def _():
            @pl.when(t > 0)
            def _():
                for c in range(len(NEAR)):
                    near_copy(t - 1, c).wait_recv()

            apply_right(t, 0, sectors)

    def second_half(t, send):
        @pl.when(far_target)
        def _():
            for c in range(3):
                apply_left(t, far_at[c], FAR[c])
                send(far_copy(t, c))
            apply_left(t, far_at[3], FAR[3])

        @pl.when(jnp.logical_not(far_target))
        def _():
            for c in range(len(NEAR)):
                apply_left(t, near_at[c], NEAR[c])
                send(near_copy(t, c))

    def send_left(copy):
        @pl.when(role == 0)
        def _():
            copy.start()

    def turn(t, carry):
        first_half(t)
        second_half(t, lambda copy: copy.start())
        return carry

    lax.fori_loop(0, last, turn, 0)
    first_half(last)
    second_half(last, send_left)
    for load in center:
        load.wait()

    rows_at = lax.broadcasted_iota(jnp.int32, (width, width), 0)
    cols_at = lax.broadcasted_iota(jnp.int32, (width, width), 1)
    diagonal = rows_at == cols_at
    own_at = sec * owned
    peer_at = peer_sec * owned
    f32, bf16 = jnp.float32, jnp.bfloat16

    def scale_of(ref, t):
        total = ref[t, 0].astype(f32)
        for i in range(1, sectors):
            total = total + ref[t, i].astype(f32)
        return (sectors * width) / jnp.sum(jnp.where(diagonal, total, 0.0))

    def scaled(block, scale):
        return (block.astype(f32) * scale).astype(bf16)

    cur_copy = pltpu.make_async_remote_copy(
        src_ref=give_c, dst_ref=lefts, send_sem=xsend.at[0], recv_sem=xrecv.at[0],
        device_id=(site, peer_sec), device_id_type=MESH)
    nxt_copy = pltpu.make_async_remote_copy(
        src_ref=give_n, dst_ref=got_n,
        send_sem=xsend.at[1], recv_sem=xrecv.at[1],
        device_id=(site, peer_sec), device_id_type=MESH)
    rgt_copies = [pltpu.make_async_remote_copy(
        src_ref=give_r.at[n], dst_ref=got_r,
        send_sem=rsend.at[n], recv_sem=rrecv.at[0],
        device_id=(target, to), device_id_type=MESH) for n, to in enumerate((peer_sec, sec))]

    @pl.when(role == 0)
    def _():
        scale_next = scale_of(fresh, last)
        for i in range(owned):
            give_n[i] = scaled(fresh[last, peer_at + i], scale_next)
        nxt_copy.start()
        for i in range(owned):
            nxt[i] = scaled(fresh[last, own_at + i], scale_next)

        @pl.when(far_source)
        def _():
            for c in range(4):
                far_copy(last, c).wait_recv()
                if c == 0:
                    pair_copy(last).start()

        @pl.when(jnp.logical_not(far_source))
        def _():
            for c in range(len(NEAR)):
                near_copy(last, c).wait_recv()

        scale_cur = scale_of(hold, steps)
        for i in range(owned):
            for s in range(phys):
                give_c[s, i] = scaled(hold[steps, tab[0, s, peer_at + i]], scale_cur)
        cur_copy.start()
        for i in range(owned):
            for s in range(phys):
                lefts[s, i] = scaled(hold[steps, tab[0, s, own_at + i]], scale_cur)

    @pl.when(role == 1)
    def _():
        scale_right = scale_of(fresh, last)
        for n, start in enumerate((peer_at, own_at)):
            for i in range(owned):
                give_r[n, i] = scaled(fresh[last, start + i], scale_right)
            rgt_copies[n].start()
        nxt_copy.wait_recv()
        for i in range(owned):
            nxt[i] = got_n[i]

    rgt_copies[0].wait_recv()
    for i in range(owned):
        rgt[i] = got_r[i].T

    def split(x):
        high = x.astype(bf16)
        return high, (x - high.astype(f32)).astype(bf16)

    def as_lhs(parts):
        return jnp.concatenate(parts, axis=1)

    def as_rhs(parts):
        wide = jnp.concatenate(parts, axis=1)
        return jnp.concatenate([wide, wide], axis=0)

    def product(lhs, rhs):
        both = jnp.dot(lhs, rhs, preferred_element_type=f32)
        return both[:, :width] + both[:, width:]

    def middle_of(part):
        return jnp.where(diagonal, 1.5, 0.0) - 0.5 * part

    def inverse_roots(grams):
        norms = [jnp.sqrt(jnp.sum(g * g, keepdims=True)) for g in grams]
        uppers, lowers = [], []
        for g, norm in zip(grams, norms):
            start = g / norm
            middle = middle_of(start)
            uppers.append(product(as_lhs(split(start)), as_rhs(split(middle))))
            lowers.append(middle)

        def repeat(n, carry):
            uppers, lowers = carry
            ups = [split(u) for u in uppers]
            lows = [split(l) for l in lowers]
            mids = [split(middle_of(product(as_lhs(l), as_rhs(u)))) for l, u in zip(lows, ups)]
            return (
                [product(as_lhs(u), as_rhs(m)) for u, m in zip(ups, mids)],
                [product(as_lhs(m), as_rhs(l)) for m, l in zip(mids, lows)],
            )

        uppers, lowers = lax.fori_loop(0, NSI - 2, repeat, (uppers, lowers))
        ups = [split(u) for u in uppers]
        lows = [split(l) for l in lowers]
        mids = [split(middle_of(product(as_lhs(l), as_rhs(u)))) for l, u in zip(lows, ups)]
        return [
            product(as_lhs(m), as_rhs(l)) / jnp.sqrt(norm)
            for m, l, norm in zip(mids, lows, norms)
        ]

    def with_itself(x, dim):
        return lax.dot_general(x, x, (((dim,), (dim,)), ((), ())), preferred_element_type=f32)

    grams = []
    for i in range(owned):
        bond = bond_v[i]
        for repeat in range(NAPP):
            half = jnp.dot(nxt[i], bond, preferred_element_type=f32).astype(bf16)
            bond = (
                jnp.dot(half, rgt[i], preferred_element_type=f32) + bond_add[0] * bond.astype(f32)
            ).astype(bf16)
        bond_v[i] = bond
        grams.append(with_itself(bond, 0))
    for i, root in enumerate(inverse_roots(grams)):
        turned = bond_v[i].T
        unit_s[i] = jnp.dot(
            as_lhs(split(root)), jnp.concatenate([turned, turned], axis=0), preferred_element_type=f32
        )
    unit_copy = pltpu.make_async_remote_copy(
        src_ref=unit_s, dst_ref=unit_r, send_sem=usem.at[0], recv_sem=usem.at[1],
        device_id=(lax.rem(site + 1, sites), sec), device_id_type=MESH)
    unit_copy.start()

    @pl.when(role == 1)
    def _():
        cur_copy.wait_recv()

    for i in range(owned):
        nows = [site_v[s, i] for s in range(phys)]
        for repeat in range(NAPP):
            halves = jnp.concatenate(
                [
                    jnp.dot(lefts[s, i], nows[s], preferred_element_type=f32).astype(bf16)
                    for s in range(phys)
                ],
                axis=0,
            )
            done = jnp.dot(halves, rgt[i], preferred_element_type=f32)
            nows = [
                (done[s * width : (s + 1) * width] + energy[s] * nows[s].astype(f32)).astype(bf16)
                for s in range(phys)
            ]
        for s in range(phys):
            site_v[s, i] = nows[s]
            outer[s, i] = with_itself(nows[s], 1)

    def gram_copy(d):
        return pltpu.make_async_remote_copy(
            src_ref=gram_s.at[d], dst_ref=gram_r.at[sec], send_sem=osend.at[d], recv_sem=orecv.at[sec],
            device_id=(site, d), device_id_type=MESH)

    def pack(n, carry):
        d = lax.rem(sec + 1 + n, secs)
        sums = []
        for i in range(owned):
            total = jnp.zeros((width, width), f32)
            for s in range(phys):
                at = tab[1, s, d * owned + i] - own_at
                mine = jnp.logical_and(at >= 0, at < owned)
                block = outer[s, jnp.clip(at, 0, owned - 1)]
                total = total + jnp.where(mine, block, 0.0)
            sums.append(total)
        gram_s[d, :width] = jnp.where(cols_at >= rows_at, sums[0], sums[1])
        line = jnp.sum(jnp.where(diagonal, sums[1], 0.0), axis=0, keepdims=True)
        gram_s[d, width:] = jnp.broadcast_to(line, (8, width))

        @pl.when(n < secs - 1)
        def _():
            gram_copy(d).start()

        return carry

    lax.fori_loop(0, secs, pack, 0)

    stacks = [jnp.concatenate([site_v[s, i] for s in range(phys)], axis=0) for i in range(owned)]
    roots = inverse_roots([with_itself(stack, 0) for stack in stacks])
    for i in range(owned):
        factor = product(as_lhs(split(roots[i])), as_rhs(split(unit_s[i]))).astype(bf16)
        stack = jnp.concatenate([site_v[s, i] for s in range(phys)], axis=0)
        fresh_left = jnp.dot(stack, factor, preferred_element_type=f32).astype(bf16)
        for s in range(phys):
            left_out[s, i] = fresh_left[s * width : (s + 1) * width]

    def gram_from(d):
        return pltpu.make_async_remote_copy(
            src_ref=gram_s.at[d], dst_ref=gram_r.at[d], send_sem=osend.at[d], recv_sem=orecv.at[d],
            device_id=(site, d), device_id_type=MESH)

    for n in range(secs - 1):
        gram_from(lax.rem(sec + 1 + n, secs)).wait_recv()
    total = gram_s[sec]
    for n in range(secs - 1):
        total = total + gram_r[lax.rem(sec + 1 + n, secs)]
    packed, line = total[:width], total[width : width + 1]
    flipped = packed.T
    grams = [
        jnp.where(cols_at >= rows_at, packed, flipped),
        jnp.where(diagonal, line, jnp.where(rows_at > cols_at, packed, flipped)),
    ]
    roots = inverse_roots(grams)
    unit_copy.wait_recv()
    for i in range(owned):
        fac_s[i] = product(as_lhs(split(unit_r[i])), as_rhs(split(roots[i]))).astype(bf16)
    fac_copies = []
    for n, (dy, e) in enumerate(others):
        to, _ = sec_of(dy, e)
        fac_copies.append(pltpu.make_async_remote_copy(
            src_ref=fac_s, dst_ref=fac.at[place], send_sem=fsend.at[n], recv_sem=frecv.at[n],
            device_id=(site, to), device_id_type=MESH))
        fac_copies[-1].start()
    for i in range(owned):
        fac[own_at + i] = fac_s[i]
    for copy in fac_copies:
        copy.wait_recv()
    for i in range(owned):
        for s in range(phys):
            right_out[s, i] = jnp.dot(
                fac[tab[0, s, own_at + i]], site_v[s, i], preferred_element_type=f32
            ).astype(bf16)

    for copy in sent + fac_copies + [unit_copy]:
        copy.wait_send()
    for n in range(secs - 1):
        gram_copy(lax.rem(sec + 1 + n, secs)).wait_send()

    def drain(t, carry):
        @pl.when(far_target)
        def _():
            for c in range(3):
                far_copy(t, c).wait_send()

        @pl.when(jnp.logical_not(far_target))
        def _():
            for c in range(len(NEAR)):
                near_copy(t, c).wait_send()

        @pl.when(far_source)
        def _():
            pair_copy(t).wait_send()

        return carry

    lax.fori_loop(0, last, drain, 0)

    @pl.when(role == 0)
    def _():
        drain(last, 0)
        nxt_copy.wait_send()
        cur_copy.wait_send()

    @pl.when(role == 1)
    def _():
        for copy in rgt_copies:
            copy.wait_send()


def update(tables, energy, bond_add, canon_l, canon_r, seed_l, seed_r, site, bond):
    sites, secs = lax.axis_size("site"), lax.axis_size("sec")
    steps = sites // 4
    phys, owned, width = canon_l.shape[:3]
    sectors = owned * secs
    bf16, f32 = jnp.bfloat16, jnp.float32
    block = (width, width)
    dma = pltpu.SemaphoreType.DMA
    smem = pl.BlockSpec(memory_space=pltpu.SMEM)
    vmem = pl.BlockSpec(memory_space=pltpu.VMEM)
    hbm = pl.BlockSpec(memory_space=pl.ANY)
    mail = pltpu.VMEM((secs, width + 8, width), f32)
    return pl.pallas_call(
        functools.partial(update_kernel, sites, secs, steps),
        out_shape=(
            jax.ShapeDtypeStruct((phys, owned, *block), bf16),
            jax.ShapeDtypeStruct((phys, owned, *block), bf16),
        ),
        in_specs=[smem, smem, smem, hbm, hbm, vmem, vmem, hbm, hbm],
        out_specs=(vmem, vmem),
        scratch_shapes=[
            pltpu.VMEM((2, phys, owned, *block), bf16),
            pltpu.VMEM((2, owned, *block), bf16),
            pltpu.VMEM((phys, sectors, *block), bf16),
            pltpu.VMEM((2, sectors, width, phys * width), bf16),
            pltpu.VMEM((steps + 1, sectors, *block), bf16),
            pltpu.VMEM((steps, sectors, *block), bf16),
            pltpu.VMEM((sectors, phys, *block), bf16),
            pltpu.VMEM((owned, *block), bf16),
            pltpu.VMEM((owned, *block), bf16),
            pltpu.VMEM((2, owned, *block), bf16),
            pltpu.VMEM((owned, *block), bf16),
            pltpu.VMEM((phys, owned, *block), bf16),
            pltpu.VMEM((phys, owned, *block), bf16),
            pltpu.VMEM((owned, *block), bf16),
            pltpu.VMEM((owned, *block), bf16),
            pltpu.VMEM((phys, owned, *block), bf16),
            pltpu.VMEM((owned, *block), bf16),
            pltpu.VMEM((phys, owned, *block), f32),
            mail, mail,
            pltpu.VMEM((owned, *block), f32),
            pltpu.VMEM((owned, *block), f32),
            pltpu.VMEM((owned, *block), bf16),
            pltpu.VMEM((sectors, *block), bf16),
            dma((4,)), dma((secs - 1,)), dma((secs - 1,)), dma((secs - 1,)), dma((secs - 1,)),
            dma((steps, 4)), dma((steps, 4)), dma((2,)), dma((2,)),
            dma((2,)), dma((secs,)), dma((secs,)), dma((secs - 1,)), dma((secs - 1,)),
            dma((steps,)), dma((2,)), dma((1,)),
        ],
        compiler_params=pltpu.CompilerParams(
            collective_id=0, has_side_effects=True, vmem_limit_bytes=56 * 1024 * 1024
        ),
        name="environments",
    )(tables, energy, bond_add, canon_l, canon_r, seed_l, seed_r, site, bond)


def per_device(
    left_canon,
    right_canon,
    center_site,
    center_bond,
    left_seed,
    right_seed,
    left_sector,
    onsite,
    bond_shift,
):
    sources = left_sector[0]
    labels = jnp.arange(sources.shape[1], dtype=jnp.int32)
    right_of = jnp.sum(
        jnp.where(sources[:, :, None] == labels[None, None, :], labels[None, :, None], 0), axis=1
    )
    left_new, right_new = update(
        jnp.stack([sources, right_of]), onsite[0], bond_shift, left_canon[0], right_canon[0],
        left_seed[0], right_seed[0], center_site[0], center_bond[0],
    )
    return (left_new[None], right_new[None])


def solution(mesh):
    return jax.shard_map(
        per_device,
        mesh=mesh,
        in_specs=(
            P("site", None, "sec", None, None),
            P("site", None, "sec", None, None),
            P("site", None, "sec", None, None),
            P("site", "sec", None, None),
            P("site", "sec", None, None),
            P("site", "sec", None, None),
            P("site", None, None),
            P("site", None),
            P("site"),
        ),
        out_specs=(P("site", None, "sec", None, None), P("site", None, "sec", None, None)),
        check_vma=False,
    )
```

```python
import functools

import jax
import jax.numpy as jnp
from jax import lax
from jax.experimental import pallas as pl
from jax.experimental.pallas import tpu as pltpu
from jax.sharding import PartitionSpec as P

NSI = 10
NAPP = 2
NEAR = (8, 8)
FAR = (3, 5, 5, 3)
MESH = pl.DeviceIdType.MESH


def update_kernel(
    sites, secs, steps,
    tab, energy, bond_add, canon_l, canon_r, seed_l, seed_r, site_in, bond_in,
    left_out, right_out,
    own_c, tall, wab, hold, fresh, pbuf, give_n, got_n, give_r, got_r, give_c, lefts, nxt, rgt, site_v, bond_v,
    outer, gram_s, gram_r, unit_s, unit_r, fac_s, fac,
    loc_sem, gsend, grecv, tsend, trecv, xsend, xrecv,
    usem, osend, orecv, fsend, frecv, psend, rsend, rrecv,
):
    site, sec = lax.axis_index("site"), lax.axis_index("sec")
    role = lax.rem(sec, 2)
    row = sec // 2
    rows = secs // 2
    phys, owned, width = canon_l.shape[0], canon_l.shape[1], canon_l.shape[2]
    sectors = secs * owned
    target = lax.rem(site + 1 - 2 * role + sites, sites)
    source = lax.rem(site - 1 + 2 * role + sites, sites)
    peer_sec = row * 2 + 1 - role
    half = lax.rem(row, 2)
    pair_sec = sec + 2 - 4 * half
    far_target = lax.rem(site, 2) != role
    far_source = lax.rem(site, 2) == role
    ends = sectors - FAR[0]
    far_at = (half * ends, FAR[0], FAR[0] + FAR[1], (1 - half) * ends)
    near_at = (0, NEAR[0])
    last = steps - 1

    loads = [
        pltpu.make_async_copy(canon_l, own_c.at[0, pl.ds(1, phys)], loc_sem.at[0]),
        pltpu.make_async_copy(canon_r, own_c.at[1, pl.ds(1, phys)], loc_sem.at[1]),
    ]
    center = [
        pltpu.make_async_copy(site_in, site_v, loc_sem.at[2]),
        pltpu.make_async_copy(bond_in, bond_v, loc_sem.at[3]),
    ]
    for load in loads + center:
        load.start()
    for i in range(owned):
        own_c[0, 0, i] = seed_l[i]
        own_c[1, 0, i] = seed_r[i].T

    barrier = pltpu.get_barrier_semaphore()
    others = [(dy, e) for dy in range(rows) for e in range(2) if (dy, e) != (0, 0)]

    def sec_of(dy, e):
        other_role = role + e - 2 * role * e
        return lax.rem(row + dy, rows) * 2 + other_role, other_role

    for dy, e in others:
        pl.semaphore_signal(barrier, inc=1, device_id=(site, sec_of(dy, e)[0]), device_id_type=MESH)
    for other in (target, source):
        pl.semaphore_signal(barrier, inc=1, device_id=(other, sec), device_id_type=MESH)
    across = lax.rem(site + 1 - 2 * role + sites, sites)
    pl.semaphore_signal(barrier, inc=1, device_id=(across, peer_sec), device_id_type=MESH)
    pl.semaphore_wait(barrier, len(others) + 3)

    place = pl.ds(sec * owned, owned)
    peer_place = pl.ds(peer_sec * owned, owned)
    parts = (pl.ds(0, 3), pl.ds(3, phys - 2))
    up_row, down_row = lax.rem(row + 1, rows), lax.rem(row + rows - 1, rows)
    up, down = up_row * 2 + role, down_row * 2 + role
    sent = []

    def gather_copy(n, src, part, at, to, slot):
        return pltpu.make_async_remote_copy(
            src_ref=src, dst_ref=tall.at[part, at], send_sem=gsend.at[n], recv_sem=grecv.at[slot],
            device_id=(site, to), device_id_type=MESH)

    def give_on(src, part, at, to, slot):
        sent.append(gather_copy(len(sent), src, part, at, to, slot))
        sent[-1].start()

    def landed(part, at, slot):
        gather_copy(0, tall.at[part, at], part, at, up, slot).wait_recv()

    for load in loads:
        load.wait()
    for h in range(2):
        give_on(own_c.at[1 - role, parts[h]], parts[h], place, peer_sec, h)
    for h in range(2):
        give_on(own_c.at[role, parts[h]], parts[h], place, up, 2 + h)
        give_on(own_c.at[role, parts[1 - h]], parts[1 - h], place, down, 9 - h)
    keep = pltpu.make_async_copy(own_c.at[role], tall.at[:, place], loc_sem.at[0])
    keep.start()

    def block_at(of_row, of_peer):
        return pl.ds((of_row * 2 + (1 - role if of_peer else role)) * owned, owned)

    for h in range(2):
        landed(parts[h], peer_place, h)
        give_on(tall.at[parts[h], peer_place], parts[h], peer_place, up, 4 + h)
        give_on(tall.at[parts[h], peer_place], parts[h], peer_place, down, 10 + h)
        at = block_at(down_row, h)
        landed(parts[0], at, 2 + 2 * h)
        give_on(tall.at[parts[0], at], parts[0], at, up, 6 + h)
        at = block_at(up_row, h)
        landed(parts[1], at, 9 + 2 * h)
        give_on(tall.at[parts[1], at], parts[1], at, down, 12 + h)
    keep.wait()
    far_row = lax.rem(row + 2, rows)
    for h in range(2):
        landed(parts[1], block_at(down_row, h), 3 + 2 * h)
        landed(parts[0], block_at(up_row, h), 8 + 2 * h)
        landed(parts[0], block_at(far_row, h), 6 + h)
        landed(parts[1], block_at(far_row, h), 12 + h)

    def arrange(i, carry):
        hold[0, i] = tall[0, i]
        for s in range(phys):
            cols = slice(s * width, (s + 1) * width)
            wab[role, i, :, cols] = tall[1 + s, tab[1, s, i]]
            wab[1 - role, i, :, cols] = tall[1 + s, i].T
        return carry

    lax.fori_loop(0, sectors, arrange, 0)

    def to_target(t, c, part):
        return pltpu.make_async_remote_copy(
            src_ref=fresh.at[t, part], dst_ref=hold.at[t + 1, part],
            send_sem=tsend.at[t, c], recv_sem=trecv.at[t, c],
            device_id=(target, sec), device_id_type=MESH)

    def far_copy(t, c):
        return to_target(t, c, pl.ds(far_at[c], FAR[c]))

    def near_copy(t, c):
        return to_target(t, c, pl.ds(near_at[c], NEAR[c]))

    def pair_copy(t):
        part = pl.ds(far_at[0], FAR[0])
        return pltpu.make_async_remote_copy(
            src_ref=hold.at[t + 1, part], dst_ref=hold.at[t + 1, part],
            send_sem=psend.at[t], recv_sem=trecv.at[t, 3],
            device_id=(site, pair_sec), device_id_type=MESH)

    def apply_right(t, start, length):
        for i in range(length):
            at = start + i
            product = jnp.dot(
                hold[t, at], wab[0, at], preferred_element_type=jnp.float32
            ).astype(jnp.bfloat16)
            for s in range(phys):
                pbuf[at, s] = product[:, s * width : (s + 1) * width]

    def apply_left(t, start, length):
        for i in range(length):
            at = start + i
            stack = jnp.concatenate([pbuf[tab[role, s, at], s] for s in range(phys)], axis=0)
            fresh[t, at] = jnp.dot(
                wab[1, at], stack, preferred_element_type=jnp.float32
            ).astype(jnp.bfloat16)

    def first_half(t):
        came_far = jnp.logical_and(t > 0, far_source)

        @pl.when(came_far)
        def _():
            far_copy(t - 1, 0).wait_recv()
            pair_copy(t - 1).start()
            far_copy(t - 1, 1).wait_recv()
            apply_right(t, far_at[0], FAR[0])
            apply_right(t, far_at[1], FAR[1])
            for c in (2, 3):
                far_copy(t - 1, c).wait_recv()
                apply_right(t, far_at[c], FAR[c])

        @pl.when(jnp.logical_not(came_far))
        def _():
            @pl.when(t > 0)
            def _():
                for c in range(len(NEAR)):
                    near_copy(t - 1, c).wait_recv()

            apply_right(t, 0, sectors)

    def second_half(t, send):
        @pl.when(far_target)
        def _():
            for c in range(3):
                apply_left(t, far_at[c], FAR[c])
                send(far_copy(t, c))
            apply_left(t, far_at[3], FAR[3])

        @pl.when(jnp.logical_not(far_target))
        def _():
            for c in range(len(NEAR)):
                apply_left(t, near_at[c], NEAR[c])
                send(near_copy(t, c))

    def send_left(copy):
        @pl.when(role == 0)
        def _():
            copy.start()

    def turn(t, carry):
        first_half(t)
        second_half(t, lambda copy: copy.start())
        return carry

    lax.fori_loop(0, last, turn, 0)
    first_half(last)
    second_half(last, send_left)
    for load in center:
        load.wait()

    rows_at = lax.broadcasted_iota(jnp.int32, (width, width), 0)
    cols_at = lax.broadcasted_iota(jnp.int32, (width, width), 1)
    diagonal = rows_at == cols_at
    own_at = sec * owned
    peer_at = peer_sec * owned
    f32, bf16 = jnp.float32, jnp.bfloat16

    def scale_of(ref, t):
        total = ref[t, 0].astype(f32)
        for i in range(1, sectors):
            total = total + ref[t, i].astype(f32)
        return (sectors * width) / jnp.sum(jnp.where(diagonal, total, 0.0))

    def scaled(block, scale):
        return (block.astype(f32) * scale).astype(bf16)

    cur_copy = pltpu.make_async_remote_copy(
        src_ref=give_c, dst_ref=lefts, send_sem=xsend.at[0], recv_sem=xrecv.at[0],
        device_id=(site, peer_sec), device_id_type=MESH)
    nxt_copy = pltpu.make_async_remote_copy(
        src_ref=give_n, dst_ref=got_n,
        send_sem=xsend.at[1], recv_sem=xrecv.at[1],
        device_id=(site, peer_sec), device_id_type=MESH)
    rgt_copies = [pltpu.make_async_remote_copy(
        src_ref=give_r.at[n], dst_ref=got_r,
        send_sem=rsend.at[n], recv_sem=rrecv.at[0],
        device_id=(target, to), device_id_type=MESH) for n, to in enumerate((peer_sec, sec))]

    @pl.when(role == 0)
    def _():
        scale_next = scale_of(fresh, last)
        for i in range(owned):
            give_n[i] = scaled(fresh[last, peer_at + i], scale_next)
        nxt_copy.start()
        for i in range(owned):
            nxt[i] = scaled(fresh[last, own_at + i], scale_next)

        @pl.when(far_source)
        def _():
            for c in range(4):
                far_copy(last, c).wait_recv()
                if c == 0:
                    pair_copy(last).start()

        @pl.when(jnp.logical_not(far_source))
        def _():
            for c in range(len(NEAR)):
                near_copy(last, c).wait_recv()

        scale_cur = scale_of(hold, steps)
        for i in range(owned):
            for s in range(phys):
                give_c[s, i] = scaled(hold[steps, tab[0, s, peer_at + i]], scale_cur)
        cur_copy.start()
        for i in range(owned):
            for s in range(phys):
                lefts[s, i] = scaled(hold[steps, tab[0, s, own_at + i]], scale_cur)

    @pl.when(role == 1)
    def _():
        scale_right = scale_of(fresh, last)
        for n, start in enumerate((peer_at, own_at)):
            for i in range(owned):
                give_r[n, i] = scaled(fresh[last, start + i], scale_right)
            rgt_copies[n].start()
        nxt_copy.wait_recv()
        for i in range(owned):
            nxt[i] = got_n[i]

    rgt_copies[0].wait_recv()
    for i in range(owned):
        rgt[i] = got_r[i].T

    def split(x):
        high = x.astype(bf16)
        return high, (x - high.astype(f32)).astype(bf16)

    def as_lhs(parts):
        return jnp.concatenate(parts, axis=1)

    def as_rhs(parts):
        wide = jnp.concatenate(parts, axis=1)
        return jnp.concatenate([wide, wide], axis=0)

    def product(lhs, rhs):
        both = jnp.dot(lhs, rhs, preferred_element_type=f32)
        return both[:, :width] + both[:, width:]

    def middle_of(part):
        return jnp.where(diagonal, 1.5, 0.0) - 0.5 * part

    def inverse_roots(grams):
        norms = [jnp.sqrt(jnp.sum(g * g, keepdims=True)) for g in grams]
        uppers, lowers = [], []
        for g, norm in zip(grams, norms):
            start = g / norm
            middle = middle_of(start)
            uppers.append(product(as_lhs(split(start)), as_rhs(split(middle))))
            lowers.append(middle)

        def repeat(n, carry):
            uppers, lowers = carry
            ups = [split(u) for u in uppers]
            lows = [split(l) for l in lowers]
            mids = [split(middle_of(product(as_lhs(l), as_rhs(u)))) for l, u in zip(lows, ups)]
            return (
                [product(as_lhs(u), as_rhs(m)) for u, m in zip(ups, mids)],
                [product(as_lhs(m), as_rhs(l)) for m, l in zip(mids, lows)],
            )

        uppers, lowers = lax.fori_loop(0, NSI - 2, repeat, (uppers, lowers))
        ups = [split(u) for u in uppers]
        lows = [split(l) for l in lowers]
        mids = [split(middle_of(product(as_lhs(l), as_rhs(u)))) for l, u in zip(lows, ups)]
        return [
            product(as_lhs(m), as_rhs(l)) / jnp.sqrt(norm)
            for m, l, norm in zip(mids, lows, norms)
        ]

    def with_itself(x, dim):
        return lax.dot_general(x, x, (((dim,), (dim,)), ((), ())), preferred_element_type=f32)

    grams = []
    for i in range(owned):
        bond = bond_v[i]
        for repeat in range(NAPP):
            half = jnp.dot(nxt[i], bond, preferred_element_type=f32).astype(bf16)
            bond = (
                jnp.dot(half, rgt[i], preferred_element_type=f32) + bond_add[0] * bond.astype(f32)
            ).astype(bf16)
        bond_v[i] = bond
        grams.append(with_itself(bond, 0))
    for i, root in enumerate(inverse_roots(grams)):
        turned = bond_v[i].T
        unit_s[i] = jnp.dot(
            as_lhs(split(root)), jnp.concatenate([turned, turned], axis=0), preferred_element_type=f32
        )
    unit_copy = pltpu.make_async_remote_copy(
        src_ref=unit_s, dst_ref=unit_r, send_sem=usem.at[0], recv_sem=usem.at[1],
        device_id=(lax.rem(site + 1, sites), sec), device_id_type=MESH)
    unit_copy.start()

    @pl.when(role == 1)
    def _():
        cur_copy.wait_recv()

    for i in range(owned):
        nows = [site_v[s, i] for s in range(phys)]
        for repeat in range(NAPP):
            halves = jnp.concatenate(
                [
                    jnp.dot(lefts[s, i], nows[s], preferred_element_type=f32).astype(bf16)
                    for s in range(phys)
                ],
                axis=0,
            )
            done = jnp.dot(halves, rgt[i], preferred_element_type=f32)
            nows = [
                (done[s * width : (s + 1) * width] + energy[s] * nows[s].astype(f32)).astype(bf16)
                for s in range(phys)
            ]
        for s in range(phys):
            site_v[s, i] = nows[s]
            outer[s, i] = with_itself(nows[s], 1)

    def gram_copy(d):
        return pltpu.make_async_remote_copy(
            src_ref=gram_s.at[d], dst_ref=gram_r.at[sec], send_sem=osend.at[d], recv_sem=orecv.at[sec],
            device_id=(site, d), device_id_type=MESH)

    def pack(n, carry):
        d = lax.rem(sec + 1 + n, secs)
        sums = []
        for i in range(owned):
            total = jnp.zeros((width, width), f32)
            for s in range(phys):
                at = tab[1, s, d * owned + i] - own_at
                mine = jnp.logical_and(at >= 0, at < owned)
                block = outer[s, jnp.clip(at, 0, owned - 1)]
                total = total + jnp.where(mine, block, 0.0)
            sums.append(total)
        gram_s[d, :width] = jnp.where(cols_at >= rows_at, sums[0], sums[1])
        line = jnp.sum(jnp.where(diagonal, sums[1], 0.0), axis=0, keepdims=True)
        gram_s[d, width:] = jnp.broadcast_to(line, (8, width))

        @pl.when(n < secs - 1)
        def _():
            gram_copy(d).start()

        return carry

    lax.fori_loop(0, secs, pack, 0)

    stacks = [jnp.concatenate([site_v[s, i] for s in range(phys)], axis=0) for i in range(owned)]
    roots = inverse_roots([with_itself(stack, 0) for stack in stacks])
    for i in range(owned):
        factor = product(as_lhs(split(roots[i])), as_rhs(split(unit_s[i]))).astype(bf16)
        stack = jnp.concatenate([site_v[s, i] for s in range(phys)], axis=0)
        fresh_left = jnp.dot(stack, factor, preferred_element_type=f32).astype(bf16)
        for s in range(phys):
            left_out[s, i] = fresh_left[s * width : (s + 1) * width]

    def gram_from(d):
        return pltpu.make_async_remote_copy(
            src_ref=gram_s.at[d], dst_ref=gram_r.at[d], send_sem=osend.at[d], recv_sem=orecv.at[d],
            device_id=(site, d), device_id_type=MESH)

    for n in range(secs - 1):
        gram_from(lax.rem(sec + 1 + n, secs)).wait_recv()
    total = gram_s[sec]
    for n in range(secs - 1):
        total = total + gram_r[lax.rem(sec + 1 + n, secs)]
    packed, line = total[:width], total[width : width + 1]
    flipped = packed.T
    grams = [
        jnp.where(cols_at >= rows_at, packed, flipped),
        jnp.where(diagonal, line, jnp.where(rows_at > cols_at, packed, flipped)),
    ]
    roots = inverse_roots(grams)
    unit_copy.wait_recv()
    for i in range(owned):
        fac_s[i] = product(as_lhs(split(unit_r[i])), as_rhs(split(roots[i]))).astype(bf16)
    fac_copies = []
    for n, (dy, e) in enumerate(others):
        to, _ = sec_of(dy, e)
        fac_copies.append(pltpu.make_async_remote_copy(
            src_ref=fac_s, dst_ref=fac.at[place], send_sem=fsend.at[n], recv_sem=frecv.at[n],
            device_id=(site, to), device_id_type=MESH))
        fac_copies[-1].start()
    for i in range(owned):
        fac[own_at + i] = fac_s[i]
    for copy in fac_copies:
        copy.wait_recv()
    for i in range(owned):
        for s in range(phys):
            right_out[s, i] = jnp.dot(
                fac[tab[0, s, own_at + i]], site_v[s, i], preferred_element_type=f32
            ).astype(bf16)

    for copy in sent + fac_copies + [unit_copy]:
        copy.wait_send()
    for n in range(secs - 1):
        gram_copy(lax.rem(sec + 1 + n, secs)).wait_send()

    def drain(t, carry):
        @pl.when(far_target)
        def _():
            for c in range(3):
                far_copy(t, c).wait_send()

        @pl.when(jnp.logical_not(far_target))
        def _():
            for c in range(len(NEAR)):
                near_copy(t, c).wait_send()

        @pl.when(far_source)
        def _():
            pair_copy(t).wait_send()

        return carry

    lax.fori_loop(0, last, drain, 0)

    @pl.when(role == 0)
    def _():
        drain(last, 0)
        nxt_copy.wait_send()
        cur_copy.wait_send()

    @pl.when(role == 1)
    def _():
        for copy in rgt_copies:
            copy.wait_send()


def update(tables, energy, bond_add, canon_l, canon_r, seed_l, seed_r, site, bond):
    sites, secs = lax.axis_size("site"), lax.axis_size("sec")
    steps = sites // 4
    phys, owned, width = canon_l.shape[:3]
    sectors = owned * secs
    bf16, f32 = jnp.bfloat16, jnp.float32
    block = (width, width)
    dma = pltpu.SemaphoreType.DMA
    smem = pl.BlockSpec(memory_space=pltpu.SMEM)
    vmem = pl.BlockSpec(memory_space=pltpu.VMEM)
    hbm = pl.BlockSpec(memory_space=pl.ANY)
    mail = pltpu.VMEM((secs, width + 8, width), f32)
    return pl.pallas_call(
        functools.partial(update_kernel, sites, secs, steps),
        out_shape=(
            jax.ShapeDtypeStruct((phys, owned, *block), bf16),
            jax.ShapeDtypeStruct((phys, owned, *block), bf16),
        ),
        in_specs=[smem, smem, smem, hbm, hbm, vmem, vmem, hbm, hbm],
        out_specs=(vmem, vmem),
        scratch_shapes=[
            pltpu.VMEM((2, 1 + phys, owned, *block), bf16),
            pltpu.VMEM((1 + phys, sectors, *block), bf16),
            pltpu.VMEM((2, sectors, width, phys * width), bf16),
            pltpu.VMEM((steps + 1, sectors, *block), bf16),
            pltpu.VMEM((steps, sectors, *block), bf16),
            pltpu.VMEM((sectors, phys, *block), bf16),
            pltpu.VMEM((owned, *block), bf16),
            pltpu.VMEM((owned, *block), bf16),
            pltpu.VMEM((2, owned, *block), bf16),
            pltpu.VMEM((owned, *block), bf16),
            pltpu.VMEM((phys, owned, *block), bf16),
            pltpu.VMEM((phys, owned, *block), bf16),
            pltpu.VMEM((owned, *block), bf16),
            pltpu.VMEM((owned, *block), bf16),
            pltpu.VMEM((phys, owned, *block), bf16),
            pltpu.VMEM((owned, *block), bf16),
            pltpu.VMEM((phys, owned, *block), f32),
            mail, mail,
            pltpu.VMEM((owned, *block), f32),
            pltpu.VMEM((owned, *block), f32),
            pltpu.VMEM((owned, *block), bf16),
            pltpu.VMEM((sectors, *block), bf16),
            dma((4,)), dma((14,)), dma((14,)),
            dma((steps, 4)), dma((steps, 4)), dma((2,)), dma((2,)),
            dma((2,)), dma((secs,)), dma((secs,)), dma((secs - 1,)), dma((secs - 1,)),
            dma((steps,)), dma((2,)), dma((1,)),
        ],
        compiler_params=pltpu.CompilerParams(
            collective_id=0, has_side_effects=True, vmem_limit_bytes=56 * 1024 * 1024
        ),
        name="environments",
    )(tables, energy, bond_add, canon_l, canon_r, seed_l, seed_r, site, bond)


def per_device(
    left_canon,
    right_canon,
    center_site,
    center_bond,
    left_seed,
    right_seed,
    left_sector,
    onsite,
    bond_shift,
):
    sources = left_sector[0]
    labels = jnp.arange(sources.shape[1], dtype=jnp.int32)
    right_of = jnp.sum(
        jnp.where(sources[:, :, None] == labels[None, None, :], labels[None, :, None], 0), axis=1
    )
    left_new, right_new = update(
        jnp.stack([sources, right_of]), onsite[0], bond_shift, left_canon[0], right_canon[0],
        left_seed[0], right_seed[0], center_site[0], center_bond[0],
    )
    return (left_new[None], right_new[None])


def solution(mesh):
    return jax.shard_map(
        per_device,
        mesh=mesh,
        in_specs=(
            P("site", None, "sec", None, None),
            P("site", None, "sec", None, None),
            P("site", None, "sec", None, None),
            P("site", "sec", None, None),
            P("site", "sec", None, None),
            P("site", "sec", None, None),
            P("site", None, None),
            P("site", None),
            P("site"),
        ),
        out_specs=(P("site", None, "sec", None, None), P("site", None, "sec", None, None)),
        check_vma=False,
    )
```

```python
import functools

import jax
import jax.numpy as jnp
from jax import lax
from jax.experimental import pallas as pl
from jax.experimental.pallas import tpu as pltpu
from jax.sharding import PartitionSpec as P

NSI = 10
NAPP = 2
NEAR = (8, 8)
FAR = (3, 5, 5, 3)
MESH = pl.DeviceIdType.MESH


def update_kernel(
    sites, secs, steps,
    tab, own_tab, energy, bond_add, canon_l, canon_r, seed_l, seed_r, site_in, bond_in,
    left_out, right_out,
    own_c, tall, wab, hold, fresh, pbuf, give_n, got_n, give_r, got_r, give_c, lefts, tab_v, tab_n, nxt, rgt, site_v, bond_v,
    outer, gram_s, gram_r, unit_s, unit_r, fac_s, fac,
    loc_sem, gsend, grecv, tsend, trecv, xsend, xrecv,
    usem, osend, orecv, fsend, frecv, psend, rsend, rrecv, bsem, lsend, lrecv,
):
    site, sec = lax.axis_index("site"), lax.axis_index("sec")
    role = lax.rem(sec, 2)
    row = sec // 2
    rows = secs // 2
    phys, owned, width = canon_l.shape[0], canon_l.shape[1], canon_l.shape[2]
    sectors = secs * owned
    target = lax.rem(site + 1 - 2 * role + sites, sites)
    source = lax.rem(site - 1 + 2 * role + sites, sites)
    peer_sec = row * 2 + 1 - role
    half = lax.rem(row, 2)
    pair_sec = sec + 2 - 4 * half
    far_target = lax.rem(site, 2) != role
    far_source = lax.rem(site, 2) == role
    ends = sectors - FAR[0]
    far_at = (half * ends, FAR[0], FAR[0] + FAR[1], (1 - half) * ends)
    near_at = (0, NEAR[0])
    last = steps - 1

    loads = [
        pltpu.make_async_copy(canon_l, own_c.at[0, pl.ds(1, phys)], loc_sem.at[0]),
        pltpu.make_async_copy(canon_r, own_c.at[1, pl.ds(1, phys)], loc_sem.at[1]),
    ]
    seeds = [
        pltpu.make_async_copy(seed_l, own_c.at[0, 0], loc_sem.at[4]),
        pltpu.make_async_copy(seed_r, own_c.at[1, 0], loc_sem.at[5]),
    ]
    center = [
        pltpu.make_async_copy(site_in, site_v, loc_sem.at[2]),
        pltpu.make_async_copy(bond_in, bond_v, loc_sem.at[3]),
    ]
    for load in seeds + loads + center:
        load.start()

    barrier = pltpu.get_barrier_semaphore()
    others = [(dy, e) for dy in range(rows) for e in range(2) if (dy, e) != (0, 0)]

    def sec_of(dy, e):
        other_role = role + e - 2 * role * e
        return lax.rem(row + dy, rows) * 2 + other_role, other_role

    for dy, e in others:
        pl.semaphore_signal(barrier, inc=1, device_id=(site, sec_of(dy, e)[0]), device_id_type=MESH)
    for other in (target, source):
        pl.semaphore_signal(barrier, inc=1, device_id=(other, sec), device_id_type=MESH)
    across = lax.rem(site + 1 - 2 * role + sites, sites)
    pl.semaphore_signal(barrier, inc=1, device_id=(across, peer_sec), device_id_type=MESH)
    for load in seeds:
        load.wait()
    for i in range(owned):
        own_c[1, 0, i] = own_c[1, 0, i].T
    pl.semaphore_wait(barrier, len(others) + 3)

    place = pl.ds(sec * owned, owned)
    peer_place = pl.ds(peer_sec * owned, owned)
    parts = (pl.ds(0, 3), pl.ds(3, phys - 2))
    up_row, down_row = lax.rem(row + 1, rows), lax.rem(row + rows - 1, rows)
    up, down = up_row * 2 + role, down_row * 2 + role
    sent = []

    def gather_copy(n, src, part, at, to, slot):
        return pltpu.make_async_remote_copy(
            src_ref=src, dst_ref=tall.at[part, at], send_sem=gsend.at[n], recv_sem=grecv.at[slot],
            device_id=(site, to), device_id_type=MESH)

    def give_on(src, part, at, to, slot):
        sent.append(gather_copy(len(sent), src, part, at, to, slot))
        sent[-1].start()

    def landed(part, at, slot):
        gather_copy(0, tall.at[part, at], part, at, up, slot).wait_recv()

    tab_copy = pltpu.make_async_remote_copy(
        src_ref=own_tab, dst_ref=tab_v, send_sem=bsem.at[0], recv_sem=bsem.at[1],
        device_id=(source, sec), device_id_type=MESH)
    tab_copy.start()
    for load in loads:
        load.wait()
    for h in range(2):
        give_on(own_c.at[1 - role, parts[h]], parts[h], place, peer_sec, h)
    for h in range(2):
        give_on(own_c.at[role, parts[h]], parts[h], place, up, 2 + h)
        give_on(own_c.at[role, parts[1 - h]], parts[1 - h], place, down, 9 - h)
    keep = pltpu.make_async_copy(own_c.at[role], tall.at[:, place], loc_sem.at[0])
    keep.start()

    def block_at(of_row, of_peer):
        return pl.ds((of_row * 2 + (1 - role if of_peer else role)) * owned, owned)

    for h in range(2):
        landed(parts[h], peer_place, h)
        give_on(tall.at[parts[h], peer_place], parts[h], peer_place, up, 4 + h)
        give_on(tall.at[parts[h], peer_place], parts[h], peer_place, down, 10 + h)
        at = block_at(down_row, h)
        landed(parts[0], at, 2 + 2 * h)
        give_on(tall.at[parts[0], at], parts[0], at, up, 6 + h)
        at = block_at(up_row, h)
        landed(parts[1], at, 9 + 2 * h)
        give_on(tall.at[parts[1], at], parts[1], at, down, 12 + h)
    keep.wait()

    def turned(start, count):
        def body(n, carry):
            i = start + n
            hold[0, i] = tall[0, i]
            for s in range(phys):
                wab[1 - role, i, :, s * width : (s + 1) * width] = tall[1 + s, i].T
            return carry

        lax.fori_loop(0, count, body, 0)

    def row_at(of_row):
        return of_row * 2 * owned

    turned(row_at(row), 2 * owned)
    for h in range(2):
        landed(parts[1], block_at(down_row, h), 3 + 2 * h)
    turned(row_at(down_row), 2 * owned)
    for h in range(2):
        landed(parts[0], block_at(up_row, h), 8 + 2 * h)
    turned(row_at(up_row), 2 * owned)
    far_row = lax.rem(row + 2, rows)
    for h in range(2):
        landed(parts[0], block_at(far_row, h), 6 + h)
        landed(parts[1], block_at(far_row, h), 12 + h)
    turned(row_at(far_row), 2 * owned)
    tab_copy.wait_recv()
    pltpu.sync_copy(tab_v, tab_n)

    def in_order(i, carry):
        for s in range(phys):
            wab[role, i, :, s * width : (s + 1) * width] = tall[1 + s, tab[1, s, i]]
        return carry

    lax.fori_loop(0, sectors, in_order, 0)

    def to_target(t, c, part):
        return pltpu.make_async_remote_copy(
            src_ref=fresh.at[t, part], dst_ref=hold.at[t + 1, part],
            send_sem=tsend.at[t, c], recv_sem=trecv.at[t, c],
            device_id=(target, sec), device_id_type=MESH)

    def far_copy(t, c):
        return to_target(t, c, pl.ds(far_at[c], FAR[c]))

    def near_copy(t, c):
        return to_target(t, c, pl.ds(near_at[c], NEAR[c]))

    def pair_copy(t):
        part = pl.ds(far_at[0], FAR[0])
        return pltpu.make_async_remote_copy(
            src_ref=hold.at[t + 1, part], dst_ref=hold.at[t + 1, part],
            send_sem=psend.at[t], recv_sem=trecv.at[t, 3],
            device_id=(site, pair_sec), device_id_type=MESH)

    def apply_right(t, start, length):
        for i in range(length):
            at = start + i
            product = jnp.dot(
                hold[t, at], wab[0, at], preferred_element_type=jnp.float32
            ).astype(jnp.bfloat16)
            for s in range(phys):
                pbuf[at, s] = product[:, s * width : (s + 1) * width]

    def apply_left(t, start, length):
        for i in range(length):
            at = start + i
            stack = jnp.concatenate([pbuf[tab[role, s, at], s] for s in range(phys)], axis=0)
            fresh[t, at] = jnp.dot(
                wab[1, at], stack, preferred_element_type=jnp.float32
            ).astype(jnp.bfloat16)

    def first_half(t):
        came_far = jnp.logical_and(t > 0, far_source)

        @pl.when(came_far)
        def _():
            far_copy(t - 1, 0).wait_recv()
            pair_copy(t - 1).start()
            far_copy(t - 1, 1).wait_recv()
            apply_right(t, far_at[0], FAR[0])
            apply_right(t, far_at[1], FAR[1])
            for c in (2, 3):
                far_copy(t - 1, c).wait_recv()
                apply_right(t, far_at[c], FAR[c])

        @pl.when(jnp.logical_not(came_far))
        def _():
            @pl.when(t > 0)
            def _():
                for c in range(len(NEAR)):
                    near_copy(t - 1, c).wait_recv()

            apply_right(t, 0, sectors)

    def second_half(t, send):
        @pl.when(far_target)
        def _():
            for c in range(3):
                apply_left(t, far_at[c], FAR[c])
                if send:
                    far_copy(t, c).start()
            apply_left(t, far_at[3], FAR[3])

        @pl.when(jnp.logical_not(far_target))
        def _():
            for c in range(len(NEAR)):
                apply_left(t, near_at[c], NEAR[c])
                if send:
                    near_copy(t, c).start()

    def turn(t, carry):
        first_half(t)
        second_half(t, True)
        return carry

    lax.fori_loop(0, last, turn, 0)
    first_half(last)
    second_half(last, False)
    for load in center:
        load.wait()

    rows_at = lax.broadcasted_iota(jnp.int32, (width, width), 0)
    cols_at = lax.broadcasted_iota(jnp.int32, (width, width), 1)
    diagonal = rows_at == cols_at
    own_at = sec * owned
    peer_at = peer_sec * owned
    f32, bf16 = jnp.float32, jnp.bfloat16

    def scale_of(ref, t):
        total = ref[t, 0].astype(f32)
        for i in range(1, sectors):
            total = total + ref[t, i].astype(f32)
        return (sectors * width) / jnp.sum(jnp.where(diagonal, total, 0.0))

    def scaled(block, scale):
        return (block.astype(f32) * scale).astype(bf16)

    def left_copy(n, i):
        return pltpu.make_async_remote_copy(
            src_ref=give_c.at[n, i], dst_ref=lefts.at[i],
            send_sem=lsend.at[n, i], recv_sem=lrecv.at[i],
            device_id=(target, (peer_sec, sec)[n]), device_id_type=MESH)

    nxt_copy = pltpu.make_async_remote_copy(
        src_ref=give_n, dst_ref=got_n,
        send_sem=xsend.at[0], recv_sem=xrecv.at[0],
        device_id=(site, peer_sec), device_id_type=MESH)
    rgt_copies = [pltpu.make_async_remote_copy(
        src_ref=give_r.at[n], dst_ref=got_r,
        send_sem=rsend.at[n], recv_sem=rrecv.at[0],
        device_id=(target, to), device_id_type=MESH) for n, to in enumerate((peer_sec, sec))]

    @pl.when(role == 0)
    def _():
        scale_next = scale_of(fresh, last)
        for i in range(owned):
            for n, start in enumerate((peer_at, own_at)):
                for s in range(phys):
                    give_c[n, i, s] = scaled(fresh[last, tab_n[s, start + i]], scale_next)
                left_copy(n, i).start()
            give_n[i] = scaled(fresh[last, peer_at + i], scale_next)
            nxt[i] = scaled(fresh[last, own_at + i], scale_next)
        nxt_copy.start()

    @pl.when(role == 1)
    def _():
        scale_right = scale_of(fresh, last)
        for n, start in enumerate((peer_at, own_at)):
            for i in range(owned):
                give_r[n, i] = scaled(fresh[last, start + i], scale_right)
            rgt_copies[n].start()

    rgt_copies[0].wait_recv()
    for i in range(owned):
        rgt[i] = got_r[i].T

    def split(x):
        high = x.astype(bf16)
        return high, (x - high.astype(f32)).astype(bf16)

    def as_lhs(parts):
        return jnp.concatenate(parts, axis=1)

    def as_rhs(parts):
        wide = jnp.concatenate(parts, axis=1)
        return jnp.concatenate([wide, wide], axis=0)

    def product(lhs, rhs):
        both = jnp.dot(lhs, rhs, preferred_element_type=f32)
        return both[:, :width] + both[:, width:]

    def middle_of(part):
        return jnp.where(diagonal, 1.5, 0.0) - 0.5 * part

    def inverse_roots(grams):
        norms = [jnp.sqrt(jnp.sum(g * g, keepdims=True)) for g in grams]
        uppers, lowers = [], []
        for g, norm in zip(grams, norms):
            start = g / norm
            middle = middle_of(start)
            uppers.append(product(as_lhs(split(start)), as_rhs(split(middle))))
            lowers.append(middle)

        def repeat(n, carry):
            uppers, lowers = carry
            ups = [split(u) for u in uppers]
            lows = [split(l) for l in lowers]
            mids = [split(middle_of(product(as_lhs(l), as_rhs(u)))) for l, u in zip(lows, ups)]
            return (
                [product(as_lhs(u), as_rhs(m)) for u, m in zip(ups, mids)],
                [product(as_lhs(m), as_rhs(l)) for m, l in zip(mids, lows)],
            )

        uppers, lowers = lax.fori_loop(0, NSI - 2, repeat, (uppers, lowers))
        ups = [split(u) for u in uppers]
        lows = [split(l) for l in lowers]
        mids = [split(middle_of(product(as_lhs(l), as_rhs(u)))) for l, u in zip(lows, ups)]
        return [
            product(as_lhs(m), as_rhs(l)) / jnp.sqrt(norm)
            for m, l, norm in zip(mids, lows, norms)
        ]

    def with_itself(x, dim):
        return lax.dot_general(x, x, (((dim,), (dim,)), ((), ())), preferred_element_type=f32)

    for i in range(owned):
        left_copy(0, i).wait_recv()
        nows = [site_v[s, i] for s in range(phys)]
        for repeat in range(NAPP):
            halves = jnp.concatenate(
                [
                    jnp.dot(lefts[i, s], nows[s], preferred_element_type=f32).astype(bf16)
                    for s in range(phys)
                ],
                axis=0,
            )
            done = jnp.dot(halves, rgt[i], preferred_element_type=f32)
            nows = [
                (done[s * width : (s + 1) * width] + energy[s] * nows[s].astype(f32)).astype(bf16)
                for s in range(phys)
            ]
        for s in range(phys):
            site_v[s, i] = nows[s]
            outer[s, i] = with_itself(nows[s], 1)

    def gram_copy(d):
        return pltpu.make_async_remote_copy(
            src_ref=gram_s.at[d], dst_ref=gram_r.at[sec], send_sem=osend.at[d], recv_sem=orecv.at[sec],
            device_id=(site, d), device_id_type=MESH)

    def pack(n, carry):
        d = lax.rem(sec + 1 + n, secs)
        sums = []
        for i in range(owned):
            total = jnp.zeros((width, width), f32)
            for s in range(phys):
                at = tab[1, s, d * owned + i] - own_at
                mine = jnp.logical_and(at >= 0, at < owned)
                block = outer[s, jnp.clip(at, 0, owned - 1)]
                total = total + jnp.where(mine, block, 0.0)
            sums.append(total)
        gram_s[d, :width] = jnp.where(cols_at >= rows_at, sums[0], sums[1])
        line = jnp.sum(jnp.where(diagonal, sums[1], 0.0), axis=0, keepdims=True)
        gram_s[d, width:] = jnp.broadcast_to(line, (8, width))

        @pl.when(n < secs - 1)
        def _():
            gram_copy(d).start()

        return carry

    lax.fori_loop(0, secs, pack, 0)

    @pl.when(role == 1)
    def _():
        nxt_copy.wait_recv()
        for i in range(owned):
            nxt[i] = got_n[i]

    for i in range(owned):
        bond = bond_v[i]
        for repeat in range(NAPP):
            half_bond = jnp.dot(nxt[i], bond, preferred_element_type=f32).astype(bf16)
            bond = (
                jnp.dot(half_bond, rgt[i], preferred_element_type=f32)
                + bond_add[0] * bond.astype(f32)
            ).astype(bf16)
        bond_v[i] = bond

    grams = [with_itself(bond_v[i], 0) for i in range(owned)]
    for i in range(owned):
        stack = jnp.concatenate([site_v[s, i] for s in range(phys)], axis=0)
        grams.append(with_itself(stack, 0))
    roots = inverse_roots(grams)
    for i in range(owned):
        turned_bond = bond_v[i].T
        unit_s[i] = jnp.dot(
            as_lhs(split(roots[i])),
            jnp.concatenate([turned_bond, turned_bond], axis=0),
            preferred_element_type=f32,
        )
    unit_copy = pltpu.make_async_remote_copy(
        src_ref=unit_s, dst_ref=unit_r, send_sem=usem.at[0], recv_sem=usem.at[1],
        device_id=(lax.rem(site + 1, sites), sec), device_id_type=MESH)
    unit_copy.start()
    roots = roots[owned:]
    for i in range(owned):
        factor = product(as_lhs(split(roots[i])), as_rhs(split(unit_s[i]))).astype(bf16)
        stack = jnp.concatenate([site_v[s, i] for s in range(phys)], axis=0)
        fresh_left = jnp.dot(stack, factor, preferred_element_type=f32).astype(bf16)
        for s in range(phys):
            left_out[s, i] = fresh_left[s * width : (s + 1) * width]

    def gram_from(d):
        return pltpu.make_async_remote_copy(
            src_ref=gram_s.at[d], dst_ref=gram_r.at[d], send_sem=osend.at[d], recv_sem=orecv.at[d],
            device_id=(site, d), device_id_type=MESH)

    for n in range(secs - 1):
        gram_from(lax.rem(sec + 1 + n, secs)).wait_recv()
    total = gram_s[sec]
    for n in range(secs - 1):
        total = total + gram_r[lax.rem(sec + 1 + n, secs)]
    packed, line = total[:width], total[width : width + 1]
    flipped = packed.T
    grams = [
        jnp.where(cols_at >= rows_at, packed, flipped),
        jnp.where(diagonal, line, jnp.where(rows_at > cols_at, packed, flipped)),
    ]
    roots = inverse_roots(grams)
    unit_copy.wait_recv()
    for i in range(owned):
        fac_s[i] = product(as_lhs(split(unit_r[i])), as_rhs(split(roots[i]))).astype(bf16)
    fac_copies = []
    for n, (dy, e) in enumerate(others):
        to, _ = sec_of(dy, e)
        fac_copies.append(pltpu.make_async_remote_copy(
            src_ref=fac_s, dst_ref=fac.at[place], send_sem=fsend.at[n], recv_sem=frecv.at[n],
            device_id=(site, to), device_id_type=MESH))
        fac_copies[-1].start()
    for i in range(owned):
        fac[own_at + i] = fac_s[i]
    for copy in fac_copies:
        copy.wait_recv()
    for i in range(owned):
        for s in range(phys):
            right_out[s, i] = jnp.dot(
                fac[tab[0, s, own_at + i]], site_v[s, i], preferred_element_type=f32
            ).astype(bf16)

    for copy in sent + fac_copies + [unit_copy, tab_copy]:
        copy.wait_send()
    for n in range(secs - 1):
        gram_copy(lax.rem(sec + 1 + n, secs)).wait_send()

    def drain(t, carry):
        @pl.when(far_target)
        def _():
            for c in range(3):
                far_copy(t, c).wait_send()

        @pl.when(jnp.logical_not(far_target))
        def _():
            for c in range(len(NEAR)):
                near_copy(t, c).wait_send()

        @pl.when(far_source)
        def _():
            pair_copy(t).wait_send()

        return carry

    lax.fori_loop(0, last, drain, 0)

    @pl.when(role == 0)
    def _():
        nxt_copy.wait_send()
        for i in range(owned):
            for n in range(2):
                left_copy(n, i).wait_send()

    @pl.when(role == 1)
    def _():
        for copy in rgt_copies:
            copy.wait_send()


def update(tables, own_table, energy, bond_add, canon_l, canon_r, seed_l, seed_r, site, bond):
    sites, secs = lax.axis_size("site"), lax.axis_size("sec")
    steps = sites // 4
    phys, owned, width = canon_l.shape[:3]
    sectors = owned * secs
    bf16, f32 = jnp.bfloat16, jnp.float32
    block = (width, width)
    dma = pltpu.SemaphoreType.DMA
    smem = pl.BlockSpec(memory_space=pltpu.SMEM)
    vmem = pl.BlockSpec(memory_space=pltpu.VMEM)
    hbm = pl.BlockSpec(memory_space=pltpu.HBM)
    mail = pltpu.VMEM((secs, width + 8, width), f32)
    return pl.pallas_call(
        functools.partial(update_kernel, sites, secs, steps),
        out_shape=(
            jax.ShapeDtypeStruct((phys, owned, *block), bf16),
            jax.ShapeDtypeStruct((phys, owned, *block), bf16),
        ),
        in_specs=[smem, vmem, smem, smem] + [hbm] * 6,
        out_specs=(vmem, vmem),
        scratch_shapes=[
            pltpu.VMEM((2, 1 + phys, owned, *block), bf16),
            pltpu.VMEM((1 + phys, sectors, *block), bf16),
            pltpu.VMEM((2, sectors, width, phys * width), bf16),
            pltpu.VMEM((steps, sectors, *block), bf16),
            pltpu.VMEM((steps, sectors, *block), bf16),
            pltpu.VMEM((sectors, phys, *block), bf16),
            pltpu.VMEM((owned, *block), bf16),
            pltpu.VMEM((owned, *block), bf16),
            pltpu.VMEM((2, owned, *block), bf16),
            pltpu.VMEM((owned, *block), bf16),
            pltpu.VMEM((2, owned, phys, *block), bf16),
            pltpu.VMEM((owned, phys, *block), bf16),
            pltpu.VMEM((8, 128), jnp.int32),
            pltpu.SMEM((8, 128), jnp.int32),
            pltpu.VMEM((owned, *block), bf16),
            pltpu.VMEM((owned, *block), bf16),
            pltpu.VMEM((phys, owned, *block), bf16),
            pltpu.VMEM((owned, *block), bf16),
            pltpu.VMEM((phys, owned, *block), f32),
            mail, mail,
            pltpu.VMEM((owned, *block), f32),
            pltpu.VMEM((owned, *block), f32),
            pltpu.VMEM((owned, *block), bf16),
            pltpu.VMEM((sectors, *block), bf16),
            dma((6,)), dma((14,)), dma((14,)),
            dma((steps, 4)), dma((steps, 4)), dma((1,)), dma((1,)),
            dma((2,)), dma((secs,)), dma((secs,)), dma((secs - 1,)), dma((secs - 1,)),
            dma((steps,)), dma((2,)), dma((1,)),
            dma((2,)), dma((2, owned)), dma((owned,)),
        ],
        compiler_params=pltpu.CompilerParams(
            collective_id=0, has_side_effects=True, vmem_limit_bytes=30 * 1024 * 1024
        ),
        name="environments",
    )(
        tables, own_table, energy, bond_add,
        *(
            pltpu.with_memory_space_constraint(x, pltpu.HBM)
            for x in (canon_l, canon_r, seed_l, seed_r, site, bond)
        ),
    )


def per_device(
    left_canon,
    right_canon,
    center_site,
    center_bond,
    left_seed,
    right_seed,
    left_sector,
    onsite,
    bond_shift,
):
    sources = left_sector[0]
    labels = jnp.arange(sources.shape[1], dtype=jnp.int32)
    right_of = jnp.sum(
        jnp.where(sources[:, :, None] == labels[None, None, :], labels[None, :, None], 0), axis=1
    )
    phys, sectors = sources.shape
    own_table = jnp.pad(sources, ((0, 8 - phys), (0, 128 - sectors)))
    left_new, right_new = update(
        jnp.stack([sources, right_of]), own_table, onsite[0], bond_shift, left_canon[0], right_canon[0],
        left_seed[0], right_seed[0], center_site[0], center_bond[0],
    )
    return (left_new[None], right_new[None])


def solution(mesh):
    return jax.shard_map(
        per_device,
        mesh=mesh,
        in_specs=(
            P("site", None, "sec", None, None),
            P("site", None, "sec", None, None),
            P("site", None, "sec", None, None),
            P("site", "sec", None, None),
            P("site", "sec", None, None),
            P("site", "sec", None, None),
            P("site", None, None),
            P("site", None),
            P("site"),
        ),
        out_specs=(P("site", None, "sec", None, None), P("site", None, "sec", None, None)),
        check_vma=False,
    )
```

```python
import functools

import jax
import jax.numpy as jnp
from jax import lax
from jax.experimental import pallas as pl
from jax.experimental.pallas import tpu as pltpu
from jax.sharding import PartitionSpec as P

NSI = 10
NAPP = 2
NEAR = (8, 8)
FAR = (3, 5, 5, 3)
MESH = pl.DeviceIdType.MESH


def update_kernel(
    sites, secs, steps,
    src_tab, own_tab, energy_in, bond_add, canon_l, canon_r, seed_l, seed_r, site_in, bond_in,
    left_out, right_out,
    own_c, tall, wab, hold, fresh, pbuf, give_n, got_n, give_r, got_r, give_c, lefts, tab, tab_v, tab_n, energy, nxt, rgt, site_v, bond_v,
    outer, gram_s, gram_r, unit_s, unit_r, fac_s, fac,
    loc_sem, gsend, grecv, tsend, trecv, xsend, xrecv,
    usem, osend, orecv, fsend, frecv, psend, rsend, rrecv, bsem, lsend, lrecv,
):
    site, sec = lax.axis_index("site"), lax.axis_index("sec")
    role = lax.rem(sec, 2)
    row = sec // 2
    rows = secs // 2
    phys, owned, width = canon_l.shape[0], canon_l.shape[1], canon_l.shape[2]
    sectors = secs * owned
    target = lax.rem(site + 1 - 2 * role + sites, sites)
    source = lax.rem(site - 1 + 2 * role + sites, sites)
    peer_sec = row * 2 + 1 - role
    half = lax.rem(row, 2)
    pair_sec = sec + 2 - 4 * half
    far_target = lax.rem(site, 2) != role
    far_source = lax.rem(site, 2) == role
    ends = sectors - FAR[0]
    far_at = (half * ends, FAR[0], FAR[0] + FAR[1], (1 - half) * ends)
    near_at = (0, NEAR[0])
    last = steps - 1

    loads = [
        pltpu.make_async_copy(canon_l, own_c.at[0, pl.ds(1, phys)], loc_sem.at[0]),
        pltpu.make_async_copy(canon_r, own_c.at[1, pl.ds(1, phys)], loc_sem.at[1]),
    ]
    seeds = [
        pltpu.make_async_copy(seed_l, own_c.at[0, 0], loc_sem.at[4]),
        pltpu.make_async_copy(seed_r, own_c.at[1, 0], loc_sem.at[5]),
    ]
    center = [
        pltpu.make_async_copy(site_in, site_v, loc_sem.at[2]),
        pltpu.make_async_copy(bond_in, bond_v, loc_sem.at[3]),
        pltpu.make_async_copy(energy_in, energy, loc_sem.at[6]),
    ]
    for load in seeds + loads + center:
        load.start()

    barrier = pltpu.get_barrier_semaphore()
    others = [(dy, e) for dy in range(rows) for e in range(2) if (dy, e) != (0, 0)]

    def sec_of(dy, e):
        other_role = role + e - 2 * role * e
        return lax.rem(row + dy, rows) * 2 + other_role, other_role

    for dy, e in others:
        pl.semaphore_signal(barrier, inc=1, device_id=(site, sec_of(dy, e)[0]), device_id_type=MESH)
    for other in (target, source):
        pl.semaphore_signal(barrier, inc=1, device_id=(other, sec), device_id_type=MESH)
    across = lax.rem(site + 1 - 2 * role + sites, sites)
    pl.semaphore_signal(barrier, inc=1, device_id=(across, peer_sec), device_id_type=MESH)
    for load in seeds:
        load.wait()
    for i in range(owned):
        own_c[1, 0, i] = own_c[1, 0, i].T
    pl.semaphore_wait(barrier, len(others) + 3)

    place = pl.ds(sec * owned, owned)
    peer_place = pl.ds(peer_sec * owned, owned)
    parts = (pl.ds(0, 3), pl.ds(3, phys - 2))
    up_row, down_row = lax.rem(row + 1, rows), lax.rem(row + rows - 1, rows)
    up, down = up_row * 2 + role, down_row * 2 + role
    sent = []

    def gather_copy(n, src, part, at, to, slot):
        return pltpu.make_async_remote_copy(
            src_ref=src, dst_ref=tall.at[part, at], send_sem=gsend.at[n], recv_sem=grecv.at[slot],
            device_id=(site, to), device_id_type=MESH)

    def give_on(src, part, at, to, slot):
        sent.append(gather_copy(len(sent), src, part, at, to, slot))
        sent[-1].start()

    def landed(part, at, slot):
        gather_copy(0, tall.at[part, at], part, at, up, slot).wait_recv()

    tab_copy = pltpu.make_async_remote_copy(
        src_ref=own_tab, dst_ref=tab_v, send_sem=bsem.at[0], recv_sem=bsem.at[1],
        device_id=(source, sec), device_id_type=MESH)
    tab_copy.start()
    for load in loads:
        load.wait()
    for h in range(2):
        give_on(own_c.at[1 - role, parts[h]], parts[h], place, peer_sec, h)
    for h in range(2):
        give_on(own_c.at[role, parts[h]], parts[h], place, up, 2 + h)
        give_on(own_c.at[role, parts[1 - h]], parts[1 - h], place, down, 9 - h)
    keep = pltpu.make_async_copy(own_c.at[role], tall.at[:, place], loc_sem.at[0])
    keep.start()

    def block_at(of_row, of_peer):
        return pl.ds((of_row * 2 + (1 - role if of_peer else role)) * owned, owned)

    for h in range(2):
        landed(parts[h], peer_place, h)
        give_on(tall.at[parts[h], peer_place], parts[h], peer_place, up, 4 + h)
        give_on(tall.at[parts[h], peer_place], parts[h], peer_place, down, 10 + h)
        at = block_at(down_row, h)
        landed(parts[0], at, 2 + 2 * h)
        give_on(tall.at[parts[0], at], parts[0], at, up, 6 + h)
        at = block_at(up_row, h)
        landed(parts[1], at, 9 + 2 * h)
        give_on(tall.at[parts[1], at], parts[1], at, down, 12 + h)
    keep.wait()

    def tabulate(n, carry):
        s, m = n // sectors, lax.rem(n, sectors)
        joined = jnp.int32(0)
        for k in range(sectors):
            joined = jnp.where(src_tab[s, k] == m, k, joined)
        tab[0, s, m] = src_tab[s, m]
        tab[1, s, m] = joined
        return carry

    lax.fori_loop(0, phys * sectors, tabulate, 0)

    def turned(start, count):
        def body(n, carry):
            i = start + n
            hold[0, i] = tall[0, i]
            for s in range(phys):
                wab[1 - role, i, :, s * width : (s + 1) * width] = tall[1 + s, i].T
            return carry

        lax.fori_loop(0, count, body, 0)

    def row_at(of_row):
        return of_row * 2 * owned

    turned(row_at(row), 2 * owned)
    for h in range(2):
        landed(parts[1], block_at(down_row, h), 3 + 2 * h)
    turned(row_at(down_row), 2 * owned)
    for h in range(2):
        landed(parts[0], block_at(up_row, h), 8 + 2 * h)
    turned(row_at(up_row), 2 * owned)
    far_row = lax.rem(row + 2, rows)
    for h in range(2):
        landed(parts[0], block_at(far_row, h), 6 + h)
        landed(parts[1], block_at(far_row, h), 12 + h)
    turned(row_at(far_row), 2 * owned)
    tab_copy.wait_recv()
    pltpu.sync_copy(tab_v, tab_n)

    def in_order(i, carry):
        for s in range(phys):
            wab[role, i, :, s * width : (s + 1) * width] = tall[1 + s, tab[1, s, i]]
        return carry

    lax.fori_loop(0, sectors, in_order, 0)

    def to_target(t, c, part):
        return pltpu.make_async_remote_copy(
            src_ref=fresh.at[t, part], dst_ref=hold.at[t + 1, part],
            send_sem=tsend.at[t, c], recv_sem=trecv.at[t, c],
            device_id=(target, sec), device_id_type=MESH)

    def far_copy(t, c):
        return to_target(t, c, pl.ds(far_at[c], FAR[c]))

    def near_copy(t, c):
        return to_target(t, c, pl.ds(near_at[c], NEAR[c]))

    def pair_copy(t):
        part = pl.ds(far_at[0], FAR[0])
        return pltpu.make_async_remote_copy(
            src_ref=hold.at[t + 1, part], dst_ref=hold.at[t + 1, part],
            send_sem=psend.at[t], recv_sem=trecv.at[t, 3],
            device_id=(site, pair_sec), device_id_type=MESH)

    def apply_right(t, start, length):
        for i in range(length):
            at = start + i
            product = jnp.dot(
                hold[t, at], wab[0, at], preferred_element_type=jnp.float32
            ).astype(jnp.bfloat16)
            for s in range(phys):
                pbuf[at, s] = product[:, s * width : (s + 1) * width]

    def apply_left(t, start, length):
        for i in range(length):
            at = start + i
            stack = jnp.concatenate([pbuf[tab[role, s, at], s] for s in range(phys)], axis=0)
            fresh[t, at] = jnp.dot(
                wab[1, at], stack, preferred_element_type=jnp.float32
            ).astype(jnp.bfloat16)

    def first_half(t):
        came_far = jnp.logical_and(t > 0, far_source)

        @pl.when(came_far)
        def _():
            far_copy(t - 1, 0).wait_recv()
            pair_copy(t - 1).start()
            far_copy(t - 1, 1).wait_recv()
            apply_right(t, far_at[0], FAR[0])
            apply_right(t, far_at[1], FAR[1])
            for c in (2, 3):
                far_copy(t - 1, c).wait_recv()
                apply_right(t, far_at[c], FAR[c])

        @pl.when(jnp.logical_not(came_far))
        def _():
            @pl.when(t > 0)
            def _():
                for c in range(len(NEAR)):
                    near_copy(t - 1, c).wait_recv()

            apply_right(t, 0, sectors)

    def second_half(t, send):
        @pl.when(far_target)
        def _():
            for c in range(3):
                apply_left(t, far_at[c], FAR[c])
                if send:
                    far_copy(t, c).start()
            apply_left(t, far_at[3], FAR[3])

        @pl.when(jnp.logical_not(far_target))
        def _():
            for c in range(len(NEAR)):
                apply_left(t, near_at[c], NEAR[c])
                if send:
                    near_copy(t, c).start()

    def turn(t, carry):
        first_half(t)
        second_half(t, True)
        return carry

    lax.fori_loop(0, last, turn, 0)
    first_half(last)
    second_half(last, False)
    for load in center:
        load.wait()

    rows_at = lax.broadcasted_iota(jnp.int32, (width, width), 0)
    cols_at = lax.broadcasted_iota(jnp.int32, (width, width), 1)
    diagonal = rows_at == cols_at
    own_at = sec * owned
    peer_at = peer_sec * owned
    f32, bf16 = jnp.float32, jnp.bfloat16

    def scale_of(ref, t):
        total = ref[t, 0].astype(f32)
        for i in range(1, sectors):
            total = total + ref[t, i].astype(f32)
        return (sectors * width) / jnp.sum(jnp.where(diagonal, total, 0.0))

    def scaled(block, scale):
        return (block.astype(f32) * scale).astype(bf16)

    def left_copy(n, i):
        return pltpu.make_async_remote_copy(
            src_ref=give_c.at[n, i], dst_ref=lefts.at[i],
            send_sem=lsend.at[n, i], recv_sem=lrecv.at[i],
            device_id=(target, (peer_sec, sec)[n]), device_id_type=MESH)

    nxt_copy = pltpu.make_async_remote_copy(
        src_ref=give_n, dst_ref=got_n,
        send_sem=xsend.at[0], recv_sem=xrecv.at[0],
        device_id=(site, peer_sec), device_id_type=MESH)
    rgt_copies = [pltpu.make_async_remote_copy(
        src_ref=give_r.at[n], dst_ref=got_r,
        send_sem=rsend.at[n], recv_sem=rrecv.at[0],
        device_id=(target, to), device_id_type=MESH) for n, to in enumerate((peer_sec, sec))]

    @pl.when(role == 0)
    def _():
        scale_next = scale_of(fresh, last)
        for i in range(owned):
            for n, start in enumerate((peer_at, own_at)):
                for s in range(phys):
                    give_c[n, i, s] = scaled(fresh[last, tab_n[s, start + i]], scale_next)
                left_copy(n, i).start()
            give_n[i] = scaled(fresh[last, peer_at + i], scale_next)
            nxt[i] = scaled(fresh[last, own_at + i], scale_next)
        nxt_copy.start()

    @pl.when(role == 1)
    def _():
        scale_right = scale_of(fresh, last)
        for n, start in enumerate((peer_at, own_at)):
            for i in range(owned):
                give_r[n, i] = scaled(fresh[last, start + i], scale_right)
            rgt_copies[n].start()

    rgt_copies[0].wait_recv()
    for i in range(owned):
        rgt[i] = got_r[i].T

    def split(x):
        high = x.astype(bf16)
        return high, (x - high.astype(f32)).astype(bf16)

    def as_lhs(parts):
        return jnp.concatenate(parts, axis=1)

    def as_rhs(parts):
        wide = jnp.concatenate(parts, axis=1)
        return jnp.concatenate([wide, wide], axis=0)

    def product(lhs, rhs):
        both = jnp.dot(lhs, rhs, preferred_element_type=f32)
        return both[:, :width] + both[:, width:]

    def middle_of(part):
        return jnp.where(diagonal, 1.5, 0.0) - 0.5 * part

    def inverse_roots(grams):
        norms = [jnp.sqrt(jnp.sum(g * g, keepdims=True)) for g in grams]
        uppers, lowers = [], []
        for g, norm in zip(grams, norms):
            start = g / norm
            middle = middle_of(start)
            uppers.append(product(as_lhs(split(start)), as_rhs(split(middle))))
            lowers.append(middle)

        def repeat(n, carry):
            uppers, lowers = carry
            ups = [split(u) for u in uppers]
            lows = [split(l) for l in lowers]
            mids = [split(middle_of(product(as_lhs(l), as_rhs(u)))) for l, u in zip(lows, ups)]
            return (
                [product(as_lhs(u), as_rhs(m)) for u, m in zip(ups, mids)],
                [product(as_lhs(m), as_rhs(l)) for m, l in zip(mids, lows)],
            )

        uppers, lowers = lax.fori_loop(0, NSI - 2, repeat, (uppers, lowers))
        ups = [split(u) for u in uppers]
        lows = [split(l) for l in lowers]
        mids = [split(middle_of(product(as_lhs(l), as_rhs(u)))) for l, u in zip(lows, ups)]
        return [
            product(as_lhs(m), as_rhs(l)) / jnp.sqrt(norm)
            for m, l, norm in zip(mids, lows, norms)
        ]

    def with_itself(x, dim):
        return lax.dot_general(x, x, (((dim,), (dim,)), ((), ())), preferred_element_type=f32)

    for i in range(owned):
        left_copy(0, i).wait_recv()
        nows = [site_v[s, i] for s in range(phys)]
        for repeat in range(NAPP):
            halves = jnp.concatenate(
                [
                    jnp.dot(lefts[i, s], nows[s], preferred_element_type=f32).astype(bf16)
                    for s in range(phys)
                ],
                axis=0,
            )
            done = jnp.dot(halves, rgt[i], preferred_element_type=f32)
            nows = [
                (done[s * width : (s + 1) * width] + energy[0, s] * nows[s].astype(f32)).astype(bf16)
                for s in range(phys)
            ]
        for s in range(phys):
            site_v[s, i] = nows[s]
            outer[s, i] = with_itself(nows[s], 1)

    def gram_copy(d):
        return pltpu.make_async_remote_copy(
            src_ref=gram_s.at[d], dst_ref=gram_r.at[sec], send_sem=osend.at[d], recv_sem=orecv.at[sec],
            device_id=(site, d), device_id_type=MESH)

    def pack(n, carry):
        d = lax.rem(sec + 1 + n, secs)
        sums = []
        for i in range(owned):
            total = jnp.zeros((width, width), f32)
            for s in range(phys):
                at = tab[1, s, d * owned + i] - own_at
                mine = jnp.logical_and(at >= 0, at < owned)
                block = outer[s, jnp.clip(at, 0, owned - 1)]
                total = total + jnp.where(mine, block, 0.0)
            sums.append(total)
        gram_s[d, :width] = jnp.where(cols_at >= rows_at, sums[0], sums[1])
        line = jnp.sum(jnp.where(diagonal, sums[1], 0.0), axis=0, keepdims=True)
        gram_s[d, width:] = jnp.broadcast_to(line, (8, width))

        @pl.when(n < secs - 1)
        def _():
            gram_copy(d).start()

        return carry

    lax.fori_loop(0, secs, pack, 0)

    @pl.when(role == 1)
    def _():
        nxt_copy.wait_recv()
        for i in range(owned):
            nxt[i] = got_n[i]

    for i in range(owned):
        bond = bond_v[i]
        for repeat in range(NAPP):
            half_bond = jnp.dot(nxt[i], bond, preferred_element_type=f32).astype(bf16)
            bond = (
                jnp.dot(half_bond, rgt[i], preferred_element_type=f32)
                + bond_add[0] * bond.astype(f32)
            ).astype(bf16)
        bond_v[i] = bond

    roots = inverse_roots([with_itself(bond_v[i], 0) for i in range(owned)])
    for i in range(owned):
        turned_bond = bond_v[i].T
        unit_s[i] = jnp.dot(
            as_lhs(split(roots[i])),
            jnp.concatenate([turned_bond, turned_bond], axis=0),
            preferred_element_type=f32,
        )
    unit_copy = pltpu.make_async_remote_copy(
        src_ref=unit_s, dst_ref=unit_r, send_sem=usem.at[0], recv_sem=usem.at[1],
        device_id=(lax.rem(site + 1, sites), sec), device_id_type=MESH)
    unit_copy.start()
    def gram_from(d):
        return pltpu.make_async_remote_copy(
            src_ref=gram_s.at[d], dst_ref=gram_r.at[d], send_sem=osend.at[d], recv_sem=orecv.at[d],
            device_id=(site, d), device_id_type=MESH)

    for n in range(secs - 1):
        gram_from(lax.rem(sec + 1 + n, secs)).wait_recv()
    total = gram_s[sec]
    for n in range(secs - 1):
        total = total + gram_r[lax.rem(sec + 1 + n, secs)]
    packed, line = total[:width], total[width : width + 1]
    flipped = packed.T
    grams = [
        jnp.where(cols_at >= rows_at, packed, flipped),
        jnp.where(diagonal, line, jnp.where(rows_at > cols_at, packed, flipped)),
    ]
    roots = inverse_roots(grams)
    unit_copy.wait_recv()
    for i in range(owned):
        fac_s[i] = product(as_lhs(split(unit_r[i])), as_rhs(split(roots[i]))).astype(bf16)
    fac_copies = []
    for n, (dy, e) in enumerate(others):
        to, _ = sec_of(dy, e)
        fac_copies.append(pltpu.make_async_remote_copy(
            src_ref=fac_s, dst_ref=fac.at[place], send_sem=fsend.at[n], recv_sem=frecv.at[n],
            device_id=(site, to), device_id_type=MESH))
        fac_copies[-1].start()
    for i in range(owned):
        fac[own_at + i] = fac_s[i]

    grams = []
    for i in range(owned):
        stack = jnp.concatenate([site_v[s, i] for s in range(phys)], axis=0)
        grams.append(with_itself(stack, 0))
    roots = inverse_roots(grams)
    for i in range(owned):
        factor = product(as_lhs(split(roots[i])), as_rhs(split(unit_s[i]))).astype(bf16)
        stack = jnp.concatenate([site_v[s, i] for s in range(phys)], axis=0)
        fresh_left = jnp.dot(stack, factor, preferred_element_type=f32).astype(bf16)
        for s in range(phys):
            left_out[s, i] = fresh_left[s * width : (s + 1) * width]

    for copy in fac_copies:
        copy.wait_recv()
    for i in range(owned):
        for s in range(phys):
            right_out[s, i] = jnp.dot(
                fac[tab[0, s, own_at + i]], site_v[s, i], preferred_element_type=f32
            ).astype(bf16)

    for copy in sent + fac_copies + [unit_copy, tab_copy]:
        copy.wait_send()
    for n in range(secs - 1):
        gram_copy(lax.rem(sec + 1 + n, secs)).wait_send()

    def drain(t, carry):
        @pl.when(far_target)
        def _():
            for c in range(3):
                far_copy(t, c).wait_send()

        @pl.when(jnp.logical_not(far_target))
        def _():
            for c in range(len(NEAR)):
                near_copy(t, c).wait_send()

        @pl.when(far_source)
        def _():
            pair_copy(t).wait_send()

        return carry

    lax.fori_loop(0, last, drain, 0)

    @pl.when(role == 0)
    def _():
        nxt_copy.wait_send()
        for i in range(owned):
            for n in range(2):
                left_copy(n, i).wait_send()

    @pl.when(role == 1)
    def _():
        for copy in rgt_copies:
            copy.wait_send()


def update(table, energy, bond_add, canon_l, canon_r, seed_l, seed_r, site, bond):
    sites, secs = lax.axis_size("site"), lax.axis_size("sec")
    steps = sites // 4
    phys, owned, width = canon_l.shape[:3]
    sectors = owned * secs
    bf16, f32 = jnp.bfloat16, jnp.float32
    block = (width, width)
    dma = pltpu.SemaphoreType.DMA
    smem = pl.BlockSpec(memory_space=pltpu.SMEM)
    vmem = pl.BlockSpec(memory_space=pltpu.VMEM)
    hbm = pl.BlockSpec(memory_space=pltpu.HBM)
    mail = pltpu.VMEM((secs, width + 8, width), f32)
    return pl.pallas_call(
        functools.partial(update_kernel, sites, secs, steps),
        out_shape=(
            jax.ShapeDtypeStruct((phys, owned, *block), bf16),
            jax.ShapeDtypeStruct((phys, owned, *block), bf16),
        ),
        in_specs=[smem, hbm, hbm, smem] + [hbm] * 6,
        out_specs=(vmem, vmem),
        scratch_shapes=[
            pltpu.VMEM((2, 1 + phys, owned, *block), bf16),
            pltpu.VMEM((1 + phys, sectors, *block), bf16),
            pltpu.VMEM((2, sectors, width, phys * width), bf16),
            pltpu.VMEM((steps, sectors, *block), bf16),
            pltpu.VMEM((steps, sectors, *block), bf16),
            pltpu.VMEM((sectors, phys, *block), bf16),
            pltpu.VMEM((owned, *block), bf16),
            pltpu.VMEM((owned, *block), bf16),
            pltpu.VMEM((2, owned, *block), bf16),
            pltpu.VMEM((owned, *block), bf16),
            pltpu.VMEM((2, owned, phys, *block), bf16),
            pltpu.VMEM((owned, phys, *block), bf16),
            pltpu.SMEM((2, phys, sectors), jnp.int32),
            pltpu.VMEM((phys, sectors), jnp.int32),
            pltpu.SMEM((phys, sectors), jnp.int32),
            pltpu.SMEM((1, phys), f32),
            pltpu.VMEM((owned, *block), bf16),
            pltpu.VMEM((owned, *block), bf16),
            pltpu.VMEM((phys, owned, *block), bf16),
            pltpu.VMEM((owned, *block), bf16),
            pltpu.VMEM((phys, owned, *block), f32),
            mail, mail,
            pltpu.VMEM((owned, *block), f32),
            pltpu.VMEM((owned, *block), f32),
            pltpu.VMEM((owned, *block), bf16),
            pltpu.VMEM((sectors, *block), bf16),
            dma((7,)), dma((14,)), dma((14,)),
            dma((steps, 4)), dma((steps, 4)), dma((1,)), dma((1,)),
            dma((2,)), dma((secs,)), dma((secs,)), dma((secs - 1,)), dma((secs - 1,)),
            dma((steps,)), dma((2,)), dma((1,)),
            dma((2,)), dma((2, owned)), dma((owned,)),
        ],
        compiler_params=pltpu.CompilerParams(
            collective_id=0, has_side_effects=True, vmem_limit_bytes=30 * 1024 * 1024
        ),
        name="environments",
    )(
        table, pltpu.with_memory_space_constraint(table, pltpu.HBM),
        pltpu.with_memory_space_constraint(energy, pltpu.HBM), bond_add,
        *(
            pltpu.with_memory_space_constraint(x, pltpu.HBM)
            for x in (canon_l, canon_r, seed_l, seed_r, site, bond)
        ),
    )


def per_device(
    left_canon,
    right_canon,
    center_site,
    center_bond,
    left_seed,
    right_seed,
    left_sector,
    onsite,
    bond_shift,
):
    left_new, right_new = update(
        left_sector[0], onsite, bond_shift, left_canon[0], right_canon[0],
        left_seed[0], right_seed[0], center_site[0], center_bond[0],
    )
    return (left_new[None], right_new[None])


def solution(mesh):
    return jax.shard_map(
        per_device,
        mesh=mesh,
        in_specs=(
            P("site", None, "sec", None, None),
            P("site", None, "sec", None, None),
            P("site", None, "sec", None, None),
            P("site", "sec", None, None),
            P("site", "sec", None, None),
            P("site", "sec", None, None),
            P("site", None, None),
            P("site", None),
            P("site"),
        ),
        out_specs=(P("site", None, "sec", None, None), P("site", None, "sec", None, None)),
        check_vma=False,
    )
```

```python
import functools

import jax
import jax.numpy as jnp
from jax import lax
from jax.experimental import pallas as pl
from jax.experimental.pallas import tpu as pltpu
from jax.sharding import PartitionSpec as P

NSI = 10
NAPP = 2
NEAR = (8, 8)
FAR = (3, 5, 5, 3)
MESH = pl.DeviceIdType.MESH


def update_kernel(
    sites, secs, steps,
    src_tab, own_tab, energy_in, bond_add, canon_l, canon_r, seed_l, seed_r, site_in, bond_in,
    left_out, right_out,
    own_c, tall, wab, hold, fresh, pbuf, give_n, got_n, give_r, got_r, give_c, lefts, tab, tab_v, tab_n, energy, nxt, rgt, site_v, bond_v,
    outer, gram_s, gram_r, unit_s, unit_r, fac_s, fac,
    loc_sem, gsend, grecv, tsend, trecv, xsend, xrecv,
    usem, osend, orecv, fsend, frecv, psend, rsend, rrecv, bsem, lsend, lrecv,
):
    site, sec = lax.axis_index("site"), lax.axis_index("sec")
    role = lax.rem(sec, 2)
    row = sec // 2
    rows = secs // 2
    phys, owned, width = canon_l.shape[0], canon_l.shape[1], canon_l.shape[2]
    sectors = secs * owned
    target = lax.rem(site + 1 - 2 * role + sites, sites)
    source = lax.rem(site - 1 + 2 * role + sites, sites)
    peer_sec = row * 2 + 1 - role
    half = lax.rem(row, 2)
    pair_sec = sec + 2 - 4 * half
    far_target = lax.rem(site, 2) != role
    far_source = lax.rem(site, 2) == role
    ends = sectors - FAR[0]
    far_at = (half * ends, FAR[0], FAR[0] + FAR[1], (1 - half) * ends)
    near_at = (0, NEAR[0])
    last = steps - 1

    loads = [
        pltpu.make_async_copy(canon_l, own_c.at[0, pl.ds(1, phys)], loc_sem.at[0]),
        pltpu.make_async_copy(canon_r, own_c.at[1, pl.ds(1, phys)], loc_sem.at[1]),
    ]
    seeds = [
        pltpu.make_async_copy(seed_l, own_c.at[0, 0], loc_sem.at[4]),
        pltpu.make_async_copy(seed_r, own_c.at[1, 0], loc_sem.at[5]),
    ]
    center = [
        pltpu.make_async_copy(site_in, site_v, loc_sem.at[2]),
        pltpu.make_async_copy(bond_in, bond_v, loc_sem.at[3]),
        pltpu.make_async_copy(energy_in, energy, loc_sem.at[6]),
    ]
    for load in seeds + loads + center:
        load.start()

    barrier = pltpu.get_barrier_semaphore()
    others = [(dy, e) for dy in range(rows) for e in range(2) if (dy, e) != (0, 0)]

    def sec_of(dy, e):
        other_role = role + e - 2 * role * e
        return lax.rem(row + dy, rows) * 2 + other_role, other_role

    for dy, e in others:
        pl.semaphore_signal(barrier, inc=1, device_id=(site, sec_of(dy, e)[0]), device_id_type=MESH)
    for other in (target, source):
        pl.semaphore_signal(barrier, inc=1, device_id=(other, sec), device_id_type=MESH)
    across = lax.rem(site + 1 - 2 * role + sites, sites)
    pl.semaphore_signal(barrier, inc=1, device_id=(across, peer_sec), device_id_type=MESH)
    for load in seeds:
        load.wait()
    for i in range(owned):
        own_c[1, 0, i] = own_c[1, 0, i].T
    pl.semaphore_wait(barrier, len(others) + 3)

    place = pl.ds(sec * owned, owned)
    peer_place = pl.ds(peer_sec * owned, owned)
    parts = (pl.ds(0, 3), pl.ds(3, phys - 2))
    up_row, down_row = lax.rem(row + 1, rows), lax.rem(row + rows - 1, rows)
    up, down = up_row * 2 + role, down_row * 2 + role
    sent = []

    def gather_copy(n, src, part, at, to, slot):
        return pltpu.make_async_remote_copy(
            src_ref=src, dst_ref=tall.at[part, at], send_sem=gsend.at[n], recv_sem=grecv.at[slot],
            device_id=(site, to), device_id_type=MESH)

    def give_on(src, part, at, to, slot):
        sent.append(gather_copy(len(sent), src, part, at, to, slot))
        sent[-1].start()

    def landed(part, at, slot):
        gather_copy(0, tall.at[part, at], part, at, up, slot).wait_recv()

    tab_copy = pltpu.make_async_remote_copy(
        src_ref=own_tab, dst_ref=tab_v, send_sem=bsem.at[0], recv_sem=bsem.at[1],
        device_id=(source, sec), device_id_type=MESH)
    tab_copy.start()
    for load in loads:
        load.wait()
    for h in (1, 0):
        give_on(own_c.at[1 - role, parts[h]], parts[h], place, peer_sec, h)
    for h in range(2):
        give_on(own_c.at[role, parts[h]], parts[h], place, up, 2 + h)
        give_on(own_c.at[role, parts[1 - h]], parts[1 - h], place, down, 9 - h)
    keep = pltpu.make_async_copy(own_c.at[role], tall.at[:, place], loc_sem.at[0])
    keep.start()

    def block_at(of_row, of_peer):
        return pl.ds((of_row * 2 + (1 - role if of_peer else role)) * owned, owned)

    for h in range(2):
        part = parts[1 - h]
        landed(part, peer_place, 1 - h)
        give_on(tall.at[part, peer_place], part, peer_place, up, 5 - h)
        give_on(tall.at[part, peer_place], part, peer_place, down, 11 - h)
        part = parts[h]
        at = block_at(down_row, h)
        landed(part, at, 2 + 3 * h)
        give_on(tall.at[part, at], part, at, up, 6 + h)
        part = parts[1 - h]
        at = block_at(up_row, h)
        landed(part, at, 9 + h)
        give_on(tall.at[part, at], part, at, down, 12 + h)
    keep.wait()

    def tabulate(n, carry):
        s, m = n // sectors, lax.rem(n, sectors)
        joined = jnp.int32(0)
        for k in range(sectors):
            joined = jnp.where(src_tab[s, k] == m, k, joined)
        tab[0, s, m] = src_tab[s, m]
        tab[1, s, m] = joined
        return carry

    lax.fori_loop(0, phys * sectors, tabulate, 0)

    def turned(start, count):
        def body(n, carry):
            i = start + n
            hold[0, i] = tall[0, i]
            for s in range(phys):
                wab[1 - role, i, :, s * width : (s + 1) * width] = tall[1 + s, i].T
            return carry

        lax.fori_loop(0, count, body, 0)

    def row_at(of_row):
        return of_row * 2 * owned

    turned(row_at(row), 2 * owned)
    for h in range(2):
        landed(parts[1 - h], block_at(down_row, h), 3 + h)
    turned(row_at(down_row), 2 * owned)
    for h in range(2):
        landed(parts[h], block_at(up_row, h), 8 + 3 * h)
    turned(row_at(up_row), 2 * owned)
    far_row = lax.rem(row + 2, rows)
    for h in range(2):
        landed(parts[h], block_at(far_row, h), 6 + h)
        landed(parts[1 - h], block_at(far_row, h), 12 + h)
    turned(row_at(far_row), 2 * owned)
    tab_copy.wait_recv()
    pltpu.sync_copy(tab_v, tab_n)

    def in_order(i, carry):
        for s in range(phys):
            wab[role, i, :, s * width : (s + 1) * width] = tall[1 + s, tab[1, s, i]]
        return carry

    lax.fori_loop(0, sectors, in_order, 0)

    def to_target(t, c, part):
        return pltpu.make_async_remote_copy(
            src_ref=fresh.at[t, part], dst_ref=hold.at[t + 1, part],
            send_sem=tsend.at[t, c], recv_sem=trecv.at[t, c],
            device_id=(target, sec), device_id_type=MESH)

    def far_copy(t, c):
        return to_target(t, c, pl.ds(far_at[c], FAR[c]))

    def near_copy(t, c):
        return to_target(t, c, pl.ds(near_at[c], NEAR[c]))

    def pair_copy(t):
        part = pl.ds(far_at[0], FAR[0])
        return pltpu.make_async_remote_copy(
            src_ref=hold.at[t + 1, part], dst_ref=hold.at[t + 1, part],
            send_sem=psend.at[t], recv_sem=trecv.at[t, 3],
            device_id=(site, pair_sec), device_id_type=MESH)

    def apply_right(t, start, length):
        for i in range(length):
            at = start + i
            product = jnp.dot(
                hold[t, at], wab[0, at], preferred_element_type=jnp.float32
            ).astype(jnp.bfloat16)
            for s in range(phys):
                pbuf[at, s] = product[:, s * width : (s + 1) * width]

    def apply_left(t, start, length):
        for i in range(length):
            at = start + i
            stack = jnp.concatenate([pbuf[tab[role, s, at], s] for s in range(phys)], axis=0)
            fresh[t, at] = jnp.dot(
                wab[1, at], stack, preferred_element_type=jnp.float32
            ).astype(jnp.bfloat16)

    def first_half(t):
        came_far = jnp.logical_and(t > 0, far_source)

        @pl.when(came_far)
        def _():
            far_copy(t - 1, 0).wait_recv()
            pair_copy(t - 1).start()
            far_copy(t - 1, 1).wait_recv()
            apply_right(t, far_at[0], FAR[0])
            apply_right(t, far_at[1], FAR[1])
            for c in (2, 3):
                far_copy(t - 1, c).wait_recv()
                apply_right(t, far_at[c], FAR[c])

        @pl.when(jnp.logical_not(came_far))
        def _():
            @pl.when(t > 0)
            def _():
                for c in range(len(NEAR)):
                    near_copy(t - 1, c).wait_recv()

            apply_right(t, 0, sectors)

    def second_half(t, send):
        @pl.when(far_target)
        def _():
            for c in range(3):
                apply_left(t, far_at[c], FAR[c])
                if send:
                    far_copy(t, c).start()
            apply_left(t, far_at[3], FAR[3])

        @pl.when(jnp.logical_not(far_target))
        def _():
            for c in range(len(NEAR)):
                apply_left(t, near_at[c], NEAR[c])
                if send:
                    near_copy(t, c).start()

    def turn(t, carry):
        first_half(t)
        second_half(t, True)
        return carry

    lax.fori_loop(0, last, turn, 0)
    first_half(last)
    second_half(last, False)
    for load in center:
        load.wait()

    rows_at = lax.broadcasted_iota(jnp.int32, (width, width), 0)
    cols_at = lax.broadcasted_iota(jnp.int32, (width, width), 1)
    diagonal = rows_at == cols_at
    own_at = sec * owned
    peer_at = peer_sec * owned
    f32, bf16 = jnp.float32, jnp.bfloat16

    def scale_of(ref, t):
        total = ref[t, 0].astype(f32)
        for i in range(1, sectors):
            total = total + ref[t, i].astype(f32)
        return (sectors * width) / jnp.sum(jnp.where(diagonal, total, 0.0))

    def scaled(block, scale):
        return (block.astype(f32) * scale).astype(bf16)

    def left_copy(n, i):
        return pltpu.make_async_remote_copy(
            src_ref=give_c.at[n, i], dst_ref=lefts.at[i],
            send_sem=lsend.at[n, i], recv_sem=lrecv.at[i],
            device_id=(target, (peer_sec, sec)[n]), device_id_type=MESH)

    nxt_copy = pltpu.make_async_remote_copy(
        src_ref=give_n, dst_ref=got_n,
        send_sem=xsend.at[0], recv_sem=xrecv.at[0],
        device_id=(site, peer_sec), device_id_type=MESH)
    rgt_copies = [pltpu.make_async_remote_copy(
        src_ref=give_r.at[n], dst_ref=got_r,
        send_sem=rsend.at[n], recv_sem=rrecv.at[0],
        device_id=(target, to), device_id_type=MESH) for n, to in enumerate((peer_sec, sec))]

    @pl.when(role == 0)
    def _():
        scale_next = scale_of(fresh, last)
        for i in range(owned):
            for n, start in enumerate((peer_at, own_at)):
                for s in range(phys):
                    give_c[n, i, s] = scaled(fresh[last, tab_n[s, start + i]], scale_next)
                left_copy(n, i).start()
            give_n[i] = scaled(fresh[last, peer_at + i], scale_next)
            nxt[i] = scaled(fresh[last, own_at + i], scale_next)
        nxt_copy.start()

    @pl.when(role == 1)
    def _():
        scale_right = scale_of(fresh, last)
        for n, start in enumerate((peer_at, own_at)):
            for i in range(owned):
                give_r[n, i] = scaled(fresh[last, start + i], scale_right)
            rgt_copies[n].start()

    rgt_copies[0].wait_recv()
    for i in range(owned):
        rgt[i] = got_r[i].T

    def split(x):
        high = x.astype(bf16)
        return high, (x - high.astype(f32)).astype(bf16)

    def as_lhs(parts):
        return jnp.concatenate(parts, axis=1)

    def as_rhs(parts):
        wide = jnp.concatenate(parts, axis=1)
        return jnp.concatenate([wide, wide], axis=0)

    def product(lhs, rhs):
        both = jnp.dot(lhs, rhs, preferred_element_type=f32)
        return both[:, :width] + both[:, width:]

    def middle_of(part):
        return jnp.where(diagonal, 1.5, 0.0) - 0.5 * part

    def inverse_roots(grams):
        norms = [jnp.sqrt(jnp.sum(g * g, keepdims=True)) for g in grams]
        uppers, lowers = [], []
        for g, norm in zip(grams, norms):
            start = g / norm
            middle = middle_of(start)
            uppers.append(product(as_lhs(split(start)), as_rhs(split(middle))))
            lowers.append(middle)

        def repeat(n, carry):
            uppers, lowers = carry
            ups = [split(u) for u in uppers]
            lows = [split(l) for l in lowers]
            mids = [split(middle_of(product(as_lhs(l), as_rhs(u)))) for l, u in zip(lows, ups)]
            return (
                [product(as_lhs(u), as_rhs(m)) for u, m in zip(ups, mids)],
                [product(as_lhs(m), as_rhs(l)) for m, l in zip(mids, lows)],
            )

        uppers, lowers = lax.fori_loop(0, NSI - 2, repeat, (uppers, lowers))
        ups = [split(u) for u in uppers]
        lows = [split(l) for l in lowers]
        mids = [split(middle_of(product(as_lhs(l), as_rhs(u)))) for l, u in zip(lows, ups)]
        return [
            product(as_lhs(m), as_rhs(l)) / jnp.sqrt(norm)
            for m, l, norm in zip(mids, lows, norms)
        ]

    def with_itself(x, dim):
        return lax.dot_general(x, x, (((dim,), (dim,)), ((), ())), preferred_element_type=f32)

    for i in range(owned):
        left_copy(0, i).wait_recv()
        nows = [site_v[s, i] for s in range(phys)]
        for repeat in range(NAPP):
            halves = jnp.concatenate(
                [
                    jnp.dot(lefts[i, s], nows[s], preferred_element_type=f32).astype(bf16)
                    for s in range(phys)
                ],
                axis=0,
            )
            done = jnp.dot(halves, rgt[i], preferred_element_type=f32)
            nows = [
                (done[s * width : (s + 1) * width] + energy[0, s] * nows[s].astype(f32)).astype(bf16)
                for s in range(phys)
            ]
        for s in range(phys):
            site_v[s, i] = nows[s]
            outer[s, i] = with_itself(nows[s], 1)

    def gram_copy(d):
        return pltpu.make_async_remote_copy(
            src_ref=gram_s.at[d], dst_ref=gram_r.at[sec], send_sem=osend.at[d], recv_sem=orecv.at[sec],
            device_id=(site, d), device_id_type=MESH)

    def pack(n, carry):
        d = lax.rem(sec + 1 + n, secs)
        sums = []
        for i in range(owned):
            total = jnp.zeros((width, width), f32)
            for s in range(phys):
                at = tab[1, s, d * owned + i] - own_at
                mine = jnp.logical_and(at >= 0, at < owned)
                block = outer[s, jnp.clip(at, 0, owned - 1)]
                total = total + jnp.where(mine, block, 0.0)
            sums.append(total)
        gram_s[d, :width] = jnp.where(cols_at >= rows_at, sums[0], sums[1])
        line = jnp.sum(jnp.where(diagonal, sums[1], 0.0), axis=0, keepdims=True)
        gram_s[d, width:] = jnp.broadcast_to(line, (8, width))

        @pl.when(n < secs - 1)
        def _():
            gram_copy(d).start()

        return carry

    lax.fori_loop(0, secs, pack, 0)

    @pl.when(role == 1)
    def _():
        nxt_copy.wait_recv()
        for i in range(owned):
            nxt[i] = got_n[i]

    for i in range(owned):
        bond = bond_v[i]
        for repeat in range(NAPP):
            half_bond = jnp.dot(nxt[i], bond, preferred_element_type=f32).astype(bf16)
            bond = (
                jnp.dot(half_bond, rgt[i], preferred_element_type=f32)
                + bond_add[0] * bond.astype(f32)
            ).astype(bf16)
        bond_v[i] = bond

    roots = inverse_roots([with_itself(bond_v[i], 0) for i in range(owned)])
    for i in range(owned):
        turned_bond = bond_v[i].T
        unit_s[i] = jnp.dot(
            as_lhs(split(roots[i])),
            jnp.concatenate([turned_bond, turned_bond], axis=0),
            preferred_element_type=f32,
        )
    unit_copy = pltpu.make_async_remote_copy(
        src_ref=unit_s, dst_ref=unit_r, send_sem=usem.at[0], recv_sem=usem.at[1],
        device_id=(lax.rem(site + 1, sites), sec), device_id_type=MESH)
    unit_copy.start()
    def gram_from(d):
        return pltpu.make_async_remote_copy(
            src_ref=gram_s.at[d], dst_ref=gram_r.at[d], send_sem=osend.at[d], recv_sem=orecv.at[d],
            device_id=(site, d), device_id_type=MESH)

    for n in range(secs - 1):
        gram_from(lax.rem(sec + 1 + n, secs)).wait_recv()
    total = gram_s[sec]
    for n in range(secs - 1):
        total = total + gram_r[lax.rem(sec + 1 + n, secs)]
    packed, line = total[:width], total[width : width + 1]
    flipped = packed.T
    grams = [
        jnp.where(cols_at >= rows_at, packed, flipped),
        jnp.where(diagonal, line, jnp.where(rows_at > cols_at, packed, flipped)),
    ]
    roots = inverse_roots(grams)
    unit_copy.wait_recv()
    for i in range(owned):
        fac_s[i] = product(as_lhs(split(unit_r[i])), as_rhs(split(roots[i]))).astype(bf16)
    fac_copies = []
    for n, (dy, e) in enumerate(others):
        to, _ = sec_of(dy, e)
        fac_copies.append(pltpu.make_async_remote_copy(
            src_ref=fac_s, dst_ref=fac.at[place], send_sem=fsend.at[n], recv_sem=frecv.at[n],
            device_id=(site, to), device_id_type=MESH))
        fac_copies[-1].start()
    for i in range(owned):
        fac[own_at + i] = fac_s[i]

    grams = []
    for i in range(owned):
        stack = jnp.concatenate([site_v[s, i] for s in range(phys)], axis=0)
        grams.append(with_itself(stack, 0))
    roots = inverse_roots(grams)
    for i in range(owned):
        factor = product(as_lhs(split(roots[i])), as_rhs(split(unit_s[i]))).astype(bf16)
        stack = jnp.concatenate([site_v[s, i] for s in range(phys)], axis=0)
        fresh_left = jnp.dot(stack, factor, preferred_element_type=f32).astype(bf16)
        for s in range(phys):
            left_out[s, i] = fresh_left[s * width : (s + 1) * width]

    for copy in fac_copies:
        copy.wait_recv()
    for i in range(owned):
        for s in range(phys):
            right_out[s, i] = jnp.dot(
                fac[tab[0, s, own_at + i]], site_v[s, i], preferred_element_type=f32
            ).astype(bf16)

    for copy in sent + fac_copies + [unit_copy, tab_copy]:
        copy.wait_send()
    for n in range(secs - 1):
        gram_copy(lax.rem(sec + 1 + n, secs)).wait_send()

    def drain(t, carry):
        @pl.when(far_target)
        def _():
            for c in range(3):
                far_copy(t, c).wait_send()

        @pl.when(jnp.logical_not(far_target))
        def _():
            for c in range(len(NEAR)):
                near_copy(t, c).wait_send()

        @pl.when(far_source)
        def _():
            pair_copy(t).wait_send()

        return carry

    lax.fori_loop(0, last, drain, 0)

    @pl.when(role == 0)
    def _():
        nxt_copy.wait_send()
        for i in range(owned):
            for n in range(2):
                left_copy(n, i).wait_send()

    @pl.when(role == 1)
    def _():
        for copy in rgt_copies:
            copy.wait_send()


def update(table, energy, bond_add, canon_l, canon_r, seed_l, seed_r, site, bond):
    sites, secs = lax.axis_size("site"), lax.axis_size("sec")
    steps = sites // 4
    phys, owned, width = canon_l.shape[:3]
    sectors = owned * secs
    bf16, f32 = jnp.bfloat16, jnp.float32
    block = (width, width)
    dma = pltpu.SemaphoreType.DMA
    smem = pl.BlockSpec(memory_space=pltpu.SMEM)
    vmem = pl.BlockSpec(memory_space=pltpu.VMEM)
    hbm = pl.BlockSpec(memory_space=pltpu.HBM)
    mail = pltpu.VMEM((secs, width + 8, width), f32)
    return pl.pallas_call(
        functools.partial(update_kernel, sites, secs, steps),
        out_shape=(
            jax.ShapeDtypeStruct((phys, owned, *block), bf16),
            jax.ShapeDtypeStruct((phys, owned, *block), bf16),
        ),
        in_specs=[smem, hbm, hbm, smem] + [hbm] * 6,
        out_specs=(vmem, vmem),
        scratch_shapes=[
            pltpu.VMEM((2, 1 + phys, owned, *block), bf16),
            pltpu.VMEM((1 + phys, sectors, *block), bf16),
            pltpu.VMEM((2, sectors, width, phys * width), bf16),
            pltpu.VMEM((steps, sectors, *block), bf16),
            pltpu.VMEM((steps, sectors, *block), bf16),
            pltpu.VMEM((sectors, phys, *block), bf16),
            pltpu.VMEM((owned, *block), bf16),
            pltpu.VMEM((owned, *block), bf16),
            pltpu.VMEM((2, owned, *block), bf16),
            pltpu.VMEM((owned, *block), bf16),
            pltpu.VMEM((2, owned, phys, *block), bf16),
            pltpu.VMEM((owned, phys, *block), bf16),
            pltpu.SMEM((2, phys, sectors), jnp.int32),
            pltpu.VMEM((phys, sectors), jnp.int32),
            pltpu.SMEM((phys, sectors), jnp.int32),
            pltpu.SMEM((1, phys), f32),
            pltpu.VMEM((owned, *block), bf16),
            pltpu.VMEM((owned, *block), bf16),
            pltpu.VMEM((phys, owned, *block), bf16),
            pltpu.VMEM((owned, *block), bf16),
            pltpu.VMEM((phys, owned, *block), f32),
            mail, mail,
            pltpu.VMEM((owned, *block), f32),
            pltpu.VMEM((owned, *block), f32),
            pltpu.VMEM((owned, *block), bf16),
            pltpu.VMEM((sectors, *block), bf16),
            dma((7,)), dma((14,)), dma((14,)),
            dma((steps, 4)), dma((steps, 4)), dma((1,)), dma((1,)),
            dma((2,)), dma((secs,)), dma((secs,)), dma((secs - 1,)), dma((secs - 1,)),
            dma((steps,)), dma((2,)), dma((1,)),
            dma((2,)), dma((2, owned)), dma((owned,)),
        ],
        compiler_params=pltpu.CompilerParams(
            collective_id=0, has_side_effects=True, vmem_limit_bytes=30 * 1024 * 1024
        ),
        name="environments",
    )(
        table, pltpu.with_memory_space_constraint(table, pltpu.HBM),
        pltpu.with_memory_space_constraint(energy, pltpu.HBM), bond_add,
        *(
            pltpu.with_memory_space_constraint(x, pltpu.HBM)
            for x in (canon_l, canon_r, seed_l, seed_r, site, bond)
        ),
    )


def per_device(
    left_canon,
    right_canon,
    center_site,
    center_bond,
    left_seed,
    right_seed,
    left_sector,
    onsite,
    bond_shift,
):
    left_new, right_new = update(
        left_sector[0], onsite, bond_shift, left_canon[0], right_canon[0],
        left_seed[0], right_seed[0], center_site[0], center_bond[0],
    )
    return (left_new[None], right_new[None])


def solution(mesh):
    return jax.shard_map(
        per_device,
        mesh=mesh,
        in_specs=(
            P("site", None, "sec", None, None),
            P("site", None, "sec", None, None),
            P("site", None, "sec", None, None),
            P("site", "sec", None, None),
            P("site", "sec", None, None),
            P("site", "sec", None, None),
            P("site", None, None),
            P("site", None),
            P("site"),
        ),
        out_specs=(P("site", None, "sec", None, None), P("site", None, "sec", None, None)),
        check_vma=False,
    )
```

```python
import functools

import jax
import jax.numpy as jnp
from jax import lax
from jax.experimental import pallas as pl
from jax.experimental.pallas import tpu as pltpu
from jax.sharding import PartitionSpec as P

NSI = 10
NAPP = 2
NEAR = (8, 8)
FAR = (3, 5, 5, 3)
MESH = pl.DeviceIdType.MESH


def update_kernel(
    sites, secs, steps,
    src_tab, own_tab, energy_in, bond_add, canon_l, canon_r, seed_l, seed_r, site_in, bond_in,
    left_out, right_out,
    own_c, tall, wab, hold, fresh, pbuf, give_n, got_n, give_r, got_r, give_c, lefts, tab, tab_v, tab_n, energy, nxt, rgt, site_v, bond_v,
    outer, gram_s, gram_r, unit_s, unit_r, fac_s, fac,
    loc_sem, gsend, grecv, tsend, trecv, xsend, xrecv,
    usem, osend, orecv, fsend, frecv, psend, rsend, rrecv, bsem, lsend, lrecv,
):
    site, sec = lax.axis_index("site"), lax.axis_index("sec")
    role = lax.rem(sec, 2)
    row = sec // 2
    rows = secs // 2
    phys, owned, width = canon_l.shape[0], canon_l.shape[1], canon_l.shape[2]
    sectors = secs * owned
    target = lax.rem(site + 1 - 2 * role + sites, sites)
    source = lax.rem(site - 1 + 2 * role + sites, sites)
    peer_sec = row * 2 + 1 - role
    half = lax.rem(row, 2)
    pair_sec = sec + 2 - 4 * half
    far_target = lax.rem(site, 2) != role
    far_source = lax.rem(site, 2) == role
    ends = sectors - FAR[0]
    far_at = (half * ends, FAR[0], FAR[0] + FAR[1], (1 - half) * ends)
    near_at = (0, NEAR[0])
    last = steps - 1

    loads = [
        pltpu.make_async_copy(canon_l, own_c.at[0, pl.ds(1, phys)], loc_sem.at[0]),
        pltpu.make_async_copy(canon_r, own_c.at[1, pl.ds(1, phys)], loc_sem.at[1]),
    ]
    seeds = [
        pltpu.make_async_copy(seed_l, own_c.at[0, 0], loc_sem.at[4]),
        pltpu.make_async_copy(seed_r, own_c.at[1, 0], loc_sem.at[5]),
    ]
    center = [
        pltpu.make_async_copy(site_in, site_v, loc_sem.at[2]),
        pltpu.make_async_copy(bond_in, bond_v, loc_sem.at[3]),
        pltpu.make_async_copy(energy_in, energy, loc_sem.at[6]),
    ]
    for load in seeds + loads + center:
        load.start()

    barrier = pltpu.get_barrier_semaphore()
    others = [(dy, e) for dy in range(rows) for e in range(2) if (dy, e) != (0, 0)]
    others.sort(key=lambda at: -min(at[0], rows - at[0]) - at[1])

    def sec_of(dy, e):
        other_role = role + e - 2 * role * e
        return lax.rem(row + dy, rows) * 2 + other_role, other_role

    for dy, e in others:
        pl.semaphore_signal(barrier, inc=1, device_id=(site, sec_of(dy, e)[0]), device_id_type=MESH)
    for other in (target, source):
        pl.semaphore_signal(barrier, inc=1, device_id=(other, sec), device_id_type=MESH)
    across = lax.rem(site + 1 - 2 * role + sites, sites)
    pl.semaphore_signal(barrier, inc=1, device_id=(across, peer_sec), device_id_type=MESH)
    for load in seeds:
        load.wait()
    for i in range(owned):
        own_c[1, 0, i] = own_c[1, 0, i].T
    pl.semaphore_wait(barrier, len(others) + 3)

    place = pl.ds(sec * owned, owned)
    peer_place = pl.ds(peer_sec * owned, owned)
    parts = (pl.ds(0, 3), pl.ds(3, phys - 2))
    up_row, down_row = lax.rem(row + 1, rows), lax.rem(row + rows - 1, rows)
    up, down = up_row * 2 + role, down_row * 2 + role
    sent = []

    def gather_copy(n, src, part, at, to, slot):
        return pltpu.make_async_remote_copy(
            src_ref=src, dst_ref=tall.at[part, at], send_sem=gsend.at[n], recv_sem=grecv.at[slot],
            device_id=(site, to), device_id_type=MESH)

    def give_on(src, part, at, to, slot):
        sent.append(gather_copy(len(sent), src, part, at, to, slot))
        sent[-1].start()

    def landed(part, at, slot):
        gather_copy(0, tall.at[part, at], part, at, up, slot).wait_recv()

    tab_copy = pltpu.make_async_remote_copy(
        src_ref=own_tab, dst_ref=tab_v, send_sem=bsem.at[0], recv_sem=bsem.at[1],
        device_id=(source, sec), device_id_type=MESH)
    tab_copy.start()
    for load in loads:
        load.wait()
    for h in (1, 0):
        give_on(own_c.at[1 - role, parts[h]], parts[h], place, peer_sec, h)
    for h in range(2):
        give_on(own_c.at[role, parts[h]], parts[h], place, up, 2 + h)
        give_on(own_c.at[role, parts[1 - h]], parts[1 - h], place, down, 9 - h)
    keep = pltpu.make_async_copy(own_c.at[role], tall.at[:, place], loc_sem.at[0])
    keep.start()

    def block_at(of_row, of_peer):
        return pl.ds((of_row * 2 + (1 - role if of_peer else role)) * owned, owned)

    for h in range(2):
        part = parts[1 - h]
        landed(part, peer_place, 1 - h)
        give_on(tall.at[part, peer_place], part, peer_place, up, 5 - h)
        give_on(tall.at[part, peer_place], part, peer_place, down, 11 - h)
        part = parts[h]
        at = block_at(down_row, h)
        landed(part, at, 2 + 3 * h)
        give_on(tall.at[part, at], part, at, up, 6 + h)
        part = parts[1 - h]
        at = block_at(up_row, h)
        landed(part, at, 9 + h)
        give_on(tall.at[part, at], part, at, down, 12 + h)
    keep.wait()

    def tabulate(n, carry):
        s, m = n // sectors, lax.rem(n, sectors)
        joined = jnp.int32(0)
        for k in range(sectors):
            joined = jnp.where(src_tab[s, k] == m, k, joined)
        tab[0, s, m] = src_tab[s, m]
        tab[1, s, m] = joined
        return carry

    lax.fori_loop(0, phys * sectors, tabulate, 0)

    def turned(start, count):
        def body(n, carry):
            i = start + n
            hold[0, i] = tall[0, i]
            for s in range(phys):
                wab[1 - role, i, :, s * width : (s + 1) * width] = tall[1 + s, i].T
            return carry

        lax.fori_loop(0, count, body, 0)

    def row_at(of_row):
        return of_row * 2 * owned

    turned(row_at(row), 2 * owned)
    for h in range(2):
        landed(parts[1 - h], block_at(down_row, h), 3 + h)
    turned(row_at(down_row), 2 * owned)
    for h in range(2):
        landed(parts[h], block_at(up_row, h), 8 + 3 * h)
    turned(row_at(up_row), 2 * owned)
    far_row = lax.rem(row + 2, rows)
    for h in range(2):
        landed(parts[h], block_at(far_row, h), 6 + h)
        landed(parts[1 - h], block_at(far_row, h), 12 + h)
    turned(row_at(far_row), 2 * owned)
    tab_copy.wait_recv()
    pltpu.sync_copy(tab_v, tab_n)

    def in_order(i, carry):
        for s in range(phys):
            wab[role, i, :, s * width : (s + 1) * width] = tall[1 + s, tab[1, s, i]]
        return carry

    lax.fori_loop(0, sectors, in_order, 0)

    def to_target(t, c, part):
        return pltpu.make_async_remote_copy(
            src_ref=fresh.at[t, part], dst_ref=hold.at[t + 1, part],
            send_sem=tsend.at[t, c], recv_sem=trecv.at[t, c],
            device_id=(target, sec), device_id_type=MESH)

    def far_copy(t, c):
        return to_target(t, c, pl.ds(far_at[c], FAR[c]))

    def near_copy(t, c):
        return to_target(t, c, pl.ds(near_at[c], NEAR[c]))

    def pair_copy(t):
        part = pl.ds(far_at[0], FAR[0])
        return pltpu.make_async_remote_copy(
            src_ref=hold.at[t + 1, part], dst_ref=hold.at[t + 1, part],
            send_sem=psend.at[t], recv_sem=trecv.at[t, 3],
            device_id=(site, pair_sec), device_id_type=MESH)

    def apply_right(t, start, length):
        for i in range(length):
            at = start + i
            product = jnp.dot(
                hold[t, at], wab[0, at], preferred_element_type=jnp.float32
            ).astype(jnp.bfloat16)
            for s in range(phys):
                pbuf[at, s] = product[:, s * width : (s + 1) * width]

    def apply_left(t, start, length):
        for i in range(length):
            at = start + i
            stack = jnp.concatenate([pbuf[tab[role, s, at], s] for s in range(phys)], axis=0)
            fresh[t, at] = jnp.dot(
                wab[1, at], stack, preferred_element_type=jnp.float32
            ).astype(jnp.bfloat16)

    def first_half(t):
        came_far = jnp.logical_and(t > 0, far_source)

        @pl.when(came_far)
        def _():
            far_copy(t - 1, 0).wait_recv()
            pair_copy(t - 1).start()
            far_copy(t - 1, 1).wait_recv()
            apply_right(t, far_at[0], FAR[0])
            apply_right(t, far_at[1], FAR[1])
            for c in (2, 3):
                far_copy(t - 1, c).wait_recv()
                apply_right(t, far_at[c], FAR[c])

        @pl.when(jnp.logical_not(came_far))
        def _():
            @pl.when(t > 0)
            def _():
                for c in range(len(NEAR)):
                    near_copy(t - 1, c).wait_recv()

            apply_right(t, 0, sectors)

    def second_half(t, send):
        @pl.when(far_target)
        def _():
            for c in range(3):
                apply_left(t, far_at[c], FAR[c])
                if send:
                    far_copy(t, c).start()
            apply_left(t, far_at[3], FAR[3])

        @pl.when(jnp.logical_not(far_target))
        def _():
            for c in range(len(NEAR)):
                apply_left(t, near_at[c], NEAR[c])
                if send:
                    near_copy(t, c).start()

    def turn(t, carry):
        first_half(t)
        second_half(t, True)
        return carry

    lax.fori_loop(0, last, turn, 0)
    first_half(last)
    second_half(last, False)
    for load in center:
        load.wait()

    rows_at = lax.broadcasted_iota(jnp.int32, (width, width), 0)
    cols_at = lax.broadcasted_iota(jnp.int32, (width, width), 1)
    diagonal = rows_at == cols_at
    own_at = sec * owned
    peer_at = peer_sec * owned
    f32, bf16 = jnp.float32, jnp.bfloat16

    def scale_of(ref, t):
        total = ref[t, 0].astype(f32)
        for i in range(1, sectors):
            total = total + ref[t, i].astype(f32)
        return (sectors * width) / jnp.sum(jnp.where(diagonal, total, 0.0))

    def scaled(block, scale):
        return (block.astype(f32) * scale).astype(bf16)

    def left_copy(n, i):
        return pltpu.make_async_remote_copy(
            src_ref=give_c.at[n, i], dst_ref=lefts.at[i],
            send_sem=lsend.at[n, i], recv_sem=lrecv.at[i],
            device_id=(target, (peer_sec, sec)[n]), device_id_type=MESH)

    nxt_copy = pltpu.make_async_remote_copy(
        src_ref=give_n, dst_ref=got_n,
        send_sem=xsend.at[0], recv_sem=xrecv.at[0],
        device_id=(site, peer_sec), device_id_type=MESH)
    rgt_copies = [pltpu.make_async_remote_copy(
        src_ref=give_r.at[n], dst_ref=got_r,
        send_sem=rsend.at[n], recv_sem=rrecv.at[0],
        device_id=(target, to), device_id_type=MESH) for n, to in enumerate((peer_sec, sec))]

    @pl.when(role == 0)
    def _():
        scale_next = scale_of(fresh, last)
        for i in range(owned):
            for n, start in enumerate((peer_at, own_at)):
                for s in range(phys):
                    give_c[n, i, s] = scaled(fresh[last, tab_n[s, start + i]], scale_next)
                left_copy(n, i).start()
            give_n[i] = scaled(fresh[last, peer_at + i], scale_next)
            nxt[i] = scaled(fresh[last, own_at + i], scale_next)
        nxt_copy.start()

    @pl.when(role == 1)
    def _():
        scale_right = scale_of(fresh, last)
        for n, start in enumerate((peer_at, own_at)):
            for i in range(owned):
                give_r[n, i] = scaled(fresh[last, start + i], scale_right)
            rgt_copies[n].start()

    rgt_copies[0].wait_recv()
    for i in range(owned):
        rgt[i] = got_r[i].T

    def split(x):
        high = x.astype(bf16)
        return high, (x - high.astype(f32)).astype(bf16)

    def as_lhs(parts):
        return jnp.concatenate(parts, axis=1)

    def as_rhs(parts):
        wide = jnp.concatenate(parts, axis=1)
        return jnp.concatenate([wide, wide], axis=0)

    def product(lhs, rhs):
        both = jnp.dot(lhs, rhs, preferred_element_type=f32)
        return both[:, :width] + both[:, width:]

    def middle_of(part):
        return jnp.where(diagonal, 1.5, 0.0) - 0.5 * part

    def inverse_roots(grams):
        norms = [jnp.sqrt(jnp.sum(g * g, keepdims=True)) for g in grams]
        uppers, lowers = [], []
        for g, norm in zip(grams, norms):
            start = g / norm
            middle = middle_of(start)
            uppers.append(product(as_lhs(split(start)), as_rhs(split(middle))))
            lowers.append(middle)

        def repeat(n, carry):
            uppers, lowers = carry
            ups = [split(u) for u in uppers]
            lows = [split(l) for l in lowers]
            mids = [split(middle_of(product(as_lhs(l), as_rhs(u)))) for l, u in zip(lows, ups)]
            return (
                [product(as_lhs(u), as_rhs(m)) for u, m in zip(ups, mids)],
                [product(as_lhs(m), as_rhs(l)) for m, l in zip(mids, lows)],
            )

        uppers, lowers = lax.fori_loop(0, NSI - 2, repeat, (uppers, lowers))
        ups = [split(u) for u in uppers]
        lows = [split(l) for l in lowers]
        mids = [split(middle_of(product(as_lhs(l), as_rhs(u)))) for l, u in zip(lows, ups)]
        return [
            product(as_lhs(m), as_rhs(l)) / jnp.sqrt(norm)
            for m, l, norm in zip(mids, lows, norms)
        ]

    def with_itself(x, dim):
        return lax.dot_general(x, x, (((dim,), (dim,)), ((), ())), preferred_element_type=f32)

    for i in range(owned):
        left_copy(0, i).wait_recv()
        nows = [site_v[s, i] for s in range(phys)]
        for repeat in range(NAPP):
            halves = jnp.concatenate(
                [
                    jnp.dot(lefts[i, s], nows[s], preferred_element_type=f32).astype(bf16)
                    for s in range(phys)
                ],
                axis=0,
            )
            done = jnp.dot(halves, rgt[i], preferred_element_type=f32)
            nows = [
                (done[s * width : (s + 1) * width] + energy[0, s] * nows[s].astype(f32)).astype(bf16)
                for s in range(phys)
            ]
        for s in range(phys):
            site_v[s, i] = nows[s]
            outer[s, i] = with_itself(nows[s], 1)

    def gram_copy(d):
        return pltpu.make_async_remote_copy(
            src_ref=gram_s.at[d], dst_ref=gram_r.at[sec], send_sem=osend.at[d], recv_sem=orecv.at[sec],
            device_id=(site, d), device_id_type=MESH)

    def pack(n, carry):
        d = lax.rem(sec + 1 + n, secs)
        sums = []
        for i in range(owned):
            total = jnp.zeros((width, width), f32)
            for s in range(phys):
                at = tab[1, s, d * owned + i] - own_at
                mine = jnp.logical_and(at >= 0, at < owned)
                block = outer[s, jnp.clip(at, 0, owned - 1)]
                total = total + jnp.where(mine, block, 0.0)
            sums.append(total)
        gram_s[d, :width] = jnp.where(cols_at >= rows_at, sums[0], sums[1])
        line = jnp.sum(jnp.where(diagonal, sums[1], 0.0), axis=0, keepdims=True)
        gram_s[d, width:] = jnp.broadcast_to(line, (8, width))

        @pl.when(n < secs - 1)
        def _():
            gram_copy(d).start()

        return carry

    lax.fori_loop(0, secs, pack, 0)

    @pl.when(role == 1)
    def _():
        nxt_copy.wait_recv()
        for i in range(owned):
            nxt[i] = got_n[i]

    for i in range(owned):
        bond = bond_v[i]
        for repeat in range(NAPP):
            half_bond = jnp.dot(nxt[i], bond, preferred_element_type=f32).astype(bf16)
            bond = (
                jnp.dot(half_bond, rgt[i], preferred_element_type=f32)
                + bond_add[0] * bond.astype(f32)
            ).astype(bf16)
        bond_v[i] = bond

    roots = inverse_roots([with_itself(bond_v[i], 0) for i in range(owned)])
    for i in range(owned):
        turned_bond = bond_v[i].T
        unit_s[i] = jnp.dot(
            as_lhs(split(roots[i])),
            jnp.concatenate([turned_bond, turned_bond], axis=0),
            preferred_element_type=f32,
        )
    unit_copy = pltpu.make_async_remote_copy(
        src_ref=unit_s, dst_ref=unit_r, send_sem=usem.at[0], recv_sem=usem.at[1],
        device_id=(lax.rem(site + 1, sites), sec), device_id_type=MESH)
    unit_copy.start()
    def gram_from(d):
        return pltpu.make_async_remote_copy(
            src_ref=gram_s.at[d], dst_ref=gram_r.at[d], send_sem=osend.at[d], recv_sem=orecv.at[d],
            device_id=(site, d), device_id_type=MESH)

    for n in range(secs - 1):
        gram_from(lax.rem(sec + 1 + n, secs)).wait_recv()
    total = gram_s[sec]
    for n in range(secs - 1):
        total = total + gram_r[lax.rem(sec + 1 + n, secs)]
    packed, line = total[:width], total[width : width + 1]
    flipped = packed.T
    grams = [
        jnp.where(cols_at >= rows_at, packed, flipped),
        jnp.where(diagonal, line, jnp.where(rows_at > cols_at, packed, flipped)),
    ]
    roots = inverse_roots(grams)
    unit_copy.wait_recv()
    for i in range(owned):
        fac_s[i] = product(as_lhs(split(unit_r[i])), as_rhs(split(roots[i]))).astype(bf16)
    fac_copies = []
    for n, (dy, e) in enumerate(others):
        to, _ = sec_of(dy, e)
        fac_copies.append(pltpu.make_async_remote_copy(
            src_ref=fac_s, dst_ref=fac.at[place], send_sem=fsend.at[n], recv_sem=frecv.at[n],
            device_id=(site, to), device_id_type=MESH))
        fac_copies[-1].start()
    for i in range(owned):
        fac[own_at + i] = fac_s[i]

    grams = []
    for i in range(owned):
        stack = jnp.concatenate([site_v[s, i] for s in range(phys)], axis=0)
        grams.append(with_itself(stack, 0))
    roots = inverse_roots(grams)
    for i in range(owned):
        factor = product(as_lhs(split(roots[i])), as_rhs(split(unit_s[i]))).astype(bf16)
        stack = jnp.concatenate([site_v[s, i] for s in range(phys)], axis=0)
        fresh_left = jnp.dot(stack, factor, preferred_element_type=f32).astype(bf16)
        for s in range(phys):
            left_out[s, i] = fresh_left[s * width : (s + 1) * width]

    for copy in fac_copies:
        copy.wait_recv()
    for i in range(owned):
        for s in range(phys):
            right_out[s, i] = jnp.dot(
                fac[tab[0, s, own_at + i]], site_v[s, i], preferred_element_type=f32
            ).astype(bf16)

    for copy in sent + fac_copies + [unit_copy, tab_copy]:
        copy.wait_send()
    for n in range(secs - 1):
        gram_copy(lax.rem(sec + 1 + n, secs)).wait_send()

    def drain(t, carry):
        @pl.when(far_target)
        def _():
            for c in range(3):
                far_copy(t, c).wait_send()

        @pl.when(jnp.logical_not(far_target))
        def _():
            for c in range(len(NEAR)):
                near_copy(t, c).wait_send()

        @pl.when(far_source)
        def _():
            pair_copy(t).wait_send()

        return carry

    lax.fori_loop(0, last, drain, 0)

    @pl.when(role == 0)
    def _():
        nxt_copy.wait_send()
        for i in range(owned):
            for n in range(2):
                left_copy(n, i).wait_send()

    @pl.when(role == 1)
    def _():
        for copy in rgt_copies:
            copy.wait_send()


def update(table, energy, bond_add, canon_l, canon_r, seed_l, seed_r, site, bond):
    sites, secs = lax.axis_size("site"), lax.axis_size("sec")
    steps = sites // 4
    phys, owned, width = canon_l.shape[:3]
    sectors = owned * secs
    bf16, f32 = jnp.bfloat16, jnp.float32
    block = (width, width)
    dma = pltpu.SemaphoreType.DMA
    smem = pl.BlockSpec(memory_space=pltpu.SMEM)
    vmem = pl.BlockSpec(memory_space=pltpu.VMEM)
    hbm = pl.BlockSpec(memory_space=pltpu.HBM)
    mail = pltpu.VMEM((secs, width + 8, width), f32)
    return pl.pallas_call(
        functools.partial(update_kernel, sites, secs, steps),
        out_shape=(
            jax.ShapeDtypeStruct((phys, owned, *block), bf16),
            jax.ShapeDtypeStruct((phys, owned, *block), bf16),
        ),
        in_specs=[smem, hbm, hbm, smem] + [hbm] * 6,
        out_specs=(vmem, vmem),
        scratch_shapes=[
            pltpu.VMEM((2, 1 + phys, owned, *block), bf16),
            pltpu.VMEM((1 + phys, sectors, *block), bf16),
            pltpu.VMEM((2, sectors, width, phys * width), bf16),
            pltpu.VMEM((steps, sectors, *block), bf16),
            pltpu.VMEM((steps, sectors, *block), bf16),
            pltpu.VMEM((sectors, phys, *block), bf16),
            pltpu.VMEM((owned, *block), bf16),
            pltpu.VMEM((owned, *block), bf16),
            pltpu.VMEM((2, owned, *block), bf16),
            pltpu.VMEM((owned, *block), bf16),
            pltpu.VMEM((2, owned, phys, *block), bf16),
            pltpu.VMEM((owned, phys, *block), bf16),
            pltpu.SMEM((2, phys, sectors), jnp.int32),
            pltpu.VMEM((phys, sectors), jnp.int32),
            pltpu.SMEM((phys, sectors), jnp.int32),
            pltpu.SMEM((1, phys), f32),
            pltpu.VMEM((owned, *block), bf16),
            pltpu.VMEM((owned, *block), bf16),
            pltpu.VMEM((phys, owned, *block), bf16),
            pltpu.VMEM((owned, *block), bf16),
            pltpu.VMEM((phys, owned, *block), f32),
            mail, mail,
            pltpu.VMEM((owned, *block), f32),
            pltpu.VMEM((owned, *block), f32),
            pltpu.VMEM((owned, *block), bf16),
            pltpu.VMEM((sectors, *block), bf16),
            dma((7,)), dma((14,)), dma((14,)),
            dma((steps, 4)), dma((steps, 4)), dma((1,)), dma((1,)),
            dma((2,)), dma((secs,)), dma((secs,)), dma((secs - 1,)), dma((secs - 1,)),
            dma((steps,)), dma((2,)), dma((1,)),
            dma((2,)), dma((2, owned)), dma((owned,)),
        ],
        compiler_params=pltpu.CompilerParams(
            collective_id=0, has_side_effects=True, vmem_limit_bytes=30 * 1024 * 1024
        ),
        name="environments",
    )(
        table, pltpu.with_memory_space_constraint(table, pltpu.HBM),
        pltpu.with_memory_space_constraint(energy, pltpu.HBM), bond_add,
        *(
            pltpu.with_memory_space_constraint(x, pltpu.HBM)
            for x in (canon_l, canon_r, seed_l, seed_r, site, bond)
        ),
    )


def per_device(
    left_canon,
    right_canon,
    center_site,
    center_bond,
    left_seed,
    right_seed,
    left_sector,
    onsite,
    bond_shift,
):
    left_new, right_new = update(
        left_sector[0], onsite, bond_shift, left_canon[0], right_canon[0],
        left_seed[0], right_seed[0], center_site[0], center_bond[0],
    )
    return (left_new[None], right_new[None])


def solution(mesh):
    return jax.shard_map(
        per_device,
        mesh=mesh,
        in_specs=(
            P("site", None, "sec", None, None),
            P("site", None, "sec", None, None),
            P("site", None, "sec", None, None),
            P("site", "sec", None, None),
            P("site", "sec", None, None),
            P("site", "sec", None, None),
            P("site", None, None),
            P("site", None),
            P("site"),
        ),
        out_specs=(P("site", None, "sec", None, None), P("site", None, "sec", None, None)),
        check_vma=False,
    )
```
